128 devices in a mesh: groups: 4 (over y, x), slab: 32 (over z, core).
Axes of the slice: x: 2, y: 2, z: 16, core: 2. Of those that a mesh axis runs over, the one named last changes fastest.
The devices are a block of a 8x8x16 slice.
Arguments:
- wavefields: float32 [2, 4, 8, 4096, 512], P(None, None, 'groups', 'slab'), parts along dimension 2, may hold values from -6 to 6
- courant: float32 [4096, 512], P('slab'), may hold values from 0.04 to 0.16
- epsilon: float32 [4096, 512], P('slab'), may hold values from 0.1 to 0.3
- anisotropy_delta: float32 [4096, 512], P('slab'), may hold values from 0 to 0.1
- tilt_angle: float32 [4096, 512], P('slab'), may hold values from -3.140625 to 3.140625
- loc_patch: int32 [1024], replicated, may hold values from 0 to 127, as said below
- slab_counts: int32 [32], replicated, may hold values from 3 to 4
- angle_table: int32 [64], replicated, may hold values from -48 to 47
Outputs:
- gathers: float32 [4096, 4096], P(('groups', 'slab')), parts along dimension 0
The draws below stay inside these ranges and needn't reach their ends.
There are 4 independent parts, one for each index of `groups`. The reference program is written for one: setup_inputs(seed, part) draws one part's arguments, and reference() takes and returns one part's arrays. A program takes and returns all parts, laid end to end along the dimension named above; an argument that names none is the same for every part. Nothing has to cross between parts.
Inputs may be any that keep to these rules, and one draw needn't show every extreme that they name: `loc_patch`: location g names a patch id slab * 4 + column block; locations g of one owner are the 32 rows of an aligned block. Within one block no slab is named by more than 2 locations, and some slab is named by exactly 2 in every block.
All inputs are finite; a program needn't handle non-finite values.
Results may differ from the reference program's by a relative error of at most 0.0055.
Values may be sent and summed in bfloat16 or wider, within the bound.
No kernel may reach another device: no remote copies, remote signals or barrier semaphores. Data moves between devices by JAX's collectives and lax.ppermute only.
A program may use at most 128 MiB of HBM per device.

```python
import math
import jax
import jax.numpy as jnp
from jax import lax

PATCH = 128
ANG = 64
SHOTS = 2
STEPS = 2
NX = 512
BINS = 64
NZ = 4096
LOC_DEV = 32
LOC = 1024
N_SLAB = 32


def draw_loc_patch(key, part):
    keys = jax.random.split(jax.random.fold_in(key, 7), 3)
    blocks = LOC // LOC_DEV
    half_count = LOC_DEV // 2
    slab_ids = jnp.arange(LOC_DEV, dtype=jnp.int32)
    scores = jax.random.randint(keys[0], (blocks, LOC_DEV), 0, 64, dtype=jnp.int32) + 32 * (slab_ids < LOC_DEV // 4).astype(jnp.int32)[None, :]
    ranked = scores * LOC_DEV + slab_ids[None, :]
    ordering = jnp.argsort(-ranked, axis=1).astype(jnp.int32)
    flips = (jax.random.randint(keys[1], (blocks, LOC_DEV), 0, 4, dtype=jnp.int32) == 0).astype(jnp.int32)
    flips = flips.at[:, 0:2].set(0)
    position = jnp.arange(LOC_DEV, dtype=jnp.int32)
    chosen_rank = position[None, :] // 2 + half_count * flips
    slabs = jnp.take_along_axis(ordering, chosen_rank, axis=1)
    columns = jax.random.randint(keys[2], (blocks, LOC_DEV), 0, NX // PATCH, dtype=jnp.int32)
    return (slabs * (NX // PATCH) + columns).reshape(LOC).astype(jnp.int32)


def place_ends(array, own_key, least, top_value):
    longest = array.shape.index(max(array.shape))
    spots = []
    for shift in (0, 1):
        where = [jax.random.randint(jax.random.fold_in(own_key, axis), (), 0, length) for axis, length in enumerate(array.shape)]
        where[longest] = (where[longest] + shift) % array.shape[longest]
        spots.append(tuple(where))
    return array.at[spots[0]].set(least).at[spots[1]].set(top_value)


def block_scale(own_key, shape, shards, low, top_value):
    def one(dim, parts):
        heights = jax.random.uniform(jax.random.fold_in(jax.random.fold_in(own_key, 6), dim), (parts,), jnp.float32, low / len(shards), top_value / len(shards))
        return jnp.repeat(jnp.exp(heights), shape[dim] // parts).reshape((-1,) + (1,) * (len(shape) - dim - 1))

    factor_of = one(*shards[0])
    for cut in shards[1:]:
        factor_of = factor_of * one(*cut)
    return factor_of


def noise(stream_key, shape, deviation, reach, shards=(), kind=jnp.bfloat16):
    level = block_scale(stream_key, shape, shards, -0.22, 0.18) if shards else 1.0
    array = jax.random.normal(stream_key, shape, jnp.float32) * deviation * level
    return jnp.minimum(jnp.maximum(array, -reach), reach).astype(kind)


def setup_inputs(seed: int = 0, part: int = 0) -> dict:
    key_of = jax.random.split(jax.random.key(seed), 9)
    part_splits = jax.random.split(jax.random.fold_in(key_of[8], part), 9)
    wavefields = noise(part_splits[0], (2, 4, SHOTS, NZ, NX), 1.0, 6.0, ((3, 32),), jnp.float32)
    courant = jnp.clip(0.04 + 0.12 * jax.random.uniform(key_of[1], (NZ, NX), jnp.float32) ** block_scale(key_of[1], (NZ, NX), ((0, 32),), -0.2, 0.2), 0.04, 0.16)
    epsilon = jnp.clip(0.1 + 0.20000001043081284 * jax.random.uniform(key_of[2], (NZ, NX), jnp.float32) ** block_scale(key_of[2], (NZ, NX), ((0, 32),), -0.2, 0.2), 0.1, 0.3)
    anisotropy_delta = jnp.clip(0.1 * jax.random.uniform(key_of[3], (NZ, NX), jnp.float32) ** block_scale(key_of[3], (NZ, NX), ((0, 32),), -0.2, 0.2), 0.0, 0.1)
    tilt_angle = jnp.clip(jax.random.uniform(key_of[4], (NZ, NX), jnp.float32, -3.140625, 3.140625), -3.140625, 3.140625)
    loc_patch = draw_loc_patch(jax.random.fold_in(key_of[8], 71), part)
    slab_counts = place_ends(jax.random.randint(key_of[6], (N_SLAB,), NX // PATCH - 1, NX // PATCH + 1), jax.random.fold_in(key_of[6], 1), NX // PATCH - 1, (NX // PATCH + 1) - 1).astype(jnp.int32)
    angle_table = place_ends(jax.random.randint(key_of[7], (ANG,), -48, 48), jax.random.fold_in(key_of[7], 1), -48, 47).astype(jnp.int32)
    return {"wavefields": wavefields, "courant": courant, "epsilon": epsilon, "anisotropy_delta": anisotropy_delta, "tilt_angle": tilt_angle, "loc_patch": loc_patch, "slab_counts": slab_counts, "angle_table": angle_table}


SECOND_TERMS = (-205.0 / 72.0, 8.0 / 5.0, -1.0 / 5.0, 8.0 / 315.0, -1.0 / 560.0)
FIRST_TERMS = (4.0 / 5.0, -1.0 / 5.0, 4.0 / 105.0, -1.0 / 280.0)

def pad_columns(field):
    widths = [(0, 0)] * (field.ndim - 1) + [(4, 4)]
    return jnp.pad(field, widths)

def derivatives(field):
    row_count = field.shape[-2] - 8
    column_count = field.shape[-1]
    middle = field[..., 4:4 + row_count, :]
    beside = pad_columns(middle)
    second_z = SECOND_TERMS[0] * middle
    second_x = SECOND_TERMS[0] * middle
    first_z = jnp.zeros_like(middle)
    for offset in range(1, 5):
        upper_rows = field[..., 4 + offset:4 + offset + row_count, :]
        lower_rows = field[..., 4 - offset:4 - offset + row_count, :]
        second_z = second_z + SECOND_TERMS[offset] * (upper_rows + lower_rows)
        first_z = first_z + FIRST_TERMS[offset - 1] * (upper_rows - lower_rows)
        second_x = second_x + SECOND_TERMS[offset] * (beside[..., 4 + offset:4 + offset + column_count] + beside[..., 4 - offset:4 - offset + column_count])
    spread = pad_columns(first_z)
    mixed_term = jnp.zeros_like(middle)
    for offset in range(1, 5):
        mixed_term = mixed_term + FIRST_TERMS[offset - 1] * (spread[..., 4 + offset:4 + offset + column_count] - spread[..., 4 - offset:4 - offset + column_count])
    return (second_x, second_z, mixed_term)

def advance(current, previous, courant, epsilon, anisotropy_delta, tilt_angle):
    second_x, second_z, mixed_term = derivatives(current)
    sine_tilt = jnp.sin(tilt_angle)
    cosine = jnp.cos(tilt_angle)
    along_axis = sine_tilt * sine_tilt * second_x + cosine * cosine * second_z + 2.0 * sine_tilt * cosine * mixed_term
    across = second_x + second_z - along_axis
    root_delta = jnp.sqrt(1.0 + 2.0 * anisotropy_delta)
    push_pressure = (1.0 + 2.0 * epsilon) * across[:, 0] + root_delta * along_axis[:, 1]
    push_other = root_delta * across[:, 0] + along_axis[:, 1]
    middle = current[..., 4:-4, :]
    return 2.0 * middle - previous + courant * jnp.stack([push_pressure, push_other], axis=1)

def depth_table(patch, bins):
    wavenumber = jnp.arange(bins, dtype=jnp.int32)[:, None]
    depth_index = jnp.arange(patch, dtype=jnp.int32)[None, :]
    phase = 2.0 * math.pi / patch * jnp.mod(wavenumber * depth_index, patch).astype(jnp.float32)
    scale = 1.0 / math.sqrt(patch)
    return jnp.concatenate([jnp.cos(phase), -jnp.sin(phase)], axis=0) * scale

def slant_table(angle_table, patch, bins):
    wavenumber = jnp.arange(bins, dtype=jnp.int32)[:, None, None]
    lateral = jnp.arange(patch, dtype=jnp.int32)[None, None, :]
    slopes = angle_table.astype(jnp.int32)[None, :, None]
    modulus = 16 * patch
    phase = 2.0 * math.pi / modulus * jnp.mod(wavenumber * slopes * lateral, modulus).astype(jnp.float32)
    scale = 1.0 / math.sqrt(patch)
    real_part = jnp.cos(phase) * scale
    imag_part = -jnp.sin(phase) * scale
    upper_half = jnp.stack([real_part, -imag_part], axis=2)
    lower_half = jnp.stack([imag_part, real_part], axis=2)
    return jnp.concatenate([upper_half, lower_half], axis=1).astype(jnp.bfloat16)

def correlate(stacked, angles):
    shaped = stacked.reshape(stacked.shape[:-1] + (2, angles))
    product = shaped[..., 0, :, :, :, :] * shaped[..., 1, :, :, :, :]
    summed = lax.optimization_barrier(jnp.sum(product, axis=(-4, -2)))
    return summed.reshape(summed.shape[:-2] + (summed.shape[-2] * angles,))

def reference(wavefields, courant, epsilon, anisotropy_delta, tilt_angle, loc_patch, slab_counts, angle_table):
    states = jnp.transpose(wavefields, (0, 2, 1, 3, 4)).reshape(2 * SHOTS, 4, NZ, NX)

    def evolve(state):
        current = state[None, 0:2]
        previous = state[None, 2:4]
        for iteration in range(STEPS):
            extended = jnp.pad(current, ((0, 0), (0, 0), (4, 4), (0, 0)))
            current, previous = (advance(extended, previous, courant, epsilon, anisotropy_delta, tilt_angle), current)
        return current[0, 0]
    pressure = lax.map(evolve, states).reshape(2, SHOTS, N_SLAB, PATCH, NX)
    table = depth_table(PATCH, BINS)
    spectra = jnp.einsum('qz,fsbzx->fsbqx', table, pressure, precision=lax.Precision.HIGHEST).astype(jnp.bfloat16)
    spectra = spectra.reshape(2, SHOTS, N_SLAB, 2, BINS, NX // PATCH, PATCH)
    slant = slant_table(angle_table, PATCH, BINS).astype(jnp.float32)

    def image_slab(slab_number):
        piece = lax.dynamic_index_in_dim(spectra, slab_number, 2, keepdims=False).astype(jnp.float32)
        stacked = jnp.einsum('kirx,fsrkpx->pfski', slant, piece, precision=lax.Precision.HIGHEST)
        return correlate(stacked, ANG)
    images = lax.map(image_slab, jnp.arange(N_SLAB, dtype=jnp.int32))
    alive = (jnp.arange(NX // PATCH, dtype=jnp.int32)[None, :] < slab_counts[:, None]).astype(jnp.float32)
    images = (images * alive[:, :, None]).reshape(N_SLAB * (NX // PATCH), BINS * ANG)
    return jnp.take(images, loc_patch, axis=0)
```

```python
import math

import jax
import jax.numpy as jnp
import numpy as np
from jax import lax
from jax.experimental import pallas as pl
from jax.experimental.pallas import tpu as pltpu
from jax.sharding import Mesh
from jax.sharding import PartitionSpec as P

SLAB = ("chip", "core")
GROUPS_SLAB = ("groups", "chip", "core")
LANES = 128
HALF = 4
SECOND = (-14336.0, 8064.0, -1008.0, 128.0, -9.0)
SECOND_REST = 14.0
SECOND_UNIT = 5040.0
FIRST = (672.0, -168.0, 32.0, -3.0)
FIRST_UNIT = 840.0
BF16 = jnp.bfloat16
F32 = jnp.float32


def weight(kind, offset):
    if abs(offset) > HALF:
        return 0.0
    if kind == 2:
        return SECOND[abs(offset)]
    if offset == 0:
        return 0.0
    return FIRST[abs(offset) - 1] * (1.0 if offset > 0 else -1.0)


def band(kind, outputs, inputs):
    table = np.zeros((len(outputs), len(inputs)), np.float32)
    for i, o in enumerate(outputs):
        for j, n in enumerate(inputs):
            if o is not None and n is not None:
                table[i, j] = weight(kind, n - o)
    return table


def row_tables(rows):
    own = list(range(rows))
    inner = list(range(-HALF, 0)) + list(range(rows, rows + HALF))
    outer = list(range(-2 * HALF, -HALF)) + list(range(rows + HALF, rows + 2 * HALF))
    pad = [None] * 8
    first_in = own + inner + outer
    first_out = own + inner + pad
    second_in = own + inner + pad
    one = np.concatenate([band(2, first_out, first_in), band(1, first_out, first_in)])
    two = np.concatenate([band(2, own, second_in), band(1, own, second_in)])
    return one, two


def column_tables(kind):
    block = list(range(2 * LANES))
    inside = band(kind, block, block).T
    across = np.zeros((2 * LANES, 2 * LANES), np.float32)
    for i in range(2 * LANES):
        for o in range(2 * LANES):
            if (i < LANES) != (o < LANES):
                across[i, o] = weight(kind, i - o)
    return inside, across


def depth_table(patch, bins):
    k = np.arange(bins)[:, None]
    z = np.arange(patch)[None, :]
    phase = (2.0 * math.pi / patch * np.mod(k * z, patch)).astype(np.float32)
    table = np.concatenate([np.cos(phase), -np.sin(phase)]).astype(np.float32) * np.float32(1.0 / math.sqrt(patch))
    return table.astype(np.float32)


def quarter_turns(quarter, cosine, sine):
    odd = (quarter & 1) == 1
    c = jnp.where(odd, sine, cosine)
    s = jnp.where(odd, cosine, sine)
    c = jnp.where(((quarter + 1) & 2) == 2, -c, c)
    s = jnp.where((quarter & 2) == 2, -s, s)
    return c, s


def small_cos_sin(y):
    y2 = y * y
    s = y * (1.0 + y2 * (-1.6666654611e-1 + y2 * (8.3321608736e-3 + y2 * -1.9515295891e-4)))
    c = 1.0 - 0.5 * y2 + y2 * y2 * (4.166664568298827e-2 + y2 * (-1.388731625493765e-3 + y2 * 2.443315711809948e-5))
    return c, s


def double_angle(theta):
    n = jnp.floor(theta * (4.0 / math.pi) + 0.5)
    y = 2.0 * theta - n * 1.5703125
    y = y - n * 4.837512969970703e-4
    y = y - n * 7.54978995489188216e-8
    c, s = small_cos_sin(y)
    return quarter_turns(n.astype(jnp.int32), c, s)


def pack_kernel(w_top, w_bot, c_top, c_bot, e_top, e_bot, d_top, d_bot, t_top, t_bot, up_ref, down_ref):
    low = lax.broadcasted_iota(jnp.int32, (8, w_top.shape[-1]), 0) < HALF

    def half_turn(x):
        return pltpu.roll(x, HALF, 0)

    def emit(out, wave, params, upward):
        def join(a, b):
            return jnp.where(low, half_turn(a), b) if upward else jnp.where(low, a, half_turn(b))

        groups = []
        for w in range(wave.shape[0]):
            for s in range(wave.shape[2]):
                groups.append(wave[w, 0, s])
                groups.append(wave[w, 1, s])
                groups.append(join(wave[w, 2, s], wave[w, 3, s]))
        courant, eps, delta, tilt = (p[...] for p in params)
        high = tilt.astype(BF16).astype(F32)
        groups += [join(courant, eps), join(delta, high), tilt - high]
        groups.append(groups[-1])
        for g in range(0, len(groups), 2):
            out[8 * g : 8 * g + 16, :] = jnp.concatenate(groups[g : g + 2], axis=0).astype(BF16)

    emit(up_ref, w_bot, (c_bot, e_bot, d_bot, t_bot), True)
    emit(down_ref, w_top, (c_top, e_top, d_top, t_top), False)


def pack(wavefields, params):
    two, four, shots, rows, cols = wavefields.shape
    last = rows // 8 - 1
    groups = 2 * shots * 3 + 4
    wave_block = (two, four, shots, 8, cols)
    specs = [
        pl.BlockSpec(wave_block, lambda i: (0, 0, 0, 0, 0)),
        pl.BlockSpec(wave_block, lambda i: (0, 0, 0, last, 0)),
    ]
    args = [wavefields, wavefields]
    for p in params:
        specs += [pl.BlockSpec((8, cols), lambda i: (0, 0)), pl.BlockSpec((8, cols), lambda i: (last, 0))]
        args += [p, p]
    out = jax.ShapeDtypeStruct((8 * groups, cols), BF16)
    return pl.pallas_call(
        pack_kernel,
        grid=(1,),
        in_specs=specs,
        out_specs=[pl.BlockSpec((8 * groups, cols), lambda i: (0, 0))] * 2,
        out_shape=[out, out],
        name="pack",
    )(*args)


def main_kernel(
    counts_ref, wave_ref, courant_ref, eps_ref, delta_ref, tilt_ref, up_ref, down_ref,
    one_ref, two_ref, xx_ref, xx_across_ref, x_ref, x_across_ref, depth_ref, angle_ref,
    out_ref,
    mix_ref, twist_ref, a_ref, b_ref, c_ref, field_ref, slope_ref, row_ref, xx_out, xz_out, next_ref,
    split_ref, spectra_ref, low_c, low_s, high_c, high_s, image_ref,
):
    step = pl.program_id(0)
    rows, cols = courant_ref.shape
    ext = rows + 2 * HALF
    tall = rows + 4 * HALF
    low = lax.broadcasted_iota(jnp.int32, (8, cols), 0) < HALF

    def half_turn(x):
        return pltpu.roll(x, HALF, 0)

    def group(g):
        return (up_ref[8 * g : 8 * g + 8, :].astype(F32), down_ref[8 * g : 8 * g + 8, :].astype(F32))

    def first_halves(g):
        u, d = group(g)
        return jnp.where(low, u, half_turn(d))

    def second_halves(g):
        u, d = group(g)
        return jnp.where(low, half_turn(u), d)

    params = wave_groups = 3 * 4

    @pl.when(step == 0)
    def _():
        def coefficients(at, courant, eps, delta, tilt):
            cosine, sine = double_angle(tilt)
            scaled = courant * (1.0 / SECOND_UNIT)
            mix_ref[at, :] = 0.5 + 0.5 * cosine
            twist_ref[at, :] = sine * (SECOND_UNIT / (FIRST_UNIT * FIRST_UNIT))
            a_ref[at, :] = scaled * (1.0 + 2.0 * eps)
            b_ref[at, :] = scaled * jnp.sqrt(1.0 + 2.0 * delta)
            c_ref[at, :] = scaled

        for r in range(0, rows, 8):
            at = slice(r, r + 8)
            coefficients(at, courant_ref[at, :], eps_ref[at, :], delta_ref[at, :], tilt_ref[at, :])
        high = second_halves(params + 1)
        tilt = high + first_halves(params + 2)
        coefficients(
            slice(rows, ext), first_halves(params), second_halves(params), first_halves(params + 1), tilt
        )

    base = 3 * step

    def dyn_group(ref, g):
        return ref[pl.ds(pl.multiple_of(8 * (base + g), 8), 8), :].astype(F32)

    halo = []
    for f in range(2):
        u, d = (dyn_group(up_ref, f), dyn_group(down_ref, f))
        inner = jnp.where(low, half_turn(u), half_turn(d))
        outer = jnp.where(low, u, d)
        halo.append(inner)
        field_ref[f * tall : f * tall + rows, :] = wave_ref[0, f, 0].astype(BF16)
        field_ref[f * tall + rows : (f + 1) * tall, :] = jnp.concatenate([inner, outer], axis=0).astype(BF16)
    u, d = (dyn_group(up_ref, 2), dyn_group(down_ref, 2))
    halo.append(jnp.where(low, u, half_turn(d)))
    halo.append(jnp.where(low, half_turn(u), d))

    def along_columns(out, source, inside, across):
        left = jnp.dot(source[:, : 2 * LANES], inside[...], preferred_element_type=F32)
        right = jnp.dot(source[:, 2 * LANES :], inside[...], preferred_element_type=F32)
        mid = jnp.dot(source[:, LANES : 3 * LANES], across[...], preferred_element_type=F32)
        n = source.shape[0]
        out[:n, :LANES] = left[:, :LANES]
        out[:n, LANES : 2 * LANES] = left[:, LANES:] + mid[:, :LANES]
        out[:n, 2 * LANES : 3 * LANES] = right[:, :LANES] + mid[:, LANES:]
        out[:n, 3 * LANES :] = right[:, LANES:]

    def derive(table, count):
        for f in range(2):
            source = field_ref[f * tall : (f + 1) * tall, :]
            product = jnp.dot(table[...], source, preferred_element_type=F32)
            row_ref[f * tall : f * tall + count, :] = product[:count]
            slope_ref[f * count : (f + 1) * count, :] = product[count:].astype(BF16)
        along_columns(xx_out, field_ref[...], xx_ref, xx_across_ref)
        along_columns(xz_out, slope_ref[: 2 * count, :], x_ref, x_across_ref)

    def pieces(f, r, count, value):
        at = slice(f * tall + r, f * tall + r + 8)
        zz = row_ref[at, :]
        xx = xx_out[at, :]
        xz = xz_out[f * count + r : f * count + r + 8, :]
        turn = mix_ref[r : r + 8, :] * (xx - zz) - twist_ref[r : r + 8, :] * xz
        rest = SECOND_REST * value
        return (zz + turn) - rest if f == 0 else (xx - turn) - rest

    derive(one_ref, tall)
    for r in range(0, ext, 8):
        at = slice(r, r + 8)
        if r < rows:
            p, q, p0, q0 = (wave_ref[0, f, 0, at, :] for f in range(4))
        else:
            p, q, p0, q0 = halo
        across = pieces(0, r, tall, p)
        along = pieces(1, r, tall, q)
        a, b, c = (a_ref[at, :], b_ref[at, :], c_ref[at, :])
        next_ref[0, at, :] = (2.0 * p - p0) + (a * across + b * along)
        next_ref[1, at, :] = (2.0 * q - q0) + (b * across + c * along)

    for f in range(2):
        field_ref[f * tall : f * tall + rows, :] = next_ref[f, :rows, :].astype(BF16)
        edge = next_ref[f, rows:ext, :]
        field_ref[f * tall + rows : (f + 1) * tall, :] = jnp.concatenate([edge, jnp.zeros_like(edge)], axis=0).astype(BF16)
    derive(two_ref, rows)
    for r in range(0, rows, 16):
        parts = []
        for h in (r, r + 8):
            at = slice(h, h + 8)
            p, q = (next_ref[0, at, :], next_ref[1, at, :])
            across = pieces(0, h, rows, p)
            along = pieces(1, h, rows, q)
            parts.append((2.0 * p - wave_ref[0, 0, 0, at, :]) + (a_ref[at, :] * across + b_ref[at, :] * along))
        value = jnp.concatenate(parts, axis=0)
        top = value.astype(BF16)
        split_ref[r : r + 16, :] = top
        split_ref[rows + r : rows + r + 16, :] = (value - top.astype(F32)).astype(BF16)
        split_ref[2 * rows + r : 2 * rows + r + 16, :] = top
    spectra = jnp.dot(depth_ref[...], split_ref[...], preferred_element_type=F32)
    bins = rows // 2
    per_slab = cols // LANES
    for part in range(2):
        for m in range(per_slab):
            start = 16 * part + per_slab * step + m
            spectra_ref[pl.ds(start, bins, stride=32), :] = spectra[
                part * bins : (part + 1) * bins, m * LANES : (m + 1) * LANES
            ]

    @pl.when(step == pl.num_programs(0) - 1)
    def _():
        right_half = lax.broadcasted_iota(jnp.int32, (LANES, LANES), 1) >= LANES // 2
        angles = jnp.concatenate([angle_ref[...], angle_ref[...]], axis=1)
        lateral = lax.broadcasted_iota(jnp.int32, (LANES, LANES), 0)
        modulus = 16 * LANES
        turn = (lateral * angles) & (modulus - 1)
        quarter = (turn + modulus // 8) >> int(math.log2(modulus // 4))
        rest = turn - quarter * (modulus // 4)
        c1, s1 = small_cos_sin(rest.astype(F32) * (2.0 * math.pi / modulus))
        c1, s1 = quarter_turns(quarter, c1, s1)

        def times(x, y):
            return (x[0] * y[0] - x[1] * y[1], x[0] * y[1] + x[1] * y[0])

        unit = (jnp.ones_like(c1), jnp.zeros_like(c1))
        value = unit
        for j in range(8):
            low_c[j], low_s[j] = value
            value = (c1, s1) if j == 0 else times(value, (c1, s1))
        eighth = value
        scale = 1.0 / math.sqrt(LANES)
        value = (jnp.where(right_half, 0.0, scale), jnp.where(right_half, scale, 0.0))
        for j in range(8):
            high_c[j], high_s[j] = value
            value = times(value, eighth)

        left_lane = lax.broadcasted_iota(jnp.int32, (8, LANES), 1) < LANES // 2
        alive = lax.broadcasted_iota(jnp.int32, (8, LANES), 0) < counts_ref[lax.axis_index(SLAB)]

        def some(j, carry):
            hc, hs = (high_c[j], high_s[j])
            pair = []
            for i in range(8):
                lc, ls = (low_c[i], low_s[i])
                real = (hc * lc - hs * ls).astype(BF16)
                imag = (hc * ls + hs * lc).astype(BF16)
                at = pl.multiple_of((8 * j + i) * 32, 32)
                left = jnp.concatenate(
                    [spectra_ref[pl.ds(at, 16), :], spectra_ref[pl.ds(at + 16, 16), :]], axis=1
                ).astype(BF16)
                stack = jnp.dot(left, jnp.concatenate([real, imag], axis=0), preferred_element_type=F32)
                product = stack[:8] * stack[8:]
                pair.append(product + half_turn_small(product))
                if i % 2 == 1:
                    even, odd = pair
                    even = even + pltpu.roll(even, LANES // 2, 1)
                    odd = odd + pltpu.roll(odd, LANES // 2, 1)
                    pair = []
                    where_to = pl.multiple_of((4 * j + i // 2) * LANES, LANES)
                    image_ref[:, pl.ds(where_to, LANES)] = jnp.where(
                        alive, jnp.where(left_lane, even, odd), 0.0
                    )
            return carry

        def half_turn_small(x):
            return pltpu.roll(x, 4, 0)

        lax.fori_loop(0, bins // 8, some, 0)
        out_ref[...] = image_ref[:per_slab, :].astype(BF16)


def images_of(wavefields, params, up, down, slab_counts, angle_table):
    two, four, shots, rows, cols = wavefields.shape
    bins = rows // 2
    per_slab = cols // rows
    angles = angle_table.shape[0]
    ext = rows + 2 * HALF
    tall = rows + 4 * HALF
    one, both = row_tables(rows)
    xx, xx_across = column_tables(2)
    x, x_across = column_tables(1)
    depth = depth_table(rows, bins)
    depth_top = depth.astype(jnp.bfloat16)
    depth_low = (depth - depth_top.astype(np.float32)).astype(jnp.bfloat16)
    depth = np.concatenate([depth_top, depth_top, depth_low], axis=1)
    tables = [jnp.asarray(t, dtype=BF16) for t in (one, both, xx, xx_across, x, x_across, depth)]

    def whole(a):
        return pl.BlockSpec(a.shape, lambda i: (0,) * a.ndim)

    angle_row = angle_table.reshape(1, angles)
    args = [slab_counts, wavefields, *params, up, down, *tables, angle_row]
    specs = [
        pl.BlockSpec(memory_space=pltpu.SMEM),
        pl.BlockSpec((1, four, 1, rows, cols), lambda i: (i // shots, 0, i % shots, 0, 0)),
    ] + [whole(a) for a in args[2:]]
    out_shape = (per_slab, bins * angles)
    scratch = [pltpu.VMEM((ext, cols), F32)] * 5 + [
        pltpu.VMEM((2 * tall, cols), BF16),
        pltpu.VMEM((2 * tall, cols), BF16),
        pltpu.VMEM((2 * tall, cols), F32),
        pltpu.VMEM((2 * tall, cols), F32),
        pltpu.VMEM((2 * tall, cols), F32),
        pltpu.VMEM((2, ext, cols), F32),
        pltpu.VMEM((3 * rows, cols), BF16),
        pltpu.VMEM((32 * bins, LANES), F32),
    ] + [pltpu.VMEM((8, LANES, LANES), F32)] * 4 + [pltpu.VMEM((8, bins * angles), F32)]
    return pl.pallas_call(
        main_kernel,
        grid=(2 * shots,),
        in_specs=specs,
        out_specs=pl.BlockSpec(out_shape, lambda i: (0, 0)),
        out_shape=jax.ShapeDtypeStruct(out_shape, BF16),
        scratch_shapes=scratch,
        name="images",
    )(*args)


def pick_kernel(loc_ref, own_ref, other_ref, out_ref):
    slab = lax.axis_index(SLAB)
    core = lax.axis_index("core")
    count = out_ref.shape[0]
    per_row = LANES // count
    loc = loc_ref[pl.ds(slab // per_row, 1), :]
    loc = pltpu.roll(loc, (LANES - (slab % per_row) * count) % LANES, 1)[:, :count]
    held = own_ref.shape[0]
    per_slab = 4
    owner = loc // per_slab
    index = (owner // 2) * per_slab + loc % per_slab
    mine = owner % 2 == core
    row = lax.broadcasted_iota(jnp.int32, (held, count), 0)
    hit = row == index
    own_hot = jnp.where(hit & mine, 1.0, 0.0).astype(BF16)
    other_hot = jnp.where(hit & jnp.logical_not(mine), 1.0, 0.0).astype(BF16)

    def choose(hot, ref):
        return lax.dot_general(hot, ref[...], (((0,), (0,)), ((), ())), preferred_element_type=F32)

    out_ref[...] = choose(own_hot, own_ref) + choose(other_hot, other_ref)


def pick(loc_patch, own, other, count):
    width = own.shape[1]
    return pl.pallas_call(
        pick_kernel,
        out_shape=jax.ShapeDtypeStruct((count, width), F32),
        name="pick",
    )(loc_patch.reshape(-1, LANES), own, other)


def per_device(
    wavefields, courant, epsilon, anisotropy_delta, tilt_angle, loc_patch, slab_counts, angle_table
):
    slabs = lax.axis_size(SLAB)
    params = (courant, epsilon, anisotropy_delta, tilt_angle)
    up_send, down_send = pack(wavefields, params)
    up = lax.ppermute(up_send, SLAB, [(i, i + 1) for i in range(slabs - 1)])
    down = lax.ppermute(down_send, SLAB, [(i + 1, i) for i in range(slabs - 1)])
    images = images_of(wavefields, params, up, down, slab_counts, angle_table)
    own = lax.all_gather(images, "chip", tiled=True)
    other = lax.ppermute(own, "core", [(0, 1), (1, 0)])
    return pick(loc_patch, own, other, loc_patch.shape[0] // slabs)


def solution(mesh):
    slabs = mesh.shape["slab"]
    finer = Mesh(mesh.devices.reshape(mesh.shape["groups"], slabs // 2, 2), GROUPS_SLAB)
    in_specs = (
        P(None, None, "groups", SLAB, None),
        P(SLAB, None),
        P(SLAB, None),
        P(SLAB, None),
        P(SLAB, None),
        P(),
        P(),
        P(),
    )
    out_specs = P(GROUPS_SLAB, None)
    return jax.shard_map(
        per_device, mesh=finer, in_specs=in_specs, out_specs=out_specs, check_vma=False
    )
```

```python
import math

import jax
import jax.numpy as jnp
import numpy as np
from jax import lax
from jax.experimental import pallas as pl
from jax.experimental.pallas import tpu as pltpu
from jax.sharding import Mesh
from jax.sharding import PartitionSpec as P

SLAB = ("far", "near", "core")
GROUPS_SLAB = ("groups", "far", "near", "core")
LANES = 128
HALF = 4
SECOND = (-14336.0, 8064.0, -1008.0, 128.0, -9.0)
SECOND_REST = 14.0
SECOND_UNIT = 5040.0
FIRST = (672.0, -168.0, 32.0, -3.0)
FIRST_UNIT = 840.0
BF16 = jnp.bfloat16
F32 = jnp.float32
VMEM_WHOLE = pl.BlockSpec(memory_space=pltpu.VMEM)


def in_vmem(*arrays):
    return [pltpu.with_memory_space_constraint(a, pltpu.VMEM) for a in arrays]


def weight(kind, offset):
    if abs(offset) > HALF:
        return 0.0
    if kind == 2:
        return SECOND[abs(offset)]
    if offset == 0:
        return 0.0
    return FIRST[abs(offset) - 1] * (1.0 if offset > 0 else -1.0)


def band(kind, outputs, inputs):
    table = np.zeros((len(outputs), len(inputs)), np.float32)
    for i, o in enumerate(outputs):
        for j, n in enumerate(inputs):
            if o is not None and n is not None:
                table[i, j] = weight(kind, n - o)
    return table


def row_tables(rows):
    own = list(range(rows))
    inner = list(range(-HALF, 0)) + list(range(rows, rows + HALF))
    outer = list(range(-2 * HALF, -HALF)) + list(range(rows + HALF, rows + 2 * HALF))
    pad = [None] * 8
    first_in = own + inner + outer
    first_out = own + inner + pad
    second_in = own + inner + pad
    one = np.concatenate([band(2, first_out, first_in), band(1, first_out, first_in)])
    two = np.concatenate([band(2, own, second_in), band(1, own, second_in)])
    return one, two


def column_tables(kind):
    block = list(range(2 * LANES))
    inside = band(kind, block, block).T
    across = np.zeros((2 * LANES, 2 * LANES), np.float32)
    for i in range(2 * LANES):
        for o in range(2 * LANES):
            if (i < LANES) != (o < LANES):
                across[i, o] = weight(kind, i - o)
    return inside, across


def depth_table(patch, bins):
    k = np.arange(bins)[:, None]
    z = np.arange(patch)[None, :]
    phase = (2.0 * math.pi / patch * np.mod(k * z, patch)).astype(np.float32)
    table = np.concatenate([np.cos(phase), -np.sin(phase)]).astype(np.float32) * np.float32(1.0 / math.sqrt(patch))
    return table.astype(np.float32)


def quarter_turns(quarter, cosine, sine):
    odd = (quarter & 1) == 1
    c = jnp.where(odd, sine, cosine)
    s = jnp.where(odd, cosine, sine)
    c = jnp.where(((quarter + 1) & 2) == 2, -c, c)
    s = jnp.where((quarter & 2) == 2, -s, s)
    return c, s


def small_cos_sin(y):
    y2 = y * y
    s = y * (1.0 + y2 * (-1.6666654611e-1 + y2 * (8.3321608736e-3 + y2 * -1.9515295891e-4)))
    c = 1.0 - 0.5 * y2 + y2 * y2 * (4.166664568298827e-2 + y2 * (-1.388731625493765e-3 + y2 * 2.443315711809948e-5))
    return c, s


def double_angle(theta):
    n = jnp.floor(theta * (4.0 / math.pi) + 0.5)
    y = 2.0 * theta - n * 1.5703125
    y = y - n * 4.837512969970703e-4
    y = y - n * 7.54978995489188216e-8
    c, s = small_cos_sin(y)
    return quarter_turns(n.astype(jnp.int32), c, s)


def pack_kernel(
    w_top, w_bot, c_top, c_bot, e_top, e_bot, d_top, d_bot, t_top, t_bot, partner_ref, neighbour_ref
):
    low = lax.broadcasted_iota(jnp.int32, (8, w_top.shape[-1]), 0) < HALF

    def half_turn(x):
        return pltpu.roll(x, HALF, 0)

    def emit(out, wave, params, upward):
        def join(a, b):
            return jnp.where(low, half_turn(a), b) if upward else jnp.where(low, a, half_turn(b))

        groups = []
        for w in range(wave.shape[0]):
            for s in range(wave.shape[2]):
                groups.append(wave[w, 0, s])
                groups.append(wave[w, 1, s])
                groups.append(join(wave[w, 2, s], wave[w, 3, s]))
        courant, eps, delta, tilt = (p[...] for p in params)
        high = tilt.astype(BF16).astype(F32)
        groups += [join(courant, eps), join(delta, high), tilt - high]
        groups.append(groups[-1])
        for g in range(0, len(groups), 2):
            out[8 * g : 8 * g + 16, :] = jnp.concatenate(groups[g : g + 2], axis=0).astype(BF16)

    tops = (w_top, (c_top, e_top, d_top, t_top))
    bottoms = (w_bot, (c_bot, e_bot, d_bot, t_bot))
    first = lax.axis_index("core") == 0

    @pl.when(first)
    def _():
        emit(partner_ref, *bottoms, True)
        emit(neighbour_ref, *tops, False)

    @pl.when(jnp.logical_not(first))
    def _():
        emit(partner_ref, *tops, False)
        emit(neighbour_ref, *bottoms, True)


def pack(wavefields, params):
    two, four, shots, rows, cols = wavefields.shape
    last = rows // 8 - 1
    groups = 2 * shots * 3 + 4
    wave_block = (two, four, shots, 8, cols)
    specs = [
        pl.BlockSpec(wave_block, lambda i: (0, 0, 0, 0, 0)),
        pl.BlockSpec(wave_block, lambda i: (0, 0, 0, last, 0)),
    ]
    args = [wavefields, wavefields]
    for p in params:
        specs += [pl.BlockSpec((8, cols), lambda i: (0, 0)), pl.BlockSpec((8, cols), lambda i: (last, 0))]
        args += [p, p]
    out = pltpu.VMEM((8 * groups, cols), BF16)
    return pl.pallas_call(
        pack_kernel,
        grid=(1,),
        in_specs=specs,
        out_specs=[VMEM_WHOLE] * 2,
        out_shape=[out, out],
        compiler_params=pltpu.CompilerParams(vmem_limit_bytes=8 << 20),
        name="pack",
    )(*(pltpu.with_memory_space_constraint(a, pltpu.HBM) for a in args))


def coefficients(courant, eps, delta, tilt):
    cosine, sine = double_angle(tilt)
    scaled = courant * (1.0 / SECOND_UNIT)
    return (
        0.5 + 0.5 * cosine,
        sine * (SECOND_UNIT / (FIRST_UNIT * FIRST_UNIT)),
        scaled * (1.0 + 2.0 * eps),
        scaled * jnp.sqrt(1.0 + 2.0 * delta),
        scaled,
    )


def prepare_kernel(
    counts_ref, courant_ref, eps_ref, delta_ref, tilt_ref, angle_ref,
    mix_ref, twist_ref, a_ref, b_ref, c_ref, low_c, low_s, high_c, high_s, alive_ref,
):
    for r in range(0, courant_ref.shape[0], 8):
        at = slice(r, r + 8)
        values = coefficients(courant_ref[at, :], eps_ref[at, :], delta_ref[at, :], tilt_ref[at, :])
        for ref, value in zip((mix_ref, twist_ref, a_ref, b_ref, c_ref), values, strict=True):
            ref[at, :] = value

    right_half = lax.broadcasted_iota(jnp.int32, (LANES, LANES), 1) >= LANES // 2
    angles = jnp.concatenate([angle_ref[...], angle_ref[...]], axis=1)
    lateral = lax.broadcasted_iota(jnp.int32, (LANES, LANES), 0)
    modulus = 16 * LANES
    turn = (lateral * angles) & (modulus - 1)
    quarter = (turn + modulus // 8) >> int(math.log2(modulus // 4))
    rest = turn - quarter * (modulus // 4)
    c1, s1 = small_cos_sin(rest.astype(F32) * (2.0 * math.pi / modulus))
    c1, s1 = quarter_turns(quarter, c1, s1)

    def times(x, y):
        return (x[0] * y[0] - x[1] * y[1], x[0] * y[1] + x[1] * y[0])

    value = (jnp.ones_like(c1), jnp.zeros_like(c1))
    for j in range(8):
        low_c[j], low_s[j] = value
        value = (c1, s1) if j == 0 else times(value, (c1, s1))
    eighth = value
    scale = 1.0 / math.sqrt(LANES)
    value = (jnp.where(right_half, 0.0, scale), jnp.where(right_half, scale, 0.0))
    for j in range(8):
        high_c[j], high_s[j] = value
        value = times(value, eighth)
    live = lax.broadcasted_iota(jnp.int32, (8, LANES), 0) < counts_ref[lax.axis_index(SLAB)]
    alive_ref[...] = jnp.where(live, 1.0, 0.0)


def prepare(params, slab_counts, angle_table):
    rows, cols = params[0].shape
    field = pltpu.VMEM((rows, cols), F32)
    table = pltpu.VMEM((8, LANES, LANES), F32)
    return pl.pallas_call(
        prepare_kernel,
        in_specs=[pl.BlockSpec(memory_space=pltpu.SMEM)] + [VMEM_WHOLE] * 5,
        out_specs=[VMEM_WHOLE] * 10,
        out_shape=[field] * 5 + [table] * 4 + [pltpu.VMEM((8, LANES), F32)],
        compiler_params=pltpu.CompilerParams(vmem_limit_bytes=8 << 20),
        name="prepare",
    )(slab_counts, *in_vmem(*params, angle_table.reshape(1, -1)))


def main_kernel(
    wave_ref, partner_ref, neighbour_ref, mix_ref, twist_ref, a_ref, b_ref, c_ref,
    low_c, low_s, high_c, high_s, alive_ref,
    one_ref, two_ref, xx_ref, xx_across_ref, x_ref, x_across_ref, depth_ref,
    out_ref,
    edge_ref, field_ref, slope_ref, row_ref, xx_out, xz_out, next_ref, split_ref, spectra_ref, image_ref,
):
    step = pl.program_id(0)
    shots = wave_ref.shape[2]
    which = step // shots
    shot = step % shots
    rows, cols = mix_ref.shape
    ext = rows + 2 * HALF
    tall = rows + 4 * HALF
    low = lax.broadcasted_iota(jnp.int32, (8, cols), 0) < HALF
    first = lax.axis_index("core") == 0

    def half_turn(x):
        return pltpu.roll(x, HALF, 0)

    def group(g):
        at = pl.ds(g if isinstance(g, int) else pl.multiple_of(g, 8), 8)
        a, b = (partner_ref[at, :].astype(F32), neighbour_ref[at, :].astype(F32))
        return jnp.where(first, b, a), jnp.where(first, a, b)

    @pl.when(step == 0)
    def _():
        start = 8 * 3 * 2 * shots

        def first_halves(g):
            u, d = group(start + 8 * g)
            return jnp.where(low, u, half_turn(d))

        def second_halves(g):
            u, d = group(start + 8 * g)
            return jnp.where(low, half_turn(u), d)

        values = coefficients(
            first_halves(0), second_halves(0), first_halves(1), second_halves(1) + first_halves(2)
        )
        for i, value in enumerate(values):
            edge_ref[i] = value

    base = 8 * 3 * step
    halo = []
    for f in range(2):
        u, d = group(base + 8 * f)
        inner = jnp.where(low, half_turn(u), half_turn(d))
        outer = jnp.where(low, u, d)
        halo.append(inner)
        field_ref[f * tall : f * tall + rows, :] = wave_ref[which, f, shot].astype(BF16)
        field_ref[f * tall + rows : (f + 1) * tall, :] = jnp.concatenate([inner, outer], axis=0).astype(BF16)
    u, d = group(base + 16)
    halo.append(jnp.where(low, u, half_turn(d)))
    halo.append(jnp.where(low, half_turn(u), d))

    def along_columns(out, source, inside, across):
        left = jnp.dot(source[:, : 2 * LANES], inside[...], preferred_element_type=F32)
        right = jnp.dot(source[:, 2 * LANES :], inside[...], preferred_element_type=F32)
        mid = jnp.dot(source[:, LANES : 3 * LANES], across[...], preferred_element_type=F32)
        n = source.shape[0]
        out[:n, :LANES] = left[:, :LANES]
        out[:n, LANES : 2 * LANES] = left[:, LANES:] + mid[:, :LANES]
        out[:n, 2 * LANES : 3 * LANES] = right[:, :LANES] + mid[:, LANES:]
        out[:n, 3 * LANES :] = right[:, LANES:]

    def derive(table, count):
        for f in range(2):
            source = field_ref[f * tall : (f + 1) * tall, :]
            product = jnp.dot(table[...], source, preferred_element_type=F32)
            row_ref[f * tall : f * tall + count, :] = product[:count]
            slope_ref[f * count : (f + 1) * count, :] = product[count:].astype(BF16)
        along_columns(xx_out, field_ref[...], xx_ref, xx_across_ref)
        along_columns(xz_out, slope_ref[: 2 * count, :], x_ref, x_across_ref)

    def coefficient(i, r):
        if r < rows:
            return (mix_ref, twist_ref, a_ref, b_ref, c_ref)[i][r : r + 8, :]
        return edge_ref[i]

    def pieces(f, r, count, value):
        at = slice(f * tall + r, f * tall + r + 8)
        zz = row_ref[at, :]
        xx = xx_out[at, :]
        xz = xz_out[f * count + r : f * count + r + 8, :]
        mix, twist = (coefficient(i, r) for i in range(2))
        turn = mix * (xx - zz) - twist * xz
        rest = SECOND_REST * value
        return (zz + turn) - rest if f == 0 else (xx - turn) - rest

    derive(one_ref, tall)
    for r in range(0, ext, 8):
        at = slice(r, r + 8)
        if r < rows:
            p, q, p0, q0 = (wave_ref[which, f, shot, at, :] for f in range(4))
        else:
            p, q, p0, q0 = halo
        across = pieces(0, r, tall, p)
        along = pieces(1, r, tall, q)
        a, b, c = (coefficient(i, r) for i in range(2, 5))
        next_ref[0, at, :] = (2.0 * p - p0) + (a * across + b * along)
        next_ref[1, at, :] = (2.0 * q - q0) + (b * across + c * along)

    for f in range(2):
        field_ref[f * tall : f * tall + rows, :] = next_ref[f, :rows, :].astype(BF16)
        edge = next_ref[f, rows:ext, :]
        field_ref[f * tall + rows : (f + 1) * tall, :] = jnp.concatenate([edge, jnp.zeros_like(edge)], axis=0).astype(BF16)
    derive(two_ref, rows)
    for r in range(0, rows, 16):
        parts = []
        for h in (r, r + 8):
            at = slice(h, h + 8)
            p, q = (next_ref[0, at, :], next_ref[1, at, :])
            across = pieces(0, h, rows, p)
            along = pieces(1, h, rows, q)
            parts.append((2.0 * p - wave_ref[which, 0, shot, at, :]) + (a_ref[at, :] * across + b_ref[at, :] * along))
        value = jnp.concatenate(parts, axis=0)
        top = value.astype(BF16)
        split_ref[r : r + 16, :] = top
        split_ref[rows + r : rows + r + 16, :] = (value - top.astype(F32)).astype(BF16)
        split_ref[2 * rows + r : 2 * rows + r + 16, :] = top
    spectra = jnp.dot(depth_ref[...], split_ref[...], preferred_element_type=F32)
    bins = rows // 2
    per_slab = cols // LANES
    for part in range(2):
        for m in range(per_slab):
            start = 16 * part + per_slab * step + m
            spectra_ref[pl.ds(start, bins, stride=32), :] = spectra[
                part * bins : (part + 1) * bins, m * LANES : (m + 1) * LANES
            ]

    @pl.when(step == pl.num_programs(0) - 1)
    def _():
        left_lane = lax.broadcasted_iota(jnp.int32, (8, LANES), 1) < LANES // 2
        alive = alive_ref[...]

        def some(j, carry):
            hc, hs = (high_c[j], high_s[j])
            pair = []
            for i in range(8):
                lc, ls = (low_c[i], low_s[i])
                real = (hc * lc - hs * ls).astype(BF16)
                imag = (hc * ls + hs * lc).astype(BF16)
                at = pl.multiple_of((8 * j + i) * 32, 32)
                left = jnp.concatenate(
                    [spectra_ref[pl.ds(at, 16), :], spectra_ref[pl.ds(at + 16, 16), :]], axis=1
                ).astype(BF16)
                stack = jnp.dot(left, jnp.concatenate([real, imag], axis=0), preferred_element_type=F32)
                product = stack[:8] * stack[8:]
                pair.append(product + half_turn_small(product))
                if i % 2 == 1:
                    even, odd = pair
                    even = even + pltpu.roll(even, LANES // 2, 1)
                    odd = odd + pltpu.roll(odd, LANES // 2, 1)
                    pair = []
                    where_to = pl.multiple_of((4 * j + i // 2) * LANES, LANES)
                    image_ref[:, pl.ds(where_to, LANES)] = alive * jnp.where(left_lane, even, odd)
            return carry

        def half_turn_small(x):
            return pltpu.roll(x, 4, 0)

        lax.fori_loop(0, bins // 8, some, 0)
        out_ref[...] = image_ref[:per_slab, :].astype(BF16)


def images_of(wavefields, partner, neighbour, prepared, angles):
    two, four, shots, rows, cols = wavefields.shape
    bins = rows // 2
    per_slab = cols // rows
    ext = rows + 2 * HALF
    tall = rows + 4 * HALF
    one, both = row_tables(rows)
    xx, xx_across = column_tables(2)
    x, x_across = column_tables(1)
    depth = depth_table(rows, bins)
    depth_top = depth.astype(jnp.bfloat16)
    depth_low = (depth - depth_top.astype(np.float32)).astype(jnp.bfloat16)
    depth = np.concatenate([depth_top, depth_top, depth_low], axis=1)
    tables = [jnp.asarray(t, dtype=BF16) for t in (one, both, xx, xx_across, x, x_across, depth)]
    args = [wavefields, partner, neighbour, *prepared, *tables]
    out_shape = (per_slab, bins * angles)
    scratch = [
        pltpu.VMEM((5, 2 * HALF, cols), F32),
        pltpu.VMEM((2 * tall, cols), BF16),
        pltpu.VMEM((2 * tall, cols), BF16),
        pltpu.VMEM((2 * tall, cols), F32),
        pltpu.VMEM((2 * tall, cols), F32),
        pltpu.VMEM((2 * tall, cols), F32),
        pltpu.VMEM((2, ext, cols), F32),
        pltpu.VMEM((3 * rows, cols), BF16),
        pltpu.VMEM((32 * bins, LANES), F32),
        pltpu.VMEM((8, bins * angles), F32),
    ]
    return pl.pallas_call(
        main_kernel,
        grid=(two * shots,),
        in_specs=[VMEM_WHOLE] * len(args),
        out_specs=VMEM_WHOLE,
        out_shape=pltpu.VMEM(out_shape, BF16),
        scratch_shapes=scratch,
        compiler_params=pltpu.CompilerParams(vmem_limit_bytes=24 << 20),
        name="images",
    )(*in_vmem(*args))


def pick_kernel(loc_ref, own_ref, other_ref, out_ref, *, per_slab):
    slab = lax.axis_index(SLAB)
    core = lax.axis_index("core")
    far, near = (lax.axis_size("far"), lax.axis_size("near"))
    count = out_ref.shape[0]
    per_row = LANES // count
    loc = loc_ref[pl.ds(slab // per_row, 1), :]
    loc = pltpu.roll(loc, (LANES - (slab % per_row) * count) % LANES, 1)[:, :count]
    held = own_ref.shape[0]
    owner = loc // per_slab
    chip = owner // 2
    index = ((chip % near) * far + chip // near) * per_slab + loc % per_slab
    mine = owner % 2 == core
    row = lax.broadcasted_iota(jnp.int32, (held, count), 0)
    hit = row == index
    own_hot = jnp.where(hit & mine, 1.0, 0.0).astype(BF16)
    other_hot = jnp.where(hit & jnp.logical_not(mine), 1.0, 0.0).astype(BF16)

    def choose(hot, ref):
        return lax.dot_general(hot, ref[...], (((0,), (0,)), ((), ())), preferred_element_type=F32)

    out_ref[...] = choose(own_hot, own_ref) + choose(other_hot, other_ref)


def pick(loc_patch, own, other, count, per_slab):
    width = own.shape[1]
    return pl.pallas_call(
        lambda *refs: pick_kernel(*refs, per_slab=per_slab),
        in_specs=[VMEM_WHOLE] * 3,
        out_shape=jax.ShapeDtypeStruct((count, width), F32),
        compiler_params=pltpu.CompilerParams(vmem_limit_bytes=8 << 20),
        name="pick",
    )(*in_vmem(loc_patch.reshape(-1, LANES), own, other))


def per_device(
    wavefields, courant, epsilon, anisotropy_delta, tilt_angle, loc_patch, slab_counts, angle_table
):
    slabs = lax.axis_size(SLAB)
    per_slab = wavefields.shape[4] // wavefields.shape[3]
    params = (courant, epsilon, anisotropy_delta, tilt_angle)
    to_partner, to_neighbour = pack(wavefields, params)
    partner = lax.ppermute(to_partner, "core", [(0, 1), (1, 0)])
    pairs = [(i, i + 1) for i in range(1, slabs - 1, 2)]
    neighbour = lax.ppermute(to_neighbour, SLAB, pairs + [(j, i) for i, j in pairs])
    prepared = prepare(params, slab_counts, angle_table)
    images = images_of(wavefields, partner, neighbour, prepared, angle_table.shape[0])
    own = lax.all_gather(lax.all_gather(images, "far", tiled=True), "near", tiled=True)
    other = lax.ppermute(own, "core", [(0, 1), (1, 0)])
    return pick(loc_patch, own, other, loc_patch.shape[0] // slabs, per_slab)


def solution(mesh):
    chips = mesh.shape["slab"] // 2
    near = 4 if chips % 4 == 0 else 1
    shape = (mesh.shape["groups"], chips // near, near, 2)
    finer = Mesh(mesh.devices.reshape(shape), GROUPS_SLAB)
    in_specs = (
        P(None, None, "groups", SLAB, None),
        P(SLAB, None),
        P(SLAB, None),
        P(SLAB, None),
        P(SLAB, None),
        P(),
        P(),
        P(),
    )
    out_specs = P(GROUPS_SLAB, None)
    return jax.shard_map(
        per_device, mesh=finer, in_specs=in_specs, out_specs=out_specs, check_vma=False
    )
```

```python
import math

import jax
import jax.numpy as jnp
import numpy as np
from jax import lax
from jax.experimental import pallas as pl
from jax.experimental.pallas import tpu as pltpu
from jax.sharding import Mesh
from jax.sharding import PartitionSpec as P

SLAB = ("chip", "core")
GROUPS_SLAB = ("groups", "chip", "core")
LANES = 128
HALF = 4
PITCH = 40
FAR, NEAR = ((0, 3, 6), (0, 1, 2))
SECOND = (-14336.0, 8064.0, -1008.0, 128.0, -9.0)
SECOND_REST = 14.0
SECOND_UNIT = 5040.0
FIRST = (672.0, -168.0, 32.0, -3.0)
FIRST_UNIT = 840.0
BF16 = jnp.bfloat16
F32 = jnp.float32
VMEM_WHOLE = pl.BlockSpec(memory_space=pltpu.VMEM)


def in_vmem(*arrays):
    return [pltpu.with_memory_space_constraint(a, pltpu.VMEM) for a in arrays]


def weight(kind, offset):
    if abs(offset) > HALF:
        return 0.0
    if kind == 2:
        return SECOND[abs(offset)]
    if offset == 0:
        return 0.0
    return FIRST[abs(offset) - 1] * (1.0 if offset > 0 else -1.0)


def band(kind, outputs, inputs):
    table = np.zeros((len(outputs), len(inputs)), np.float32)
    for i, o in enumerate(outputs):
        for j, n in enumerate(inputs):
            if o is not None and n is not None:
                table[i, j] = weight(kind, n - o)
    return table


def row_tables(rows):
    own = list(range(rows))
    inner = list(range(-HALF, 0)) + list(range(rows, rows + HALF))
    outer = list(range(-2 * HALF, -HALF)) + list(range(rows + HALF, rows + 2 * HALF))
    pad = [None] * 8
    first_in = own + inner + outer
    first_out = own + inner + pad
    second_in = own + inner + pad
    one = np.concatenate([band(2, first_out, first_in), band(1, first_out, first_in)])
    two = np.concatenate([band(2, own, second_in), band(1, own, second_in)])
    return one, two


def column_tables(kind):
    block = list(range(2 * LANES))
    inside = band(kind, block, block).T
    across = np.zeros((2 * LANES, 2 * LANES), np.float32)
    for i in range(2 * LANES):
        for o in range(2 * LANES):
            if (i < LANES) != (o < LANES):
                across[i, o] = weight(kind, i - o)
    return inside, across


def depth_table(patch, bins):
    k = np.arange(bins)[:, None]
    z = np.arange(patch)[None, :]
    phase = (2.0 * math.pi / patch * np.mod(k * z, patch)).astype(np.float32)
    table = np.concatenate([np.cos(phase), -np.sin(phase)]).astype(np.float32) * np.float32(1.0 / math.sqrt(patch))
    return table.astype(np.float32)


def quarter_turns(quarter, cosine, sine):
    odd = (quarter & 1) == 1
    c = jnp.where(odd, sine, cosine)
    s = jnp.where(odd, cosine, sine)
    c = jnp.where(((quarter + 1) & 2) == 2, -c, c)
    s = jnp.where((quarter & 2) == 2, -s, s)
    return c, s


def small_cos_sin(y):
    y2 = y * y
    s = y * (1.0 + y2 * (-1.6666654611e-1 + y2 * (8.3321608736e-3 + y2 * -1.9515295891e-4)))
    c = 1.0 - 0.5 * y2 + y2 * y2 * (4.166664568298827e-2 + y2 * (-1.388731625493765e-3 + y2 * 2.443315711809948e-5))
    return c, s


def double_angle(theta):
    n = jnp.floor(theta * (4.0 / math.pi) + 0.5)
    y = 2.0 * theta - n * 1.5703125
    y = y - n * 4.837512969970703e-4
    y = y - n * 7.54978995489188216e-8
    c, s = small_cos_sin(y)
    return quarter_turns(n.astype(jnp.int32), c, s)


def pack_kernel(
    w_top, w_bot, c_top, c_bot, e_top, e_bot, d_top, d_bot, t_top, t_bot, partner_ref, neighbour_ref
):
    low = lax.broadcasted_iota(jnp.int32, (8, w_top.shape[-1]), 0) < HALF

    def half_turn(x):
        return pltpu.roll(x, HALF, 0)

    def emit(out, wave, params, upward):
        def join(a, b):
            return jnp.where(low, half_turn(a), b) if upward else jnp.where(low, a, half_turn(b))

        groups = []
        for w in range(wave.shape[0]):
            for s in range(wave.shape[2]):
                groups.append(wave[w, 0, s])
                groups.append(wave[w, 1, s])
                groups.append(join(wave[w, 2, s], wave[w, 3, s]))
        courant, eps, delta, tilt = (p[...] for p in params)
        high = tilt.astype(BF16).astype(F32)
        groups += [join(courant, eps), join(delta, high), tilt - high]
        groups.append(groups[-1])
        for g in range(0, len(groups), 2):
            out[8 * g : 8 * g + 16, :] = jnp.concatenate(groups[g : g + 2], axis=0).astype(BF16)

    tops = (w_top, (c_top, e_top, d_top, t_top))
    bottoms = (w_bot, (c_bot, e_bot, d_bot, t_bot))
    first = lax.axis_index("core") == 0

    @pl.when(first)
    def _():
        emit(partner_ref, *bottoms, True)
        emit(neighbour_ref, *tops, False)

    @pl.when(jnp.logical_not(first))
    def _():
        emit(partner_ref, *tops, False)
        emit(neighbour_ref, *bottoms, True)


def pack(wavefields, params):
    two, four, shots, rows, cols = wavefields.shape
    last = rows // 8 - 1
    groups = 2 * shots * 3 + 4
    wave_block = (two, four, shots, 8, cols)
    specs = [
        pl.BlockSpec(wave_block, lambda i: (0, 0, 0, 0, 0)),
        pl.BlockSpec(wave_block, lambda i: (0, 0, 0, last, 0)),
    ]
    args = [wavefields, wavefields]
    for p in params:
        specs += [pl.BlockSpec((8, cols), lambda i: (0, 0)), pl.BlockSpec((8, cols), lambda i: (last, 0))]
        args += [p, p]
    out = pltpu.VMEM((8 * groups, cols), BF16)
    return pl.pallas_call(
        pack_kernel,
        grid=(1,),
        in_specs=specs,
        out_specs=[VMEM_WHOLE] * 2,
        out_shape=[out, out],
        compiler_params=pltpu.CompilerParams(vmem_limit_bytes=8 << 20),
        name="pack",
    )(*(pltpu.with_memory_space_constraint(a, pltpu.HBM) for a in args))


def coefficients(courant, eps, delta, tilt):
    cosine, sine = double_angle(tilt)
    scaled = courant * (1.0 / SECOND_UNIT)
    return (
        0.5 + 0.5 * cosine,
        sine * (SECOND_UNIT / (FIRST_UNIT * FIRST_UNIT)),
        scaled * (1.0 + 2.0 * eps),
        scaled * jnp.sqrt(1.0 + 2.0 * delta),
        scaled,
    )


def prepare_kernel(
    counts_ref, courant_ref, eps_ref, delta_ref, tilt_ref, angle_ref,
    mix_ref, twist_ref, a_ref, b_ref, c_ref, low_c, low_s, high_c, high_s, alive_ref,
):
    for r in range(0, courant_ref.shape[0], 8):
        at = slice(r, r + 8)
        values = coefficients(courant_ref[at, :], eps_ref[at, :], delta_ref[at, :], tilt_ref[at, :])
        for ref, value in zip((mix_ref, twist_ref, a_ref, b_ref, c_ref), values, strict=True):
            ref[at, :] = value

    right_half = lax.broadcasted_iota(jnp.int32, (LANES, LANES), 1) >= LANES // 2
    angles = jnp.concatenate([angle_ref[...], angle_ref[...]], axis=1)
    lateral = lax.broadcasted_iota(jnp.int32, (LANES, LANES), 0)
    modulus = 16 * LANES
    turn = (lateral * angles) & (modulus - 1)
    quarter = (turn + modulus // 8) >> int(math.log2(modulus // 4))
    rest = turn - quarter * (modulus // 4)
    c1, s1 = small_cos_sin(rest.astype(F32) * (2.0 * math.pi / modulus))
    c1, s1 = quarter_turns(quarter, c1, s1)

    def times(x, y):
        return (x[0] * y[0] - x[1] * y[1], x[0] * y[1] + x[1] * y[0])

    value = (jnp.ones_like(c1), jnp.zeros_like(c1))
    for j in range(8):
        low_c[j], low_s[j] = value
        value = (c1, s1) if j == 0 else times(value, (c1, s1))
    eighth = value
    scale = 1.0 / math.sqrt(LANES)
    value = (jnp.where(right_half, 0.0, scale), jnp.where(right_half, scale, 0.0))
    for j in range(8):
        high_c[j], high_s[j] = value
        value = times(value, eighth)
    live = lax.broadcasted_iota(jnp.int32, (8, LANES), 0) < counts_ref[lax.axis_index(SLAB)]
    alive_ref[...] = jnp.where(live, 1.0, 0.0)


def prepare(params, slab_counts, angle_table):
    rows, cols = params[0].shape
    field = pltpu.VMEM((rows, cols), F32)
    table = pltpu.VMEM((8, LANES, LANES), F32)
    return pl.pallas_call(
        prepare_kernel,
        in_specs=[pl.BlockSpec(memory_space=pltpu.SMEM)] + [VMEM_WHOLE] * 5,
        out_specs=[VMEM_WHOLE] * 10,
        out_shape=[field] * 5 + [table] * 4 + [pltpu.VMEM((8, LANES), F32)],
        compiler_params=pltpu.CompilerParams(vmem_limit_bytes=8 << 20),
        name="prepare",
    )(slab_counts, *in_vmem(*params, angle_table.reshape(1, -1)))


def main_kernel(
    wave_ref, partner_ref, neighbour_ref, mix_ref, twist_ref, a_ref, b_ref, c_ref,
    low_c, low_s, high_c, high_s, alive_ref,
    one_ref, two_ref, xx_ref, xx_across_ref, x_ref, x_across_ref, depth_ref,
    out_ref,
    edge_ref, field_ref, slope_ref, row_ref, xx_out, xz_out, next_ref, split_ref, spectra_ref, image_ref,
):
    step = pl.program_id(0)
    shots = wave_ref.shape[2]
    rows, cols = mix_ref.shape
    ext = rows + 2 * HALF
    tall = rows + 4 * HALF
    low = lax.broadcasted_iota(jnp.int32, (8, cols), 0) < HALF
    first = lax.axis_index("core") == 0

    def half_turn(x):
        return pltpu.roll(x, HALF, 0)

    def group(g):
        at = pl.ds(g if isinstance(g, int) else pl.multiple_of(g, 8), 8)
        a, b = (partner_ref[at, :].astype(F32), neighbour_ref[at, :].astype(F32))
        return jnp.where(first, b, a), jnp.where(first, a, b)

    @pl.when(step == 0)
    def _():
        start = 8 * 3 * 2 * shots

        def first_halves(g):
            u, d = group(start + 8 * g)
            return jnp.where(low, u, half_turn(d))

        def second_halves(g):
            u, d = group(start + 8 * g)
            return jnp.where(low, half_turn(u), d)

        values = coefficients(
            first_halves(0), second_halves(0), first_halves(1), second_halves(1) + first_halves(2)
        )
        for i, value in enumerate(values):
            edge_ref[i] = value

    bins = rows // 2
    per_slab = cols // LANES

    def along_columns(out, source, inside, across):
        n = source.shape[0]
        out[:n, LANES : 3 * LANES] = jnp.dot(
            source[:, LANES : 3 * LANES], across[...], preferred_element_type=F32
        )
        left = jnp.dot(source[:, : 2 * LANES], inside[...], preferred_element_type=F32)
        out[:n, :LANES] = left[:, :LANES]
        out[:n, LANES : 2 * LANES] += left[:, LANES:]
        right = jnp.dot(source[:, 2 * LANES :], inside[...], preferred_element_type=F32)
        out[:n, 2 * LANES : 3 * LANES] += right[:, :LANES]
        out[:n, 3 * LANES :] = right[:, LANES:]

    def coefficient(i, r):
        if r < rows:
            return (mix_ref, twist_ref, a_ref, b_ref, c_ref)[i][r : r + 8, :]
        return edge_ref[i]

    class Item:
        def __init__(self, shot):
            self.shot = shot
            self.field, self.slope, self.zz, self.xx, self.xz, self.next, self.split = (
                ref.at[shot]
                for ref in (field_ref, slope_ref, row_ref, xx_out, xz_out, next_ref, split_ref)
            )

        def load(self):
            base = 8 * 3 * (step * shots + self.shot)
            self.halo = []
            for f in range(2):
                u, d = group(base + 8 * f)
                inner = jnp.where(low, half_turn(u), half_turn(d))
                outer = jnp.where(low, u, d)
                self.halo.append(inner)
                self.field[f * tall : f * tall + rows, :] = wave_ref[step, f, self.shot].astype(BF16)
                self.field[f * tall + rows : (f + 1) * tall, :] = jnp.concatenate(
                    [inner, outer], axis=0
                ).astype(BF16)
            u, d = group(base + 16)
            self.halo.append(jnp.where(low, u, half_turn(d)))
            self.halo.append(jnp.where(low, half_turn(u), d))

        def derive(self, table, count):
            for f in range(2):
                source = self.field[f * tall : (f + 1) * tall, :]
                product = jnp.dot(table[count:, :], source, preferred_element_type=F32)
                self.slope[f * count : (f + 1) * count, :] = product.astype(BF16)
                self.zz[f * tall : f * tall + count, :] = jnp.dot(
                    table[:count, :], source, preferred_element_type=F32
                )
            along_columns(self.xx, self.field[...], xx_ref, xx_across_ref)
            along_columns(self.xz, self.slope[: 2 * count, :], x_ref, x_across_ref)

        def pieces(self, f, r, count, value):
            at = slice(f * tall + r, f * tall + r + 8)
            zz = self.zz[at, :]
            xx = self.xx[at, :]
            xz = self.xz[f * count + r : f * count + r + 8, :]
            mix, twist = (coefficient(i, r) for i in range(2))
            turn = mix * (xx - zz) - twist * xz
            rest = SECOND_REST * value
            return (zz + turn) - rest if f == 0 else (xx - turn) - rest

        def first(self):
            for r in range(0, ext, 8):
                at = slice(r, r + 8)
                if r < rows:
                    p, q, p0, q0 = (wave_ref[step, f, self.shot, at, :] for f in range(4))
                else:
                    p, q, p0, q0 = self.halo
                across = self.pieces(0, r, tall, p)
                along = self.pieces(1, r, tall, q)
                a, b, c = (coefficient(i, r) for i in range(2, 5))
                self.next[0, at, :] = (2.0 * p - p0) + (a * across + b * along)
                self.next[1, at, :] = (2.0 * q - q0) + (b * across + c * along)

        def turn_over(self):
            for f in range(2):
                self.field[f * tall : f * tall + rows, :] = self.next[f, :rows, :].astype(BF16)
                edge = self.next[f, rows:ext, :]
                self.field[f * tall + rows : (f + 1) * tall, :] = jnp.concatenate(
                    [edge, jnp.zeros_like(edge)], axis=0
                ).astype(BF16)

        def second(self):
            for r in range(0, rows, 16):
                parts = []
                for h in (r, r + 8):
                    at = slice(h, h + 8)
                    p, q = (self.next[0, at, :], self.next[1, at, :])
                    across = self.pieces(0, h, rows, p)
                    along = self.pieces(1, h, rows, q)
                    parts.append(
                        (2.0 * p - wave_ref[step, 0, self.shot, at, :])
                        + (a_ref[at, :] * across + b_ref[at, :] * along)
                    )
                value = jnp.concatenate(parts, axis=0)
                top = value.astype(BF16)
                self.split[r : r + 16, :] = top
                self.split[rows + r : rows + r + 16, :] = (value - top.astype(F32)).astype(BF16)
                self.split[2 * rows + r : 2 * rows + r + 16, :] = top

        def transform(self):
            spectra = jnp.dot(depth_ref[...], self.split[...], preferred_element_type=F32)
            for part in range(2):
                for m in range(per_slab):
                    start = 16 * part + per_slab * (step * shots + self.shot) + m
                    spectra_ref[pl.ds(start, bins, stride=PITCH), :] = spectra[
                        part * bins : (part + 1) * bins, m * LANES : (m + 1) * LANES
                    ]

    items = [Item(shot) for shot in range(shots)]
    for item in items:
        item.load()
        item.derive(one_ref, tall)
    for item in items:
        item.first()
        item.turn_over()
        item.derive(two_ref, rows)
    for item in items:
        item.second()
        item.transform()

    @pl.when(step == pl.num_programs(0) - 1)
    def _():
        left_lane = lax.broadcasted_iota(jnp.int32, (8, LANES), 1) < LANES // 2
        alive = alive_ref[...]

        def some(j, carry):
            hc, hs = (high_c[j], high_s[j])
            pair = []
            for i in range(8):
                lc, ls = (low_c[i], low_s[i])
                real = (hc * lc - hs * ls).astype(BF16)
                imag = (hc * ls + hs * lc).astype(BF16)
                at = pl.multiple_of((8 * j + i) * PITCH, 8)
                left = jnp.concatenate(
                    [spectra_ref[pl.ds(at, 16), :], spectra_ref[pl.ds(at + 16, 16), :]], axis=1
                ).astype(BF16)
                stack = jnp.dot(left, jnp.concatenate([real, imag], axis=0), preferred_element_type=F32)
                product = stack[:8] * stack[8:]
                pair.append(product + half_turn_small(product))
                if i % 2 == 1:
                    even, odd = pair
                    even = even + pltpu.roll(even, LANES // 2, 1)
                    odd = odd + pltpu.roll(odd, LANES // 2, 1)
                    pair = []
                    where_to = pl.multiple_of((4 * j + i // 2) * LANES, LANES)
                    image_ref[:, pl.ds(where_to, LANES)] = alive * jnp.where(left_lane, even, odd)
            return carry

        def half_turn_small(x):
            return pltpu.roll(x, 4, 0)

        lax.fori_loop(0, bins // 8, some, 0)
        out_ref[...] = image_ref[:per_slab, :].astype(BF16)


def images_of(wavefields, partner, neighbour, prepared, angles):
    two, four, shots, rows, cols = wavefields.shape
    bins = rows // 2
    per_slab = cols // rows
    ext = rows + 2 * HALF
    tall = rows + 4 * HALF
    one, both = row_tables(rows)
    xx, xx_across = column_tables(2)
    x, x_across = column_tables(1)
    depth = depth_table(rows, bins)
    depth_top = depth.astype(jnp.bfloat16)
    depth_low = (depth - depth_top.astype(np.float32)).astype(jnp.bfloat16)
    depth = np.concatenate([depth_top, depth_top, depth_low], axis=1)
    tables = [jnp.asarray(t, dtype=BF16) for t in (one, both, xx, xx_across, x, x_across, depth)]
    args = [wavefields, partner, neighbour, *prepared, *tables]
    out_shape = (per_slab, bins * angles)
    scratch = [
        pltpu.VMEM((5, 2 * HALF, cols), F32),
        pltpu.VMEM((shots, 2 * tall, cols), BF16),
        pltpu.VMEM((shots, 2 * tall, cols), BF16),
        pltpu.VMEM((shots, 2 * tall, cols), F32),
        pltpu.VMEM((shots, 2 * tall, cols), F32),
        pltpu.VMEM((shots, 2 * tall, cols), F32),
        pltpu.VMEM((shots, 2, ext, cols), F32),
        pltpu.VMEM((shots, 3 * rows, cols), BF16),
        pltpu.VMEM((PITCH * bins, LANES), F32),
        pltpu.VMEM((8, bins * angles), F32),
    ]
    return pl.pallas_call(
        main_kernel,
        grid=(two,),
        in_specs=[VMEM_WHOLE] * len(args),
        out_specs=VMEM_WHOLE,
        out_shape=pltpu.VMEM(out_shape, BF16),
        scratch_shapes=scratch,
        compiler_params=pltpu.CompilerParams(vmem_limit_bytes=32 << 20),
        name="images",
    )(*in_vmem(*args))


def pick_kernel(loc_ref, own_ref, other_ref, out_ref, *, per_slab):
    slab = lax.axis_index(SLAB)
    chip, core = (lax.axis_index("chip"), lax.axis_index("core"))
    chips = lax.axis_size("chip")
    count = out_ref.shape[0]
    per_row = LANES // count
    loc = loc_ref[pl.ds(slab // per_row, 1), :]
    loc = pltpu.roll(loc, (LANES - (slab % per_row) * count) % LANES, 1)[:, :count]
    held = own_ref.shape[0]
    owner = loc // per_slab
    ahead = lax.rem(owner // 2 - chip + chips, chips)
    up = ahead <= chips // 2
    hops = jnp.where(up, ahead, chips - ahead)
    holder = jnp.where(up, 1, 0)
    place = (hops % len(NEAR)) * len(FAR) + hops // len(NEAR)
    index = (2 * place + jnp.where(owner % 2 == holder, 0, 1)) * per_slab + loc % per_slab
    mine = holder == core
    row = lax.broadcasted_iota(jnp.int32, (held, count), 0)
    hit = row == index
    own_hot = jnp.where(hit & mine, 1.0, 0.0).astype(BF16)
    other_hot = jnp.where(hit & jnp.logical_not(mine), 1.0, 0.0).astype(BF16)

    def choose(hot, ref):
        return lax.dot_general(hot, ref[...], (((0,), (0,)), ((), ())), preferred_element_type=F32)

    out_ref[...] = choose(own_hot, own_ref) + choose(other_hot, other_ref)


def pick(loc_patch, own, other, count, per_slab):
    width = own.shape[1]
    return pl.pallas_call(
        lambda *refs: pick_kernel(*refs, per_slab=per_slab),
        in_specs=[VMEM_WHOLE] * 3,
        out_shape=jax.ShapeDtypeStruct((count, width), F32),
        compiler_params=pltpu.CompilerParams(vmem_limit_bytes=8 << 20),
        name="pick",
    )(*in_vmem(loc_patch.reshape(-1, LANES), own, other))


def swap_cores(array):
    return lax.ppermute(array, "core", [(0, 1), (1, 0)])


def onward(array, hops):
    chips = lax.axis_size("chip")
    pairs = [(2 * i, 2 * ((i + hops) % chips)) for i in range(chips)]
    pairs += [(2 * i + 1, 2 * ((i - hops) % chips) + 1) for i in range(chips)]
    return lax.ppermute(array, SLAB, pairs)


def spread(images):
    held = jnp.concatenate([images, swap_cores(images)])
    for hops in (FAR, NEAR):
        held = jnp.concatenate([held] + [onward(held, h) for h in hops[1:]])
    return held


def per_device(
    wavefields, courant, epsilon, anisotropy_delta, tilt_angle, loc_patch, slab_counts, angle_table
):
    slabs = lax.axis_size(SLAB)
    assert FAR[-1] + NEAR[-1] >= slabs // 4
    per_slab = wavefields.shape[4] // wavefields.shape[3]
    params = (courant, epsilon, anisotropy_delta, tilt_angle)
    to_partner, to_neighbour = pack(wavefields, params)
    partner = swap_cores(to_partner)
    pairs = [(i, i + 1) for i in range(1, slabs - 1, 2)]
    neighbour = lax.ppermute(to_neighbour, SLAB, pairs + [(j, i) for i, j in pairs])
    prepared = prepare(params, slab_counts, angle_table)
    images = images_of(wavefields, partner, neighbour, prepared, angle_table.shape[0])
    own = spread(images)
    return pick(loc_patch, own, swap_cores(own), loc_patch.shape[0] // slabs, per_slab)


def solution(mesh):
    shape = (mesh.shape["groups"], mesh.shape["slab"] // 2, 2)
    finer = Mesh(mesh.devices.reshape(shape), GROUPS_SLAB)
    in_specs = (
        P(None, None, "groups", SLAB, None),
        P(SLAB, None),
        P(SLAB, None),
        P(SLAB, None),
        P(SLAB, None),
        P(),
        P(),
        P(),
    )
    out_specs = P(GROUPS_SLAB, None)
    return jax.shard_map(
        per_device, mesh=finer, in_specs=in_specs, out_specs=out_specs, check_vma=False
    )
```

```python
import math

import jax
import jax.numpy as jnp
import numpy as np
from jax import lax
from jax.experimental import pallas as pl
from jax.experimental.pallas import tpu as pltpu
from jax.sharding import Mesh
from jax.sharding import PartitionSpec as P

SLAB = ("chip", "core")
GROUPS_SLAB = ("groups", "chip", "core")
LANES = 128
HALF = 4
PITCH = 40
FAR, NEAR = ((0, 3, 6), (0, 1, 2))
SECOND = (-14336.0, 8064.0, -1008.0, 128.0, -9.0)
SECOND_REST = 14.0
SECOND_UNIT = 5040.0
FIRST = (672.0, -168.0, 32.0, -3.0)
FIRST_UNIT = 840.0
BF16 = jnp.bfloat16
F32 = jnp.float32
VMEM_WHOLE = pl.BlockSpec(memory_space=pltpu.VMEM)


def in_vmem(*arrays):
    return [pltpu.with_memory_space_constraint(a, pltpu.VMEM) for a in arrays]


def weight(kind, offset):
    if abs(offset) > HALF:
        return 0.0
    if kind == 2:
        return SECOND[abs(offset)]
    if offset == 0:
        return 0.0
    return FIRST[abs(offset) - 1] * (1.0 if offset > 0 else -1.0)


def band(kind, outputs, inputs):
    table = np.zeros((len(outputs), len(inputs)), np.float32)
    for i, o in enumerate(outputs):
        for j, n in enumerate(inputs):
            if o is not None and n is not None:
                table[i, j] = weight(kind, n - o)
    return table


def row_tables(rows):
    own = list(range(rows))
    inner = list(range(-HALF, 0)) + list(range(rows, rows + HALF))
    outer = list(range(-2 * HALF, -HALF)) + list(range(rows + HALF, rows + 2 * HALF))
    pad = [None] * 8
    ends = own[:8] + own[-8:]
    edge_in = ends + inner + outer + own[8:16] + own[-16:-8]
    edge_out = ends + inner + pad
    second_in = own + inner + pad
    tables = ((own, own), (edge_out, edge_in), (own, second_in))
    return [np.concatenate([band(2, o, i), band(1, o, i)]) for o, i in tables]


def column_tables(kind):
    block = list(range(2 * LANES))
    inside = band(kind, block, block).T
    across = np.zeros((2 * LANES, 2 * LANES), np.float32)
    for i in range(2 * LANES):
        for o in range(2 * LANES):
            if (i < LANES) != (o < LANES):
                across[i, o] = weight(kind, i - o)
    return inside, across


def depth_table(patch, bins):
    k = np.arange(bins)[:, None]
    z = np.arange(patch)[None, :]
    phase = (2.0 * math.pi / patch * np.mod(k * z, patch)).astype(np.float32)
    table = np.concatenate([np.cos(phase), -np.sin(phase)]).astype(np.float32) * np.float32(1.0 / math.sqrt(patch))
    return table.astype(np.float32)


def quarter_turns(quarter, cosine, sine):
    odd = (quarter & 1) == 1
    c = jnp.where(odd, sine, cosine)
    s = jnp.where(odd, cosine, sine)
    c = jnp.where(((quarter + 1) & 2) == 2, -c, c)
    s = jnp.where((quarter & 2) == 2, -s, s)
    return c, s


def small_cos_sin(y):
    y2 = y * y
    s = y * (1.0 + y2 * (-1.6666654611e-1 + y2 * (8.3321608736e-3 + y2 * -1.9515295891e-4)))
    c = 1.0 - 0.5 * y2 + y2 * y2 * (4.166664568298827e-2 + y2 * (-1.388731625493765e-3 + y2 * 2.443315711809948e-5))
    return c, s


def double_angle(theta):
    n = jnp.floor(theta * (4.0 / math.pi) + 0.5)
    y = 2.0 * theta - n * 1.5703125
    y = y - n * 4.837512969970703e-4
    y = y - n * 7.54978995489188216e-8
    c, s = small_cos_sin(y)
    return quarter_turns(n.astype(jnp.int32), c, s)


def pack_kernel(
    w_top, w_bot, c_top, c_bot, e_top, e_bot, d_top, d_bot, t_top, t_bot, partner_ref, neighbour_ref
):
    low = lax.broadcasted_iota(jnp.int32, (8, w_top.shape[-1]), 0) < HALF

    def half_turn(x):
        return pltpu.roll(x, HALF, 0)

    def emit(out, wave, params, upward):
        def join(a, b):
            return jnp.where(low, half_turn(a), b) if upward else jnp.where(low, a, half_turn(b))

        groups = []
        for w in range(wave.shape[0]):
            for s in range(wave.shape[2]):
                groups.append(wave[w, 0, s])
                groups.append(wave[w, 1, s])
                groups.append(join(wave[w, 2, s], wave[w, 3, s]))
        courant, eps, delta, tilt = (p[...] for p in params)
        high = tilt.astype(BF16).astype(F32)
        groups += [join(courant, eps), join(delta, high), tilt - high]
        groups.append(groups[-1])
        for g in range(0, len(groups), 2):
            out[8 * g : 8 * g + 16, :] = jnp.concatenate(groups[g : g + 2], axis=0).astype(BF16)

    tops = (w_top, (c_top, e_top, d_top, t_top))
    bottoms = (w_bot, (c_bot, e_bot, d_bot, t_bot))
    first = lax.axis_index("core") == 0

    @pl.when(first)
    def _():
        emit(partner_ref, *bottoms, True)
        emit(neighbour_ref, *tops, False)

    @pl.when(jnp.logical_not(first))
    def _():
        emit(partner_ref, *tops, False)
        emit(neighbour_ref, *bottoms, True)


def pack(wavefields, params):
    two, four, shots, rows, cols = wavefields.shape
    last = rows // 8 - 1
    groups = 2 * shots * 3 + 4
    wave_block = (two, four, shots, 8, cols)
    specs = [
        pl.BlockSpec(wave_block, lambda i: (0, 0, 0, 0, 0)),
        pl.BlockSpec(wave_block, lambda i: (0, 0, 0, last, 0)),
    ]
    args = [wavefields, wavefields]
    for p in params:
        specs += [pl.BlockSpec((8, cols), lambda i: (0, 0)), pl.BlockSpec((8, cols), lambda i: (last, 0))]
        args += [p, p]
    out = pltpu.VMEM((8 * groups, cols), BF16)
    return pl.pallas_call(
        pack_kernel,
        grid=(1,),
        in_specs=specs,
        out_specs=[VMEM_WHOLE] * 2,
        out_shape=[out, out],
        compiler_params=pltpu.CompilerParams(vmem_limit_bytes=8 << 20),
        name="pack",
    )(*(pltpu.with_memory_space_constraint(a, pltpu.HBM) for a in args))


def coefficients(courant, eps, delta, tilt):
    cosine, sine = double_angle(tilt)
    scaled = courant * (1.0 / SECOND_UNIT)
    return (
        0.5 + 0.5 * cosine,
        sine * (SECOND_UNIT / (FIRST_UNIT * FIRST_UNIT)),
        scaled * (1.0 + 2.0 * eps),
        scaled * jnp.sqrt(1.0 + 2.0 * delta),
        scaled,
    )


def along_columns(out, source, inside, across):
    out[:, LANES : 3 * LANES] = jnp.dot(source[:, LANES : 3 * LANES], across[...], preferred_element_type=F32)
    left = jnp.dot(source[:, : 2 * LANES], inside[...], preferred_element_type=F32)
    out[:, :LANES] = left[:, :LANES]
    out[:, LANES : 2 * LANES] += left[:, LANES:]
    right = jnp.dot(source[:, 2 * LANES :], inside[...], preferred_element_type=F32)
    out[:, 2 * LANES : 3 * LANES] += right[:, :LANES]
    out[:, 3 * LANES :] = right[:, LANES:]


def derive(field, slope, zz, xx, xz, table, columns, fields):
    count = table.shape[0] // 2
    for f in range(2):
        source = field[f]
        product = jnp.dot(table[count:, :], source, preferred_element_type=F32)
        slope[f * count : (f + 1) * count, :] = product.astype(BF16)
        zz[f * count : (f + 1) * count, :] = jnp.dot(table[:count, :], source, preferred_element_type=F32)
    along_columns(xx, fields, columns[0], columns[1])
    along_columns(xz, slope[...], columns[2], columns[3])


def tilted(f, value, zz, xx, xz, mix, twist):
    turn = mix * (xx - zz) - twist * xz
    rest = SECOND_REST * value
    return (zz + turn) - rest if f == 0 else (xx - turn) - rest


def early_kernel(
    counts_ref, wave_ref, courant_ref, eps_ref, delta_ref, tilt_ref, angle_ref, own_ref,
    xx_ref, xx_across_ref, x_ref, x_across_ref,
    mix_ref, twist_ref, a_ref, b_ref, c_ref, low_c, low_s, high_c, high_s, alive_ref, next_ref,
    field_ref, slope_ref, zz_ref, xx_out, xz_out,
):
    rows, cols = courant_ref.shape
    wavefields, _, shots = wave_ref.shape[:3]
    columns = (xx_ref, xx_across_ref, x_ref, x_across_ref)
    items = [(w, s) for w in range(wavefields) for s in range(shots)]

    def matmuls(i):
        w, s = items[i]
        k = i % 2
        for f in range(2):
            field_ref[k, f * rows : (f + 1) * rows, :] = wave_ref[w, f, s].astype(BF16)
        parts = [field_ref.at[k, f * rows : (f + 1) * rows, :][...] for f in range(2)]
        derive(
            parts, slope_ref.at[k], zz_ref.at[k], xx_out.at[k], xz_out.at[k], own_ref, columns,
            field_ref.at[k][...],
        )

    def advance(i):
        w, s = items[i]
        k = i % 2
        for r in range(8, rows - 8, 8):
            at = slice(r, r + 8)
            p, q, p0, q0 = (wave_ref[w, f, s, at, :] for f in range(4))
            mix, twist = (mix_ref[at, :], twist_ref[at, :])

            def operator(f, value):
                here = slice(f * rows + r, f * rows + r + 8)
                return tilted(f, value, zz_ref[k, here, :], xx_out[k, here, :], xz_out[k, here, :], mix, twist)

            across, along = (operator(0, p), operator(1, q))
            a, b, c = (a_ref[at, :], b_ref[at, :], c_ref[at, :])
            next_ref[i, 0, at, :] = (2.0 * p - p0) + (a * across + b * along)
            next_ref[i, 1, at, :] = (2.0 * q - q0) + (b * across + c * along)

    matmuls(0)
    for r in range(0, rows, 8):
        at = slice(r, r + 8)
        values = coefficients(courant_ref[at, :], eps_ref[at, :], delta_ref[at, :], tilt_ref[at, :])
        for ref, value in zip((mix_ref, twist_ref, a_ref, b_ref, c_ref), values, strict=True):
            ref[at, :] = value
    for i in range(1, len(items)):
        matmuls(i)
        advance(i - 1)
    slant_factors(angle_ref, low_c, low_s, high_c, high_s)
    advance(len(items) - 1)
    live = lax.broadcasted_iota(jnp.int32, (8, LANES), 0) < counts_ref[lax.axis_index(SLAB)]
    alive_ref[...] = jnp.where(live, 1.0, 0.0)


def slant_factors(angle_ref, low_c, low_s, high_c, high_s):
    right_half = lax.broadcasted_iota(jnp.int32, (LANES, LANES), 1) >= LANES // 2
    angles = jnp.concatenate([angle_ref[...], angle_ref[...]], axis=1)
    lateral = lax.broadcasted_iota(jnp.int32, (LANES, LANES), 0)
    modulus = 16 * LANES
    turn = (lateral * angles) & (modulus - 1)
    quarter = (turn + modulus // 8) >> int(math.log2(modulus // 4))
    rest = turn - quarter * (modulus // 4)
    c1, s1 = small_cos_sin(rest.astype(F32) * (2.0 * math.pi / modulus))
    c1, s1 = quarter_turns(quarter, c1, s1)

    def times(x, y):
        return (x[0] * y[0] - x[1] * y[1], x[0] * y[1] + x[1] * y[0])

    value = (jnp.ones_like(c1), jnp.zeros_like(c1))
    for j in range(8):
        low_c[j], low_s[j] = value
        value = (c1, s1) if j == 0 else times(value, (c1, s1))
    eighth = value
    scale = 1.0 / math.sqrt(LANES)
    value = (jnp.where(right_half, 0.0, scale), jnp.where(right_half, scale, 0.0))
    for j in range(8):
        high_c[j], high_s[j] = value
        value = times(value, eighth)


def late_kernel(
    wave_ref, partner_ref, neighbour_ref, mix_ref, twist_ref, a_ref, b_ref, c_ref,
    low_c, low_s, high_c, high_s, alive_ref, next_ref,
    edge_table_ref, two_ref, xx_ref, xx_across_ref, x_ref, x_across_ref, depth_ref,
    out_ref,
    edge_z, edge_x, edge_slope, edge_zz, edge_xx, edge_xz, edge_next,
    field_ref, slope_ref, zz_ref, xx_out, xz_out, split_ref, spectra_ref, image_ref,
):
    wavefields, _, shots, rows, cols = wave_ref.shape
    bins = rows // 2
    per_slab = cols // LANES
    columns = (xx_ref, xx_across_ref, x_ref, x_across_ref)
    items = [(w, s) for w in range(wavefields) for s in range(shots)]
    low = lax.broadcasted_iota(jnp.int32, (8, cols), 0) < HALF
    first = lax.axis_index("core") == 0
    coefficient_refs = (mix_ref, twist_ref, a_ref, b_ref, c_ref)

    def half_turn(x):
        return pltpu.roll(x, HALF, 0)

    def group(g):
        at = slice(8 * g, 8 * g + 8)
        a, b = (partner_ref[at, :].astype(F32), neighbour_ref[at, :].astype(F32))
        return jnp.where(first, b, a), jnp.where(first, a, b)

    def first_halves(g):
        u, d = group(g)
        return jnp.where(low, u, half_turn(d))

    def second_halves(g):
        u, d = group(g)
        return jnp.where(low, half_turn(u), d)

    tall = 32
    halos = []
    for i, (w, s) in enumerate(items):
        halo = []
        for f in range(2):
            u, d = group(3 * i + f)
            inner = jnp.where(low, half_turn(u), half_turn(d))
            outer = jnp.where(low, u, d)
            halo.append(inner)
            pieces = (
                wave_ref[w, f, s, 0:8, :], wave_ref[w, f, s, rows - 8 : rows, :], inner, outer,
                wave_ref[w, f, s, 8:16, :], wave_ref[w, f, s, rows - 16 : rows - 8, :],
            )
            for n in range(0, 6, 2):
                pair = jnp.concatenate(pieces[n : n + 2], axis=0).astype(BF16)
                edge_z[i, f, 8 * n : 8 * n + 16, :] = pair
                if n < 4:
                    at = (2 * i + f) * tall + 8 * n
                    edge_x[at : at + 16, :] = pair
        halo += [first_halves(3 * i + 2), second_halves(3 * i + 2)]
        halos.append(halo)
    for i in range(len(items)):
        for f in range(2):
            product = jnp.dot(edge_table_ref[...], edge_z[i, f], preferred_element_type=F32)
            at = (2 * i + f) * tall
            edge_zz[at : at + tall, :] = product[:tall]
            edge_slope[at : at + tall, :] = product[tall:].astype(BF16)
    along_columns(edge_xx, edge_x[...], xx_ref, xx_across_ref)
    along_columns(edge_xz, edge_slope[...], x_ref, x_across_ref)
    g = 3 * len(items)
    beyond = coefficients(
        first_halves(g), second_halves(g), first_halves(g + 1), second_halves(g + 1) + first_halves(g + 2)
    )

    def edge_advance(i):
        w, s = items[i]
        for n, r in enumerate((0, rows - 8, None)):
            if r is None:
                fields = halos[i]
                mix, twist, a, b, c = beyond
            else:
                at = slice(r, r + 8)
                fields = [wave_ref[w, f, s, at, :] for f in range(4)]
                mix, twist, a, b, c = (ref[at, :] for ref in coefficient_refs)
            p, q, p0, q0 = fields

            def operator(f, value):
                here = slice((2 * i + f) * tall + 8 * n, (2 * i + f) * tall + 8 * n + 8)
                return tilted(f, value, edge_zz[here, :], edge_xx[here, :], edge_xz[here, :], mix, twist)

            across, along = (operator(0, p), operator(1, q))
            edge_next[i, 0, 8 * n : 8 * n + 8, :] = (2.0 * p - p0) + (a * across + b * along)
            edge_next[i, 1, 8 * n : 8 * n + 8, :] = (2.0 * q - q0) + (b * across + c * along)

    def current(i, f, r):
        if r == 0:
            return edge_next[i, f, 0:8, :]
        if r == rows - 8:
            return edge_next[i, f, 8:16, :]
        return next_ref[i, f, r : r + 8, :]

    def matmuls(i):
        k = i % 2
        for f in range(2):
            for r in range(0, rows, 16):
                pair = jnp.concatenate([current(i, f, r), current(i, f, r + 8)], axis=0)
                pair = pair.astype(BF16)
                field_ref[k, f * rows + r : f * rows + r + 16, :] = pair
            edge = edge_next[i, f, 16:24, :]
            pair = jnp.concatenate([edge, jnp.zeros_like(edge)], axis=0).astype(BF16)
            field_ref[k, 2 * rows + 16 * f : 2 * rows + 16 * f + 16, :] = pair
        parts = [
            jnp.concatenate(
                [
                    field_ref[k, f * rows : (f + 1) * rows, :],
                    field_ref[k, 2 * rows + 16 * f : 2 * rows + 16 * f + 16, :],
                ],
                axis=0,
            )
            for f in range(2)
        ]
        derive(
            parts, slope_ref.at[k], zz_ref.at[k], xx_out.at[k], xz_out.at[k], two_ref, columns,
            field_ref[k, : 2 * rows, :],
        )

    def advance(i):
        w, s = items[i]
        k = i % 2
        for r in range(0, rows, 16):
            parts = []
            for h in (r, r + 8):
                at = slice(h, h + 8)
                mix, twist, a, b = (ref[at, :] for ref in coefficient_refs[:4])

                def operator(f, value):
                    here = slice(f * rows + h, f * rows + h + 8)
                    return tilted(
                        f, value, zz_ref[k, here, :], xx_out[k, here, :], xz_out[k, here, :], mix, twist
                    )

                p, q = (current(i, f, h) for f in range(2))
                across, along = (operator(0, p), operator(1, q))
                parts.append((2.0 * p - wave_ref[w, 0, s, at, :]) + (a * across + b * along))
            value = jnp.concatenate(parts, axis=0)
            top = value.astype(BF16)
            split_ref[k, r : r + 16, :] = top
            split_ref[k, rows + r : rows + r + 16, :] = (value - top.astype(F32)).astype(BF16)
            split_ref[k, 2 * rows + r : 2 * rows + r + 16, :] = top

    def transform(i):
        spectra = jnp.dot(depth_ref[...], split_ref[i % 2], preferred_element_type=F32)
        for part in range(2):
            for m in range(per_slab):
                start = 16 * part + per_slab * i + m
                spectra_ref[pl.ds(start, bins, stride=PITCH), :] = spectra[
                    part * bins : (part + 1) * bins, m * LANES : (m + 1) * LANES
                ]

    for i in range(len(items)):
        edge_advance(i)
    matmuls(0)
    for i in range(1, len(items)):
        matmuls(i)
        advance(i - 1)
        transform(i - 1)
    advance(len(items) - 1)
    transform(len(items) - 1)

    left_lane = lax.broadcasted_iota(jnp.int32, (8, LANES), 1) < LANES // 2
    alive = alive_ref[...]

    def some(j, carry):
        hc, hs = (high_c[j], high_s[j])
        pair = []
        for i in range(8):
            lc, ls = (low_c[i], low_s[i])
            real = (hc * lc - hs * ls).astype(BF16)
            imag = (hc * ls + hs * lc).astype(BF16)
            at = pl.multiple_of((8 * j + i) * PITCH, 8)
            left = jnp.concatenate(
                [spectra_ref[pl.ds(at, 16), :], spectra_ref[pl.ds(at + 16, 16), :]], axis=1
            ).astype(BF16)
            stack = jnp.dot(left, jnp.concatenate([real, imag], axis=0), preferred_element_type=F32)
            product = stack[:8] * stack[8:]
            pair.append(product + pltpu.roll(product, 4, 0))
            if i % 2 == 1:
                even, odd = pair
                even = even + pltpu.roll(even, LANES // 2, 1)
                odd = odd + pltpu.roll(odd, LANES // 2, 1)
                pair = []
                where_to = pl.multiple_of((4 * j + i // 2) * LANES, LANES)
                image_ref[:, pl.ds(where_to, LANES)] = alive * jnp.where(left_lane, even, odd)
        return carry

    lax.fori_loop(0, bins // 8, some, 0)
    out_ref[...] = image_ref[:per_slab, :].astype(BF16)


def column_operands():
    return [jnp.asarray(t, dtype=BF16) for kind in (2, 1) for t in column_tables(kind)]


def early(wavefields, params, slab_counts, angle_table):
    two, four, shots, rows, cols = wavefields.shape
    field = pltpu.VMEM((rows, cols), F32)
    table = pltpu.VMEM((8, LANES, LANES), F32)
    own = jnp.asarray(row_tables(rows)[0], dtype=BF16)
    args = [wavefields, *params, angle_table.reshape(1, -1), own, *column_operands()]
    outs = [field] * 5 + [table] * 4 + [
        pltpu.VMEM((8, LANES), F32),
        pltpu.VMEM((two * shots, 2, rows, cols), F32),
    ]
    return pl.pallas_call(
        early_kernel,
        in_specs=[pl.BlockSpec(memory_space=pltpu.SMEM)] + [VMEM_WHOLE] * len(args),
        out_specs=[VMEM_WHOLE] * len(outs),
        out_shape=outs,
        scratch_shapes=[
            pltpu.VMEM((2, 2 * rows, cols), BF16),
            pltpu.VMEM((2, 2 * rows, cols), BF16),
            pltpu.VMEM((2, 2 * rows, cols), F32),
            pltpu.VMEM((2, 2 * rows, cols), F32),
            pltpu.VMEM((2, 2 * rows, cols), F32),
        ],
        compiler_params=pltpu.CompilerParams(vmem_limit_bytes=24 << 20),
        name="early",
    )(slab_counts, *in_vmem(*args))


def late(wavefields, partner, neighbour, prepared, angles):
    two, four, shots, rows, cols = wavefields.shape
    bins = rows // 2
    per_slab = cols // rows
    items = two * shots
    _, edge, both = (jnp.asarray(t, dtype=BF16) for t in row_tables(rows))
    depth = depth_table(rows, bins)
    depth_top = depth.astype(jnp.bfloat16)
    depth_low = (depth - depth_top.astype(np.float32)).astype(jnp.bfloat16)
    depth = jnp.asarray(np.concatenate([depth_top, depth_top, depth_low], axis=1), dtype=BF16)
    args = [wavefields, partner, neighbour, *prepared, edge, both, *column_operands(), depth]
    out_shape = (per_slab, bins * angles)
    scratch = [
        pltpu.VMEM((items, 2, 48, cols), BF16),
        pltpu.VMEM((items * 2 * 32, cols), BF16),
        pltpu.VMEM((items * 2 * 32, cols), BF16),
        pltpu.VMEM((items * 2 * 32, cols), F32),
        pltpu.VMEM((items * 2 * 32, cols), F32),
        pltpu.VMEM((items * 2 * 32, cols), F32),
        pltpu.VMEM((items, 2, 24, cols), F32),
        pltpu.VMEM((2, 2 * (rows + 16), cols), BF16),
        pltpu.VMEM((2, 2 * rows, cols), BF16),
        pltpu.VMEM((2, 2 * rows, cols), F32),
        pltpu.VMEM((2, 2 * rows, cols), F32),
        pltpu.VMEM((2, 2 * rows, cols), F32),
        pltpu.VMEM((2, 3 * rows, cols), BF16),
        pltpu.VMEM((PITCH * bins, LANES), F32),
        pltpu.VMEM((8, bins * angles), F32),
    ]
    return pl.pallas_call(
        late_kernel,
        in_specs=[VMEM_WHOLE] * len(args),
        out_specs=VMEM_WHOLE,
        out_shape=pltpu.VMEM(out_shape, BF16),
        scratch_shapes=scratch,
        compiler_params=pltpu.CompilerParams(vmem_limit_bytes=32 << 20),
        name="late",
    )(*in_vmem(*args))


def pick_kernel(loc_ref, own_ref, other_ref, out_ref, *, per_slab):
    slab = lax.axis_index(SLAB)
    chip, core = (lax.axis_index("chip"), lax.axis_index("core"))
    chips = lax.axis_size("chip")
    count = out_ref.shape[0]
    per_row = LANES // count
    loc = loc_ref[pl.ds(slab // per_row, 1), :]
    loc = pltpu.roll(loc, (LANES - (slab % per_row) * count) % LANES, 1)[:, :count]
    held = own_ref.shape[0]
    owner = loc // per_slab
    ahead = lax.rem(owner // 2 - chip + chips, chips)
    up = ahead <= chips // 2
    hops = jnp.where(up, ahead, chips - ahead)
    holder = jnp.where(up, 1, 0)
    place = (hops % len(NEAR)) * len(FAR) + hops // len(NEAR)
    index = (2 * place + jnp.where(owner % 2 == holder, 0, 1)) * per_slab + loc % per_slab
    mine = holder == core
    row = lax.broadcasted_iota(jnp.int32, (held, count), 0)
    hit = row == index
    own_hot = jnp.where(hit & mine, 1.0, 0.0).astype(BF16)
    other_hot = jnp.where(hit & jnp.logical_not(mine), 1.0, 0.0).astype(BF16)

    def choose(hot, ref):
        return lax.dot_general(hot, ref[...], (((0,), (0,)), ((), ())), preferred_element_type=F32)

    out_ref[...] = choose(own_hot, own_ref) + choose(other_hot, other_ref)


def pick(loc_patch, own, other, count, per_slab):
    width = own.shape[1]
    return pl.pallas_call(
        lambda *refs: pick_kernel(*refs, per_slab=per_slab),
        in_specs=[VMEM_WHOLE] * 3,
        out_shape=jax.ShapeDtypeStruct((count, width), F32),
        compiler_params=pltpu.CompilerParams(vmem_limit_bytes=8 << 20),
        name="pick",
    )(*in_vmem(loc_patch.reshape(-1, LANES), own, other))


def swap_cores(array):
    return lax.ppermute(array, "core", [(0, 1), (1, 0)])


def onward(array, hops):
    chips = lax.axis_size("chip")
    pairs = [(2 * i, 2 * ((i + hops) % chips)) for i in range(chips)]
    pairs += [(2 * i + 1, 2 * ((i - hops) % chips) + 1) for i in range(chips)]
    return lax.ppermute(array, SLAB, pairs)


def spread(images):
    held = jnp.concatenate([images, swap_cores(images)])
    for hops in (FAR, NEAR):
        held = jnp.concatenate([held] + [onward(held, h) for h in hops[1:]])
    return held


def per_device(
    wavefields, courant, epsilon, anisotropy_delta, tilt_angle, loc_patch, slab_counts, angle_table
):
    slabs = lax.axis_size(SLAB)
    assert FAR[-1] + NEAR[-1] >= slabs // 4
    per_slab = wavefields.shape[4] // wavefields.shape[3]
    params = (courant, epsilon, anisotropy_delta, tilt_angle)
    to_partner, to_neighbour = pack(wavefields, params)
    partner = swap_cores(to_partner)
    pairs = [(i, i + 1) for i in range(1, slabs - 1, 2)]
    neighbour = lax.ppermute(to_neighbour, SLAB, pairs + [(j, i) for i, j in pairs])
    prepared = early(wavefields, params, slab_counts, angle_table)
    images = late(wavefields, partner, neighbour, prepared, angle_table.shape[0])
    own = spread(images)
    return pick(loc_patch, own, swap_cores(own), loc_patch.shape[0] // slabs, per_slab)


def solution(mesh):
    shape = (mesh.shape["groups"], mesh.shape["slab"] // 2, 2)
    finer = Mesh(mesh.devices.reshape(shape), GROUPS_SLAB)
    in_specs = (
        P(None, None, "groups", SLAB, None),
        P(SLAB, None),
        P(SLAB, None),
        P(SLAB, None),
        P(SLAB, None),
        P(),
        P(),
        P(),
    )
    out_specs = P(GROUPS_SLAB, None)
    return jax.shard_map(
        per_device, mesh=finer, in_specs=in_specs, out_specs=out_specs, check_vma=False
    )
```

```python
import math

import jax
import jax.numpy as jnp
import numpy as np
from jax import lax
from jax.experimental import pallas as pl
from jax.experimental.pallas import tpu as pltpu
from jax.sharding import Mesh
from jax.sharding import PartitionSpec as P

SLAB = ("chip", "core")
GROUPS_SLAB = ("groups", "chip", "core")
LANES = 128
HALF = 4
RUN = 8
PITCH = 40
FAR, NEAR = ((0, 3, 6), (0, 1, 2))
SECOND = (-14336.0, 8064.0, -1008.0, 128.0, -9.0)
SECOND_REST = 14.0
SECOND_UNIT = 5040.0
FIRST = (672.0, -168.0, 32.0, -3.0)
FIRST_UNIT = 840.0
BF16 = jnp.bfloat16
F32 = jnp.float32
VMEM_WHOLE = pl.BlockSpec(memory_space=pltpu.VMEM)


def in_vmem(*arrays):
    return [pltpu.with_memory_space_constraint(a, pltpu.VMEM) for a in arrays]


def weight(kind, offset):
    if abs(offset) > HALF:
        return 0.0
    if kind == 2:
        return SECOND[abs(offset)]
    if offset == 0:
        return 0.0
    return FIRST[abs(offset) - 1] * (1.0 if offset > 0 else -1.0)


def band(kind, outputs, inputs):
    table = np.zeros((len(outputs), len(inputs)), np.float32)
    for i, o in enumerate(outputs):
        for j, n in enumerate(inputs):
            if o is not None and n is not None:
                table[i, j] = weight(kind, n - o)
    return table


def row_tables(rows):
    own = list(range(rows))
    inner = list(range(-HALF, 0)) + list(range(rows, rows + HALF))
    outer = list(range(-2 * HALF, -HALF)) + list(range(rows + HALF, rows + 2 * HALF))
    pad = [None] * 8
    ends = own[:8] + own[-8:]
    edge_in = ends + inner + outer + own[8:16] + own[-16:-8]
    edge_out = ends + inner + pad
    second_in = own + inner + pad
    tables = ((own, own), (edge_out, edge_in), (own, second_in))
    return [np.concatenate([band(2, o, i), band(1, o, i)]) for o, i in tables]


def column_tables(kind):
    block = list(range(2 * LANES))
    inside = band(kind, block, block).T
    across = np.zeros((2 * LANES, 2 * LANES), np.float32)
    for i in range(2 * LANES):
        for o in range(2 * LANES):
            if (i < LANES) != (o < LANES):
                across[i, o] = weight(kind, i - o)
    return inside, across


def depth_table(patch, bins):
    k = np.arange(bins)[:, None]
    z = np.arange(patch)[None, :]
    phase = (2.0 * math.pi / patch * np.mod(k * z, patch)).astype(np.float32)
    table = np.concatenate([np.cos(phase), -np.sin(phase)]).astype(np.float32) * np.float32(1.0 / math.sqrt(patch))
    return table.astype(np.float32)


def quarter_turns(quarter, cosine, sine):
    odd = (quarter & 1) == 1
    c = jnp.where(odd, sine, cosine)
    s = jnp.where(odd, cosine, sine)
    c = jnp.where(((quarter + 1) & 2) == 2, -c, c)
    s = jnp.where((quarter & 2) == 2, -s, s)
    return c, s


def small_cos_sin(y):
    y2 = y * y
    s = y * (1.0 + y2 * (-1.6666654611e-1 + y2 * (8.3321608736e-3 + y2 * -1.9515295891e-4)))
    c = 1.0 - 0.5 * y2 + y2 * y2 * (4.166664568298827e-2 + y2 * (-1.388731625493765e-3 + y2 * 2.443315711809948e-5))
    return c, s


def double_angle(theta):
    n = jnp.floor(theta * (4.0 / math.pi) + 0.5)
    y = 2.0 * theta - n * 1.5703125
    y = y - n * 4.837512969970703e-4
    y = y - n * 7.54978995489188216e-8
    c, s = small_cos_sin(y)
    return quarter_turns(n.astype(jnp.int32), c, s)


def pack_kernel(
    w_top, w_bot, c_top, c_bot, e_top, e_bot, d_top, d_bot, t_top, t_bot, partner_ref, neighbour_ref
):
    low = lax.broadcasted_iota(jnp.int32, (8, w_top.shape[-1]), 0) < HALF

    def half_turn(x):
        return pltpu.roll(x, HALF, 0)

    def emit(out, wave, params, upward):
        def join(a, b):
            return jnp.where(low, half_turn(a), b) if upward else jnp.where(low, a, half_turn(b))

        groups = []
        for w in range(wave.shape[0]):
            for s in range(wave.shape[2]):
                groups.append(wave[w, 0, s])
                groups.append(wave[w, 1, s])
                groups.append(join(wave[w, 2, s], wave[w, 3, s]))
        courant, eps, delta, tilt = (p[...] for p in params)
        high = tilt.astype(BF16).astype(F32)
        groups += [join(courant, eps), join(delta, high), tilt - high]
        groups.append(groups[-1])
        for g in range(0, len(groups), 2):
            out[8 * g : 8 * g + 16, :] = jnp.concatenate(groups[g : g + 2], axis=0).astype(BF16)

    tops = (w_top, (c_top, e_top, d_top, t_top))
    bottoms = (w_bot, (c_bot, e_bot, d_bot, t_bot))
    first = lax.axis_index("core") == 0

    @pl.when(first)
    def _():
        emit(partner_ref, *bottoms, True)
        emit(neighbour_ref, *tops, False)

    @pl.when(jnp.logical_not(first))
    def _():
        emit(partner_ref, *tops, False)
        emit(neighbour_ref, *bottoms, True)


def pack(wavefields, params):
    two, four, shots, rows, cols = wavefields.shape
    last = rows // 8 - 1
    groups = 2 * shots * 3 + 4
    wave_block = (two, four, shots, 8, cols)
    specs = [
        pl.BlockSpec(wave_block, lambda i: (0, 0, 0, 0, 0)),
        pl.BlockSpec(wave_block, lambda i: (0, 0, 0, last, 0)),
    ]
    args = [wavefields, wavefields]
    for p in params:
        specs += [pl.BlockSpec((8, cols), lambda i: (0, 0)), pl.BlockSpec((8, cols), lambda i: (last, 0))]
        args += [p, p]
    out = pltpu.VMEM((8 * groups, cols), BF16)
    return pl.pallas_call(
        pack_kernel,
        grid=(1,),
        in_specs=specs,
        out_specs=[VMEM_WHOLE] * 2,
        out_shape=[out, out],
        compiler_params=pltpu.CompilerParams(vmem_limit_bytes=8 << 20),
        name="pack",
    )(*(pltpu.with_memory_space_constraint(a, pltpu.HBM) for a in args))


def coefficients(courant, eps, delta, tilt):
    cosine, sine = double_angle(tilt)
    scaled = courant * (1.0 / SECOND_UNIT)
    stretch = 1.0 + 2.0 * delta
    return (
        0.5 + 0.5 * cosine,
        sine * (SECOND_UNIT / (FIRST_UNIT * FIRST_UNIT)),
        scaled * (1.0 + 2.0 * eps),
        scaled * (stretch * lax.rsqrt(stretch)),
        scaled,
    )


def along_columns(out, source, inside, across):
    out[:, LANES : 3 * LANES] = jnp.dot(source[:, LANES : 3 * LANES], across[...], preferred_element_type=F32)
    left = jnp.dot(source[:, : 2 * LANES], inside[...], preferred_element_type=F32)
    out[:, :LANES] = left[:, :LANES]
    out[:, LANES : 2 * LANES] += left[:, LANES:]
    right = jnp.dot(source[:, 2 * LANES :], inside[...], preferred_element_type=F32)
    out[:, 2 * LANES : 3 * LANES] += right[:, :LANES]
    out[:, 3 * LANES :] = right[:, LANES:]


def derive(field, slope, zz, xx, xz, table, columns, fields):
    count = table.shape[0] // 2
    for f in range(2):
        source = field[f]
        product = jnp.dot(table[count:, :], source, preferred_element_type=F32)
        slope[f * count : (f + 1) * count, :] = product.astype(BF16)
        zz[f * count : (f + 1) * count, :] = jnp.dot(table[:count, :], source, preferred_element_type=F32)
    along_columns(xx, fields, columns[0], columns[1])
    along_columns(xz, slope[...], columns[2], columns[3])


def tilted(f, value, zz, xx, xz, mix, twist):
    turn = mix * (xx - zz) - twist * xz
    rest = SECOND_REST * value
    return (zz + turn) - rest if f == 0 else (xx - turn) - rest


def early_kernel(
    counts_ref, wave_ref, courant_ref, eps_ref, delta_ref, tilt_ref, angle_ref, own_ref,
    xx_ref, xx_across_ref, x_ref, x_across_ref,
    mix_ref, twist_ref, a_ref, b_ref, c_ref, low_c, low_s, high_c, high_s, alive_ref, next_ref,
    field_ref, slope_ref, zz_ref, xx_out, xz_out,
):
    rows, cols = courant_ref.shape
    wavefields, _, shots = wave_ref.shape[:3]
    columns = (xx_ref, xx_across_ref, x_ref, x_across_ref)
    items = [(w, s) for w in range(wavefields) for s in range(shots)]

    def matmuls(i):
        w, s = items[i]
        k = i % 2
        for f in range(2):
            field_ref[k, f * rows : (f + 1) * rows, :] = wave_ref[w, f, s].astype(BF16)
        parts = [field_ref.at[k, f * rows : (f + 1) * rows, :][...] for f in range(2)]
        derive(
            parts, slope_ref.at[k], zz_ref.at[k], xx_out.at[k], xz_out.at[k], own_ref, columns,
            field_ref.at[k][...],
        )

    def advance(i):
        w, s = items[i]
        k = i % 2
        for r in range(8, rows - 8, 8):
            at = slice(r, r + 8)
            p, q, p0, q0 = (wave_ref[w, f, s, at, :] for f in range(4))
            mix, twist = (mix_ref[at, :], twist_ref[at, :])

            def operator(f, value):
                here = slice(f * rows + r, f * rows + r + 8)
                return tilted(f, value, zz_ref[k, here, :], xx_out[k, here, :], xz_out[k, here, :], mix, twist)

            across, along = (operator(0, p), operator(1, q))
            a, b, c = (a_ref[at, :], b_ref[at, :], c_ref[at, :])
            next_ref[i, 0, at, :] = (2.0 * p - p0) + (a * across + b * along)
            next_ref[i, 1, at, :] = (2.0 * q - q0) + (b * across + c * along)

    matmuls(0)
    for r in range(0, rows, 8):
        at = slice(r, r + 8)
        values = coefficients(courant_ref[at, :], eps_ref[at, :], delta_ref[at, :], tilt_ref[at, :])
        for ref, value in zip((mix_ref, twist_ref, a_ref, b_ref, c_ref), values, strict=True):
            ref[at, :] = value
    for i in range(1, len(items)):
        matmuls(i)
        advance(i - 1)
    slant_factors(angle_ref, low_c, low_s, high_c, high_s)
    advance(len(items) - 1)
    live = lax.broadcasted_iota(jnp.int32, (8, LANES), 0) < counts_ref[lax.axis_index(SLAB)]
    alive_ref[...] = jnp.where(live, 1.0, 0.0)


def slant_factors(angle_ref, low_c, low_s, high_c, high_s):
    right_half = lax.broadcasted_iota(jnp.int32, (LANES, LANES), 1) >= LANES // 2
    angles = jnp.concatenate([angle_ref[...], angle_ref[...]], axis=1)
    lateral = lax.broadcasted_iota(jnp.int32, (LANES, LANES), 0)
    modulus = 16 * LANES
    turn = (lateral * angles) & (modulus - 1)
    quarter = (turn + modulus // 8) >> int(math.log2(modulus // 4))
    rest = turn - quarter * (modulus // 4)
    c1, s1 = small_cos_sin(rest.astype(F32) * (2.0 * math.pi / modulus))
    c1, s1 = quarter_turns(quarter, c1, s1)

    def times(x, y):
        return (x[0] * y[0] - x[1] * y[1], x[0] * y[1] + x[1] * y[0])

    low_c[...], low_s[...] = (c1, s1)
    stride = (c1, s1)
    for _ in range(int(math.log2(RUN))):
        stride = times(stride, stride)
    scale = 1.0 / math.sqrt(LANES)
    value = (jnp.where(right_half, 0.0, scale), jnp.where(right_half, scale, 0.0))
    for j in range(high_c.shape[0]):
        high_c[j], high_s[j] = value
        value = times(value, stride)


def late_kernel(
    wave_ref, partner_ref, neighbour_ref, mix_ref, twist_ref, a_ref, b_ref, c_ref,
    low_c, low_s, high_c, high_s, alive_ref, next_ref,
    edge_table_ref, two_ref, xx_ref, xx_across_ref, x_ref, x_across_ref, depth_ref,
    out_ref,
    edge_z, edge_x, edge_slope, edge_zz, edge_xx, edge_xz, edge_next,
    field_ref, slope_ref, zz_ref, xx_out, xz_out, split_ref, spectra_ref, image_ref, slant_ref,
):
    wavefields, _, shots, rows, cols = wave_ref.shape
    bins = rows // 2
    per_slab = cols // LANES
    columns = (xx_ref, xx_across_ref, x_ref, x_across_ref)
    items = [(w, s) for w in range(wavefields) for s in range(shots)]
    low = lax.broadcasted_iota(jnp.int32, (8, cols), 0) < HALF
    first = lax.axis_index("core") == 0
    coefficient_refs = (mix_ref, twist_ref, a_ref, b_ref, c_ref)

    def half_turn(x):
        return pltpu.roll(x, HALF, 0)

    def group(g):
        at = slice(8 * g, 8 * g + 8)
        a, b = (partner_ref[at, :].astype(F32), neighbour_ref[at, :].astype(F32))
        return jnp.where(first, b, a), jnp.where(first, a, b)

    def first_halves(g):
        u, d = group(g)
        return jnp.where(low, u, half_turn(d))

    def second_halves(g):
        u, d = group(g)
        return jnp.where(low, half_turn(u), d)

    tall = 32
    halos = []
    for i, (w, s) in enumerate(items):
        halo = []
        for f in range(2):
            u, d = group(3 * i + f)
            inner = jnp.where(low, half_turn(u), half_turn(d))
            outer = jnp.where(low, u, d)
            halo.append(inner)
            pieces = (
                wave_ref[w, f, s, 0:8, :], wave_ref[w, f, s, rows - 8 : rows, :], inner, outer,
                wave_ref[w, f, s, 8:16, :], wave_ref[w, f, s, rows - 16 : rows - 8, :],
            )
            for n in range(0, 6, 2):
                pair = jnp.concatenate(pieces[n : n + 2], axis=0).astype(BF16)
                edge_z[i, f, 8 * n : 8 * n + 16, :] = pair
                if n < 4:
                    at = (2 * i + f) * tall + 8 * n
                    edge_x[at : at + 16, :] = pair
        halo += [first_halves(3 * i + 2), second_halves(3 * i + 2)]
        halos.append(halo)
    for i in range(len(items)):
        for f in range(2):
            product = jnp.dot(edge_table_ref[...], edge_z[i, f], preferred_element_type=F32)
            at = (2 * i + f) * tall
            edge_zz[at : at + tall, :] = product[:tall]
            edge_slope[at : at + tall, :] = product[tall:].astype(BF16)
    along_columns(edge_xx, edge_x[...], xx_ref, xx_across_ref)
    along_columns(edge_xz, edge_slope[...], x_ref, x_across_ref)
    g = 3 * len(items)
    beyond = coefficients(
        first_halves(g), second_halves(g), first_halves(g + 1), second_halves(g + 1) + first_halves(g + 2)
    )

    def edge_advance(i):
        w, s = items[i]
        for n, r in enumerate((0, rows - 8, None)):
            if r is None:
                fields = halos[i]
                mix, twist, a, b, c = beyond
            else:
                at = slice(r, r + 8)
                fields = [wave_ref[w, f, s, at, :] for f in range(4)]
                mix, twist, a, b, c = (ref[at, :] for ref in coefficient_refs)
            p, q, p0, q0 = fields

            def operator(f, value):
                here = slice((2 * i + f) * tall + 8 * n, (2 * i + f) * tall + 8 * n + 8)
                return tilted(f, value, edge_zz[here, :], edge_xx[here, :], edge_xz[here, :], mix, twist)

            across, along = (operator(0, p), operator(1, q))
            edge_next[i, 0, 8 * n : 8 * n + 8, :] = (2.0 * p - p0) + (a * across + b * along)
            edge_next[i, 1, 8 * n : 8 * n + 8, :] = (2.0 * q - q0) + (b * across + c * along)

    def current(i, f, r):
        if r == 0:
            return edge_next[i, f, 0:8, :]
        if r == rows - 8:
            return edge_next[i, f, 8:16, :]
        return next_ref[i, f, r : r + 8, :]

    def matmuls(i):
        k = i % 2
        for f in range(2):
            for r in range(0, rows, 16):
                pair = jnp.concatenate([current(i, f, r), current(i, f, r + 8)], axis=0)
                pair = pair.astype(BF16)
                field_ref[k, f * rows + r : f * rows + r + 16, :] = pair
            edge = edge_next[i, f, 16:24, :]
            pair = jnp.concatenate([edge, jnp.zeros_like(edge)], axis=0).astype(BF16)
            field_ref[k, 2 * rows + 16 * f : 2 * rows + 16 * f + 16, :] = pair
        parts = [
            jnp.concatenate(
                [
                    field_ref[k, f * rows : (f + 1) * rows, :],
                    field_ref[k, 2 * rows + 16 * f : 2 * rows + 16 * f + 16, :],
                ],
                axis=0,
            )
            for f in range(2)
        ]
        derive(
            parts, slope_ref.at[k], zz_ref.at[k], xx_out.at[k], xz_out.at[k], two_ref, columns,
            field_ref[k, : 2 * rows, :],
        )

    def advance(i):
        w, s = items[i]
        k = i % 2
        for r in range(0, rows, 16):
            parts = []
            for h in (r, r + 8):
                at = slice(h, h + 8)
                mix, twist, a, b = (ref[at, :] for ref in coefficient_refs[:4])

                def operator(f, value):
                    here = slice(f * rows + h, f * rows + h + 8)
                    return tilted(
                        f, value, zz_ref[k, here, :], xx_out[k, here, :], xz_out[k, here, :], mix, twist
                    )

                p, q = (current(i, f, h) for f in range(2))
                across, along = (operator(0, p), operator(1, q))
                parts.append((2.0 * p - wave_ref[w, 0, s, at, :]) + (a * across + b * along))
            value = jnp.concatenate(parts, axis=0)
            top = value.astype(BF16)
            split_ref[k, r : r + 16, :] = top
            split_ref[k, rows + r : rows + r + 16, :] = (value - top.astype(F32)).astype(BF16)
            split_ref[k, 2 * rows + r : 2 * rows + r + 16, :] = top

    def transform(i):
        spectra = jnp.dot(depth_ref[...], split_ref[i % 2], preferred_element_type=F32)
        for part in range(2):
            for m in range(per_slab):
                start = 16 * part + per_slab * i + m
                spectra_ref[pl.ds(start, bins, stride=PITCH), :] = spectra[
                    part * bins : (part + 1) * bins, m * LANES : (m + 1) * LANES
                ]

    for i in range(len(items)):
        edge_advance(i)
    matmuls(0)
    for i in range(1, len(items)):
        matmuls(i)
        advance(i - 1)
        transform(i - 1)
    advance(len(items) - 1)
    transform(len(items) - 1)

    left_lane = lax.broadcasted_iota(jnp.int32, (8, LANES), 1) < LANES // 2
    alive = alive_ref[...]
    for j in range(bins // RUN):
        slot = j % 2
        for r in range(0, LANES, 16):
            at = slice(r, r + 16)
            one = (low_c[at, :], low_s[at, :])
            back = (high_c[j, at, :], high_s[j, at, :])
            here = (back[0] * one[0] - back[1] * one[1], back[0] * one[1] + back[1] * one[0])
            twice = 2.0 * one[0]
            for i in range(RUN):
                slant_ref[slot, i, at, :] = back[0].astype(BF16)
                slant_ref[slot, i, LANES + r : LANES + r + 16, :] = back[1].astype(BF16)
                back, here = here, tuple(twice * x - y for x, y in zip(here, back, strict=True))
        pair = []
        for i in range(RUN):
            at = (RUN * j + i) * PITCH
            left = jnp.concatenate(
                [spectra_ref[at : at + 16, :], spectra_ref[at + 16 : at + 32, :]], axis=1
            ).astype(BF16)
            stack = jnp.dot(left, slant_ref[slot, i], preferred_element_type=F32)
            product = stack[:8] * stack[8:]
            pair.append(product + pltpu.roll(product, 4, 0))
            if i % 2 == 1:
                even, odd = pair
                even = even + pltpu.roll(even, LANES // 2, 1)
                odd = odd + pltpu.roll(odd, LANES // 2, 1)
                pair = []
                where_to = (RUN * j + i) // 2 * LANES
                image_ref[:, where_to : where_to + LANES] = alive * jnp.where(left_lane, even, odd)
    out_ref[...] = image_ref[:per_slab, :].astype(BF16)


def column_operands():
    return [jnp.asarray(t, dtype=BF16) for kind in (2, 1) for t in column_tables(kind)]


def early(wavefields, params, slab_counts, angle_table):
    two, four, shots, rows, cols = wavefields.shape
    field = pltpu.VMEM((rows, cols), F32)
    table = pltpu.VMEM((rows // 2 // RUN, LANES, LANES), F32)
    own = jnp.asarray(row_tables(rows)[0], dtype=BF16)
    args = [wavefields, *params, angle_table.reshape(1, -1), own, *column_operands()]
    outs = [field] * 5 + [pltpu.VMEM((LANES, LANES), F32)] * 2 + [table] * 2 + [
        pltpu.VMEM((8, LANES), F32),
        pltpu.VMEM((two * shots, 2, rows, cols), F32),
    ]
    return pl.pallas_call(
        early_kernel,
        in_specs=[pl.BlockSpec(memory_space=pltpu.SMEM)] + [VMEM_WHOLE] * len(args),
        out_specs=[VMEM_WHOLE] * len(outs),
        out_shape=outs,
        scratch_shapes=[
            pltpu.VMEM((2, 2 * rows, cols), BF16),
            pltpu.VMEM((2, 2 * rows, cols), BF16),
            pltpu.VMEM((2, 2 * rows, cols), F32),
            pltpu.VMEM((2, 2 * rows, cols), F32),
            pltpu.VMEM((2, 2 * rows, cols), F32),
        ],
        compiler_params=pltpu.CompilerParams(vmem_limit_bytes=24 << 20),
        name="early",
    )(slab_counts, *in_vmem(*args))


def late(wavefields, partner, neighbour, prepared, angles):
    two, four, shots, rows, cols = wavefields.shape
    bins = rows // 2
    per_slab = cols // rows
    items = two * shots
    _, edge, both = (jnp.asarray(t, dtype=BF16) for t in row_tables(rows))
    depth = depth_table(rows, bins)
    depth_top = depth.astype(jnp.bfloat16)
    depth_low = (depth - depth_top.astype(np.float32)).astype(jnp.bfloat16)
    depth = jnp.asarray(np.concatenate([depth_top, depth_top, depth_low], axis=1), dtype=BF16)
    args = [wavefields, partner, neighbour, *prepared, edge, both, *column_operands(), depth]
    out_shape = (per_slab, bins * angles)
    scratch = [
        pltpu.VMEM((items, 2, 48, cols), BF16),
        pltpu.VMEM((items * 2 * 32, cols), BF16),
        pltpu.VMEM((items * 2 * 32, cols), BF16),
        pltpu.VMEM((items * 2 * 32, cols), F32),
        pltpu.VMEM((items * 2 * 32, cols), F32),
        pltpu.VMEM((items * 2 * 32, cols), F32),
        pltpu.VMEM((items, 2, 24, cols), F32),
        pltpu.VMEM((2, 2 * (rows + 16), cols), BF16),
        pltpu.VMEM((2, 2 * rows, cols), BF16),
        pltpu.VMEM((2, 2 * rows, cols), F32),
        pltpu.VMEM((2, 2 * rows, cols), F32),
        pltpu.VMEM((2, 2 * rows, cols), F32),
        pltpu.VMEM((2, 3 * rows, cols), BF16),
        pltpu.VMEM((PITCH * bins, LANES), F32),
        pltpu.VMEM((8, bins * angles), F32),
        pltpu.VMEM((2, RUN, 2 * LANES, LANES), BF16),
    ]
    return pl.pallas_call(
        late_kernel,
        in_specs=[VMEM_WHOLE] * len(args),
        out_specs=VMEM_WHOLE,
        out_shape=pltpu.VMEM(out_shape, BF16),
        scratch_shapes=scratch,
        compiler_params=pltpu.CompilerParams(vmem_limit_bytes=32 << 20),
        name="late",
    )(*in_vmem(*args))


def pick_kernel(loc_ref, *refs, per_slab):
    held_refs, (mine_ref, theirs_ref) = (refs[:-2], refs[-2:])
    slab = lax.axis_index(SLAB)
    chip, core = (lax.axis_index("chip"), lax.axis_index("core"))
    chips = lax.axis_size("chip")
    count = mine_ref.shape[0]
    per_row = LANES // count
    row = loc_ref[pl.ds(slab // per_row, 1), :]
    spot = slab % per_row
    partner = spot + 1 - 2 * core
    loc = jnp.concatenate(
        [pltpu.roll(row, (LANES - s * count) % LANES, 1)[:, :count] for s in (spot, partner)], axis=1
    )
    owner = loc // per_slab
    ahead = lax.rem(owner // 2 - chip + chips, chips)
    up = ahead <= chips // 2
    hops = jnp.where(up, ahead, chips - ahead)
    holder = jnp.where(up, 1, 0)
    index = (2 * (hops // len(NEAR)) + jnp.where(owner % 2 == holder, 0, 1)) * per_slab + loc % per_slab
    total = None
    for near, ref in enumerate(held_refs):
        held = lax.broadcasted_iota(jnp.int32, (ref.shape[0], 2 * count), 0)
        hit = (held == index) & (holder == core) & (hops % len(NEAR) == near)
        hot = jnp.where(hit, 1.0, 0.0).astype(BF16)
        part = lax.dot_general(hot, ref[...], (((0,), (0,)), ((), ())), preferred_element_type=F32)
        total = part if total is None else total + part
    mine_ref[...] = total[:count]
    theirs_ref[...] = total[count:].astype(BF16)


def pick(loc_patch, held, count, per_slab):
    width = held[0].shape[1]
    return pl.pallas_call(
        lambda *refs: pick_kernel(*refs, per_slab=per_slab),
        in_specs=[VMEM_WHOLE] * (1 + len(held)),
        out_specs=[VMEM_WHOLE] * 2,
        out_shape=[pltpu.VMEM((count, width), F32), pltpu.VMEM((count, width), BF16)],
        compiler_params=pltpu.CompilerParams(vmem_limit_bytes=8 << 20),
        name="pick",
    )(*in_vmem(loc_patch.reshape(-1, LANES), *held))


def swap_cores(array):
    return lax.ppermute(array, "core", [(0, 1), (1, 0)])


def onward(array, hops):
    chips = lax.axis_size("chip")
    pairs = [(2 * i, 2 * ((i + hops) % chips)) for i in range(chips)]
    pairs += [(2 * i + 1, 2 * ((i - hops) % chips) + 1) for i in range(chips)]
    return lax.ppermute(array, SLAB, pairs)


def spread(images):
    held = jnp.concatenate([images, swap_cores(images)])
    held = jnp.concatenate([held] + [onward(held, h) for h in FAR[1:]])
    return [held] + [onward(held, h) for h in NEAR[1:]]


def per_device(
    wavefields, courant, epsilon, anisotropy_delta, tilt_angle, loc_patch, slab_counts, angle_table
):
    slabs = lax.axis_size(SLAB)
    assert FAR[-1] + NEAR[-1] >= slabs // 4
    per_slab = wavefields.shape[4] // wavefields.shape[3]
    params = (courant, epsilon, anisotropy_delta, tilt_angle)
    to_partner, to_neighbour = pack(wavefields, params)
    partner = swap_cores(to_partner)
    pairs = [(i, i + 1) for i in range(1, slabs - 1, 2)]
    neighbour = lax.ppermute(to_neighbour, SLAB, pairs + [(j, i) for i, j in pairs])
    prepared = early(wavefields, params, slab_counts, angle_table)
    images = late(wavefields, partner, neighbour, prepared, angle_table.shape[0])
    mine, theirs = pick(loc_patch, spread(images), loc_patch.shape[0] // slabs, per_slab)
    return mine + swap_cores(theirs).astype(F32)


def solution(mesh):
    shape = (mesh.shape["groups"], mesh.shape["slab"] // 2, 2)
    finer = Mesh(mesh.devices.reshape(shape), GROUPS_SLAB)
    in_specs = (
        P(None, None, "groups", SLAB, None),
        P(SLAB, None),
        P(SLAB, None),
        P(SLAB, None),
        P(SLAB, None),
        P(),
        P(),
        P(),
    )
    out_specs = P(GROUPS_SLAB, None)
    return jax.shard_map(
        per_device, mesh=finer, in_specs=in_specs, out_specs=out_specs, check_vma=False
    )
```

```python
import math

import jax
import jax.numpy as jnp
import numpy as np
from jax import lax
from jax.experimental import pallas as pl
from jax.experimental.pallas import tpu as pltpu
from jax.sharding import Mesh
from jax.sharding import PartitionSpec as P


SLAB = ("chip", "core")
GROUPS_SLAB = ("groups", "chip", "core")
LANES = 128
HALF = 4
RUN = 8
PITCH = 40
FAR, NEAR = ((0, 3, 6), (0, 1, 2))
SECOND = (-14336.0, 8064.0, -1008.0, 128.0, -9.0)
SECOND_REST = 14.0
SECOND_UNIT = 5040.0
FIRST = (672.0, -168.0, 32.0, -3.0)
FIRST_UNIT = 840.0
BF16 = jnp.bfloat16
F32 = jnp.float32
VMEM_WHOLE = pl.BlockSpec(memory_space=pltpu.VMEM)


def in_vmem(*arrays):
    return [pltpu.with_memory_space_constraint(a, pltpu.VMEM) for a in arrays]


def weight(kind, offset):
    if abs(offset) > HALF:
        return 0.0
    if kind == 2:
        return SECOND[abs(offset)]
    if offset == 0:
        return 0.0
    return FIRST[abs(offset) - 1] * (1.0 if offset > 0 else -1.0)


def band(kind, outputs, inputs):
    table = np.zeros((len(outputs), len(inputs)), np.float32)
    for i, o in enumerate(outputs):
        for j, n in enumerate(inputs):
            if o is not None and n is not None:
                table[i, j] = weight(kind, n - o)
    return table


def row_tables(rows):
    own = list(range(rows))
    inner = list(range(-HALF, 0)) + list(range(rows, rows + HALF))
    outer = list(range(-2 * HALF, -HALF)) + list(range(rows + HALF, rows + 2 * HALF))
    pad = [None] * 8
    ends = own[:8] + own[-8:]
    edge_in = ends + inner + outer + own[8:16] + own[-16:-8]
    edge_out = ends + inner + pad
    second_in = own + inner + pad
    tables = ((own, own), (edge_out, edge_in), (own, second_in))
    return [np.concatenate([band(2, o, i), band(1, o, i)]) for o, i in tables]


def column_tables(kind):
    block = list(range(2 * LANES))
    inside = band(kind, block, block).T
    across = np.zeros((2 * LANES, 2 * LANES), np.float32)
    for i in range(2 * LANES):
        for o in range(2 * LANES):
            if (i < LANES) != (o < LANES):
                across[i, o] = weight(kind, i - o)
    return inside, across


def depth_table(patch, bins):
    k = np.arange(bins)[:, None]
    z = np.arange(patch)[None, :]
    phase = (2.0 * math.pi / patch * np.mod(k * z, patch)).astype(np.float32)
    table = np.concatenate([np.cos(phase), -np.sin(phase)]).astype(np.float32) * np.float32(1.0 / math.sqrt(patch))
    return table.astype(np.float32)


def quarter_turns(quarter, cosine, sine):
    odd = (quarter & 1) == 1
    c = jnp.where(odd, sine, cosine)
    s = jnp.where(odd, cosine, sine)
    c = jnp.where(((quarter + 1) & 2) == 2, -c, c)
    s = jnp.where((quarter & 2) == 2, -s, s)
    return c, s


def small_cos_sin(y):
    y2 = y * y
    s = y * (1.0 + y2 * (-1.6666654611e-1 + y2 * (8.3321608736e-3 + y2 * -1.9515295891e-4)))
    c = 1.0 - 0.5 * y2 + y2 * y2 * (4.166664568298827e-2 + y2 * (-1.388731625493765e-3 + y2 * 2.443315711809948e-5))
    return c, s


def double_angle(theta):
    n = jnp.floor(theta * (4.0 / math.pi) + 0.5)
    y = 2.0 * theta - n * 1.5703125
    y = y - n * 4.837512969970703e-4
    y = y - n * 7.54978995489188216e-8
    c, s = small_cos_sin(y)
    return quarter_turns(n.astype(jnp.int32), c, s)


def pack_kernel(
    w_top, w_bot, c_top, c_bot, e_top, e_bot, d_top, d_bot, t_top, t_bot, partner_ref, neighbour_ref
):
    low = lax.broadcasted_iota(jnp.int32, (8, w_top.shape[-1]), 0) < HALF

    def half_turn(x):
        return pltpu.roll(x, HALF, 0)

    def emit(out, wave, params, upward):
        def join(a, b):
            return jnp.where(low, half_turn(a), b) if upward else jnp.where(low, a, half_turn(b))

        groups = []
        for w in range(wave.shape[0]):
            for s in range(wave.shape[2]):
                groups.append(wave[w, 0, s])
                groups.append(wave[w, 1, s])
                groups.append(join(wave[w, 2, s], wave[w, 3, s]))
        courant, eps, delta, tilt = (p[...] for p in params)
        high = tilt.astype(BF16).astype(F32)
        groups += [join(courant, eps), join(delta, high), tilt - high]
        groups.append(groups[-1])
        for g in range(0, len(groups), 2):
            out[8 * g : 8 * g + 16, :] = jnp.concatenate(groups[g : g + 2], axis=0).astype(BF16)

    tops = (w_top, (c_top, e_top, d_top, t_top))
    bottoms = (w_bot, (c_bot, e_bot, d_bot, t_bot))
    first = lax.axis_index("core") == 0

    @pl.when(first)
    def _():
        emit(partner_ref, *bottoms, True)
        emit(neighbour_ref, *tops, False)

    @pl.when(jnp.logical_not(first))
    def _():
        emit(partner_ref, *tops, False)
        emit(neighbour_ref, *bottoms, True)


def pack(wavefields, params):
    two, four, shots, rows, cols = wavefields.shape
    last = rows // 8 - 1
    groups = 2 * shots * 3 + 4
    wave_block = (two, four, shots, 8, cols)
    specs = [
        pl.BlockSpec(wave_block, lambda i: (0, 0, 0, 0, 0)),
        pl.BlockSpec(wave_block, lambda i: (0, 0, 0, last, 0)),
    ]
    args = [wavefields, wavefields]
    for p in params:
        specs += [pl.BlockSpec((8, cols), lambda i: (0, 0)), pl.BlockSpec((8, cols), lambda i: (last, 0))]
        args += [p, p]
    out = pltpu.VMEM((8 * groups, cols), BF16)
    return pl.pallas_call(
        pack_kernel,
        grid=(1,),
        in_specs=specs,
        out_specs=[VMEM_WHOLE] * 2,
        out_shape=[out, out],
        compiler_params=pltpu.CompilerParams(vmem_limit_bytes=8 << 20),
        name="pack",
    )(*(pltpu.with_memory_space_constraint(a, pltpu.HBM) for a in args))


def coefficients(courant, eps, delta, tilt):
    cosine, sine = double_angle(tilt)
    scaled = courant * (1.0 / SECOND_UNIT)
    stretch = 1.0 + 2.0 * delta
    return (
        0.5 + 0.5 * cosine,
        sine * (SECOND_UNIT / (FIRST_UNIT * FIRST_UNIT)),
        scaled * (1.0 + 2.0 * eps),
        scaled * (stretch * lax.rsqrt(stretch)),
        scaled,
    )


def along_columns(out, source, inside, across):
    out[:, LANES : 3 * LANES] = jnp.dot(source[:, LANES : 3 * LANES], across[...], preferred_element_type=F32)
    left = jnp.dot(source[:, : 2 * LANES], inside[...], preferred_element_type=F32)
    out[:, :LANES] = left[:, :LANES]
    out[:, LANES : 2 * LANES] += left[:, LANES:]
    right = jnp.dot(source[:, 2 * LANES :], inside[...], preferred_element_type=F32)
    out[:, 2 * LANES : 3 * LANES] += right[:, :LANES]
    out[:, 3 * LANES :] = right[:, LANES:]


def derive(field, slope, zz, xx, xz, table, columns, fields):
    count = table.shape[0] // 2
    for f in range(2):
        source = field[f]
        product = jnp.dot(table[count:, :], source, preferred_element_type=F32)
        slope[f * count : (f + 1) * count, :] = product.astype(BF16)
        zz[f * count : (f + 1) * count, :] = jnp.dot(table[:count, :], source, preferred_element_type=F32)
    along_columns(xx, fields, columns[0], columns[1])
    along_columns(xz, slope[...], columns[2], columns[3])


def tilted(f, value, zz, xx, xz, mix, twist):
    turn = mix * (xx - zz) - twist * xz
    rest = SECOND_REST * value
    return (zz + turn) - rest if f == 0 else (xx - turn) - rest


def early_kernel(
    counts_ref, wave_ref, courant_ref, eps_ref, delta_ref, tilt_ref, angle_ref, own_ref,
    xx_ref, xx_across_ref, x_ref, x_across_ref,
    mix_ref, twist_ref, a_ref, b_ref, c_ref, low_c, low_s, high_c, high_s, alive_ref, next_ref,
    field_ref, slope_ref, zz_ref, xx_out, xz_out,
):
    rows, _ = courant_ref.shape
    wavefields, _, shots = wave_ref.shape[:3]
    columns = (xx_ref, xx_across_ref, x_ref, x_across_ref)
    items = [(w, s) for w in range(wavefields) for s in range(shots)]

    def matmuls(i):
        w, s = items[i]
        k = i % 2
        for f in range(2):
            field_ref[k, f * rows : (f + 1) * rows, :] = wave_ref[w, f, s].astype(BF16)
        parts = [field_ref.at[k, f * rows : (f + 1) * rows, :][...] for f in range(2)]
        derive(
            parts, slope_ref.at[k], zz_ref.at[k], xx_out.at[k], xz_out.at[k], own_ref, columns,
            field_ref.at[k][...],
        )

    def advance(i):
        w, s = items[i]
        k = i % 2
        for r in range(8, rows - 8, 8):
            at = slice(r, r + 8)
            p, q, p0, q0 = (wave_ref[w, f, s, at, :] for f in range(4))
            mix, twist = (mix_ref[at, :], twist_ref[at, :])

            def operator(f, value):
                here = slice(f * rows + r, f * rows + r + 8)
                return tilted(f, value, zz_ref[k, here, :], xx_out[k, here, :], xz_out[k, here, :], mix, twist)

            across, along = (operator(0, p), operator(1, q))
            a, b, c = (a_ref[at, :], b_ref[at, :], c_ref[at, :])
            next_ref[i, 0, at, :] = (2.0 * p - p0) + (a * across + b * along)
            next_ref[i, 1, at, :] = (2.0 * q - q0) + (b * across + c * along)

    matmuls(0)
    for r in range(0, rows, 8):
        at = slice(r, r + 8)
        values = coefficients(courant_ref[at, :], eps_ref[at, :], delta_ref[at, :], tilt_ref[at, :])
        for ref, value in zip((mix_ref, twist_ref, a_ref, b_ref, c_ref), values, strict=True):
            ref[at, :] = value
    for i in range(1, len(items)):
        matmuls(i)
        advance(i - 1)
    slant_factors(angle_ref, low_c, low_s, high_c, high_s)
    advance(len(items) - 1)
    live = lax.broadcasted_iota(jnp.int32, (8, LANES), 0) < counts_ref[lax.axis_index(SLAB)]
    alive_ref[...] = jnp.where(live, 1.0, 0.0)


def slant_factors(angle_ref, low_c, low_s, high_c, high_s):
    right_half = lax.broadcasted_iota(jnp.int32, (LANES, LANES), 1) >= LANES // 2
    angles = jnp.concatenate([angle_ref[...], angle_ref[...]], axis=1)
    lateral = lax.broadcasted_iota(jnp.int32, (LANES, LANES), 0)
    modulus = 16 * LANES
    turn = (lateral * angles) & (modulus - 1)
    quarter = (turn + modulus // 8) >> int(math.log2(modulus // 4))
    rest = turn - quarter * (modulus // 4)
    c1, s1 = small_cos_sin(rest.astype(F32) * (2.0 * math.pi / modulus))
    c1, s1 = quarter_turns(quarter, c1, s1)

    def times(x, y):
        return (x[0] * y[0] - x[1] * y[1], x[0] * y[1] + x[1] * y[0])

    low_c[...], low_s[...] = (c1, s1)
    stride = (c1, s1)
    for _ in range(int(math.log2(RUN))):
        stride = times(stride, stride)
    scale = 1.0 / math.sqrt(LANES)
    value = (jnp.where(right_half, 0.0, scale), jnp.where(right_half, scale, 0.0))
    for j in range(high_c.shape[0]):
        high_c[j], high_s[j] = value
        value = times(value, stride)


def late_kernel(
    wave_ref, partner_ref, neighbour_ref, mix_ref, twist_ref, a_ref, b_ref, c_ref,
    low_c, low_s, high_c, high_s, alive_ref, next_ref,
    edge_table_ref, two_ref, xx_ref, xx_across_ref, x_ref, x_across_ref, depth_ref,
    out_ref,
    edge_z, edge_x, edge_slope, edge_zz, edge_xx, edge_xz, edge_next,
    field_ref, slope_ref, zz_ref, xx_out, xz_out, split_ref, spectra_ref, image_ref, slant_ref,
):
    wavefields, _, shots, rows, cols = wave_ref.shape
    bins = rows // 2
    per_slab = cols // LANES
    columns = (xx_ref, xx_across_ref, x_ref, x_across_ref)
    items = [(w, s) for w in range(wavefields) for s in range(shots)]
    low = lax.broadcasted_iota(jnp.int32, (8, cols), 0) < HALF
    first = lax.axis_index("core") == 0
    coefficient_refs = (mix_ref, twist_ref, a_ref, b_ref, c_ref)

    def half_turn(x):
        return pltpu.roll(x, HALF, 0)

    def group(g):
        at = slice(8 * g, 8 * g + 8)
        a, b = (partner_ref[at, :].astype(F32), neighbour_ref[at, :].astype(F32))
        return jnp.where(first, b, a), jnp.where(first, a, b)

    def first_halves(g):
        u, d = group(g)
        return jnp.where(low, u, half_turn(d))

    def second_halves(g):
        u, d = group(g)
        return jnp.where(low, half_turn(u), d)

    tall = 32
    halos = []
    for i, (w, s) in enumerate(items):
        halo = []
        for f in range(2):
            u, d = group(3 * i + f)
            inner = jnp.where(low, half_turn(u), half_turn(d))
            outer = jnp.where(low, u, d)
            halo.append(inner)
            pieces = (
                wave_ref[w, f, s, 0:8, :], wave_ref[w, f, s, rows - 8 : rows, :], inner, outer,
                wave_ref[w, f, s, 8:16, :], wave_ref[w, f, s, rows - 16 : rows - 8, :],
            )
            for n in range(0, 6, 2):
                pair = jnp.concatenate(pieces[n : n + 2], axis=0).astype(BF16)
                edge_z[i, f, 8 * n : 8 * n + 16, :] = pair
                if n < 4:
                    at = (2 * i + f) * tall + 8 * n
                    edge_x[at : at + 16, :] = pair
        halo += [first_halves(3 * i + 2), second_halves(3 * i + 2)]
        halos.append(halo)
    for i in range(len(items)):
        for f in range(2):
            product = jnp.dot(edge_table_ref[...], edge_z[i, f], preferred_element_type=F32)
            at = (2 * i + f) * tall
            edge_zz[at : at + tall, :] = product[:tall]
            edge_slope[at : at + tall, :] = product[tall:].astype(BF16)
    along_columns(edge_xx, edge_x[...], xx_ref, xx_across_ref)
    along_columns(edge_xz, edge_slope[...], x_ref, x_across_ref)
    g = 3 * len(items)
    beyond = coefficients(
        first_halves(g), second_halves(g), first_halves(g + 1), second_halves(g + 1) + first_halves(g + 2)
    )

    def edge_advance(i):
        w, s = items[i]
        for n, r in enumerate((0, rows - 8, None)):
            if r is None:
                fields = halos[i]
                mix, twist, a, b, c = beyond
            else:
                at = slice(r, r + 8)
                fields = [wave_ref[w, f, s, at, :] for f in range(4)]
                mix, twist, a, b, c = (ref[at, :] for ref in coefficient_refs)
            p, q, p0, q0 = fields

            def operator(f, value):
                here = slice((2 * i + f) * tall + 8 * n, (2 * i + f) * tall + 8 * n + 8)
                return tilted(f, value, edge_zz[here, :], edge_xx[here, :], edge_xz[here, :], mix, twist)

            across, along = (operator(0, p), operator(1, q))
            edge_next[i, 0, 8 * n : 8 * n + 8, :] = (2.0 * p - p0) + (a * across + b * along)
            edge_next[i, 1, 8 * n : 8 * n + 8, :] = (2.0 * q - q0) + (b * across + c * along)

    def current(i, f, r):
        if r == 0:
            return edge_next[i, f, 0:8, :]
        if r == rows - 8:
            return edge_next[i, f, 8:16, :]
        return next_ref[i, f, r : r + 8, :]

    def matmuls(i):
        k = i % 2
        for f in range(2):
            for r in range(0, rows, 16):
                pair = jnp.concatenate([current(i, f, r), current(i, f, r + 8)], axis=0)
                pair = pair.astype(BF16)
                field_ref[k, f * rows + r : f * rows + r + 16, :] = pair
            edge = edge_next[i, f, 16:24, :]
            pair = jnp.concatenate([edge, jnp.zeros_like(edge)], axis=0).astype(BF16)
            field_ref[k, 2 * rows + 16 * f : 2 * rows + 16 * f + 16, :] = pair
        parts = [
            jnp.concatenate(
                [
                    field_ref[k, f * rows : (f + 1) * rows, :],
                    field_ref[k, 2 * rows + 16 * f : 2 * rows + 16 * f + 16, :],
                ],
                axis=0,
            )
            for f in range(2)
        ]
        derive(
            parts, slope_ref.at[k], zz_ref.at[k], xx_out.at[k], xz_out.at[k], two_ref, columns,
            field_ref[k, : 2 * rows, :],
        )

    def advance(i):
        w, s = items[i]
        k = i % 2
        for r in range(0, rows, 16):
            parts = []
            for h in (r, r + 8):
                at = slice(h, h + 8)
                mix, twist, a, b = (ref[at, :] for ref in coefficient_refs[:4])

                def operator(f, value):
                    here = slice(f * rows + h, f * rows + h + 8)
                    return tilted(
                        f, value, zz_ref[k, here, :], xx_out[k, here, :], xz_out[k, here, :], mix, twist
                    )

                p, q = (current(i, f, h) for f in range(2))
                across, along = (operator(0, p), operator(1, q))
                parts.append((2.0 * p - wave_ref[w, 0, s, at, :]) + (a * across + b * along))
            value = jnp.concatenate(parts, axis=0)
            top = value.astype(BF16)
            split_ref[k, r : r + 16, :] = top
            split_ref[k, rows + r : rows + r + 16, :] = (value - top.astype(F32)).astype(BF16)
            split_ref[k, 2 * rows + r : 2 * rows + r + 16, :] = top

    def transform(i):
        spectra = jnp.dot(depth_ref[...], split_ref[i % 2], preferred_element_type=F32)
        for part in range(2):
            for m in range(per_slab):
                start = 16 * part + per_slab * i + m
                spectra_ref[pl.ds(start, bins, stride=PITCH), :] = spectra[
                    part * bins : (part + 1) * bins, m * LANES : (m + 1) * LANES
                ]

    for i in range(len(items)):
        edge_advance(i)
    matmuls(0)
    for i in range(1, len(items)):
        matmuls(i)
        advance(i - 1)
        transform(i - 1)
    advance(len(items) - 1)
    transform(len(items) - 1)

    left_lane = lax.broadcasted_iota(jnp.int32, (8, LANES), 1) < LANES // 2
    alive = alive_ref[...]
    for j in range(bins // RUN):
        slot = j % 2
        for r in range(0, LANES, 16):
            at = slice(r, r + 16)
            one = (low_c[at, :], low_s[at, :])
            back = (high_c[j, at, :], high_s[j, at, :])
            here = (back[0] * one[0] - back[1] * one[1], back[0] * one[1] + back[1] * one[0])
            twice = 2.0 * one[0]
            for i in range(RUN):
                slant_ref[slot, i, at, :] = back[0].astype(BF16)
                slant_ref[slot, i, LANES + r : LANES + r + 16, :] = back[1].astype(BF16)
                back, here = here, tuple(twice * x - y for x, y in zip(here, back, strict=True))
        pair = []
        for i in range(RUN):
            at = (RUN * j + i) * PITCH
            left = jnp.concatenate(
                [spectra_ref[at : at + 16, :], spectra_ref[at + 16 : at + 32, :]], axis=1
            ).astype(BF16)
            stack = jnp.dot(left, slant_ref[slot, i], preferred_element_type=F32)
            product = stack[:8] * stack[8:]
            pair.append(product + pltpu.roll(product, 4, 0))
            if i % 2 == 1:
                even, odd = pair
                even = even + pltpu.roll(even, LANES // 2, 1)
                odd = odd + pltpu.roll(odd, LANES // 2, 1)
                pair = []
                where_to = (RUN * j + i) // 2 * LANES
                image_ref[:, where_to : where_to + LANES] = alive * jnp.where(left_lane, even, odd)
    out_ref[...] = image_ref[:per_slab, :].astype(BF16)


def column_operands():
    return [jnp.asarray(t, dtype=BF16) for kind in (2, 1) for t in column_tables(kind)]


def early(wavefields, params, slab_counts, angle_table):
    two, _, shots, rows, cols = wavefields.shape
    field = pltpu.VMEM((rows, cols), F32)
    table = pltpu.VMEM((rows // 2 // RUN, LANES, LANES), F32)
    own = jnp.asarray(row_tables(rows)[0], dtype=BF16)
    args = [wavefields, *params, angle_table.reshape(1, -1), own, *column_operands()]
    outs = [field] * 5 + [pltpu.VMEM((LANES, LANES), F32)] * 2 + [table] * 2 + [
        pltpu.VMEM((8, LANES), F32),
        pltpu.VMEM((two * shots, 2, rows, cols), F32),
    ]
    return pl.pallas_call(
        early_kernel,
        in_specs=[pl.BlockSpec(memory_space=pltpu.SMEM)] + [VMEM_WHOLE] * len(args),
        out_specs=[VMEM_WHOLE] * len(outs),
        out_shape=outs,
        scratch_shapes=[
            pltpu.VMEM((2, 2 * rows, cols), BF16),
            pltpu.VMEM((2, 2 * rows, cols), BF16),
            pltpu.VMEM((2, 2 * rows, cols), F32),
            pltpu.VMEM((2, 2 * rows, cols), F32),
            pltpu.VMEM((2, 2 * rows, cols), F32),
        ],
        compiler_params=pltpu.CompilerParams(vmem_limit_bytes=24 << 20),
        name="early",
    )(slab_counts, *in_vmem(*args))


def late(wavefields, partner, neighbour, prepared, angles):
    two, _, shots, rows, cols = wavefields.shape
    bins = rows // 2
    per_slab = cols // rows
    items = two * shots
    _, edge, both = (jnp.asarray(t, dtype=BF16) for t in row_tables(rows))
    depth = depth_table(rows, bins)
    depth_top = depth.astype(jnp.bfloat16)
    depth_low = (depth - depth_top.astype(np.float32)).astype(jnp.bfloat16)
    depth = jnp.asarray(np.concatenate([depth_top, depth_top, depth_low], axis=1), dtype=BF16)
    args = [wavefields, partner, neighbour, *prepared, edge, both, *column_operands(), depth]
    out_shape = (per_slab, bins * angles)
    scratch = [
        pltpu.VMEM((items, 2, 48, cols), BF16),
        pltpu.VMEM((items * 2 * 32, cols), BF16),
        pltpu.VMEM((items * 2 * 32, cols), BF16),
        pltpu.VMEM((items * 2 * 32, cols), F32),
        pltpu.VMEM((items * 2 * 32, cols), F32),
        pltpu.VMEM((items * 2 * 32, cols), F32),
        pltpu.VMEM((items, 2, 24, cols), F32),
        pltpu.VMEM((2, 2 * (rows + 16), cols), BF16),
        pltpu.VMEM((2, 2 * rows, cols), BF16),
        pltpu.VMEM((2, 2 * rows, cols), F32),
        pltpu.VMEM((2, 2 * rows, cols), F32),
        pltpu.VMEM((2, 2 * rows, cols), F32),
        pltpu.VMEM((2, 3 * rows, cols), BF16),
        pltpu.VMEM((PITCH * bins, LANES), F32),
        pltpu.VMEM((8, bins * angles), F32),
        pltpu.VMEM((2, RUN, 2 * LANES, LANES), BF16),
    ]
    return pl.pallas_call(
        late_kernel,
        in_specs=[VMEM_WHOLE] * len(args),
        out_specs=VMEM_WHOLE,
        out_shape=pltpu.VMEM(out_shape, BF16),
        scratch_shapes=scratch,
        compiler_params=pltpu.CompilerParams(vmem_limit_bytes=32 << 20),
        name="late",
    )(*in_vmem(*args))


def pick_kernel(loc_ref, *refs, per_slab):
    held_refs, (mine_ref, theirs_ref) = (refs[:-2], refs[-2:])
    slab = lax.axis_index(SLAB)
    chip, core = (lax.axis_index("chip"), lax.axis_index("core"))
    chips = lax.axis_size("chip")
    count = mine_ref.shape[0]
    per_row = LANES // count
    row = loc_ref[pl.ds(slab // per_row, 1), :]
    spot = slab % per_row
    partner = spot + 1 - 2 * core
    loc = jnp.concatenate(
        [pltpu.roll(row, (LANES - s * count) % LANES, 1)[:, :count] for s in (spot, partner)], axis=1
    )
    owner = loc // per_slab
    ahead = lax.rem(owner // 2 - chip + chips, chips)
    up = ahead <= chips // 2
    hops = jnp.where(up, ahead, chips - ahead)
    holder = jnp.where(hops == chips // 2, owner % 2, jnp.where(up, 1, 0))
    index = (2 * (hops // len(NEAR)) + jnp.where(owner % 2 == holder, 0, 1)) * per_slab + loc % per_slab
    total = None
    for near, ref in enumerate(held_refs):
        held = lax.broadcasted_iota(jnp.int32, (ref.shape[0], 2 * count), 0)
        hit = (held == index) & (holder == core) & (hops % len(NEAR) == near)
        hot = jnp.where(hit, 1.0, 0.0).astype(BF16)
        part = lax.dot_general(hot, ref[...], (((0,), (0,)), ((), ())), preferred_element_type=F32)
        total = part if total is None else total + part
    mine_ref[...] = total[:count]
    theirs_ref[...] = total[count:].astype(BF16)


def pick(loc_patch, held, count, per_slab):
    width = held[0].shape[1]
    return pl.pallas_call(
        lambda *refs: pick_kernel(*refs, per_slab=per_slab),
        in_specs=[VMEM_WHOLE] * (1 + len(held)),
        out_specs=[VMEM_WHOLE] * 2,
        out_shape=[pltpu.VMEM((count, width), F32), pltpu.VMEM((count, width), BF16)],
        compiler_params=pltpu.CompilerParams(vmem_limit_bytes=8 << 20),
        name="pick",
    )(*in_vmem(loc_patch.reshape(-1, LANES), *held))


def swap_cores(array):
    return lax.ppermute(array, "core", [(0, 1), (1, 0)])


def onward(array, hops):
    chips = lax.axis_size("chip")
    pairs = [(2 * i, 2 * ((i + hops) % chips)) for i in range(chips)]
    pairs += [(2 * i + 1, 2 * ((i - hops) % chips) + 1) for i in range(chips)]
    return lax.ppermute(array, SLAB, pairs)


def spread(images):
    held = jnp.concatenate([images, swap_cores(images)])
    held = jnp.concatenate([held] + [onward(held, h) for h in FAR[1:]])
    short = held[: held.shape[0] - images.shape[0]]
    return [held] + [onward(short if h == NEAR[-1] else held, h) for h in NEAR[1:]]


def per_device(
    wavefields, courant, epsilon, anisotropy_delta, tilt_angle, loc_patch, slab_counts, angle_table
):
    slabs = lax.axis_size(SLAB)
    assert FAR[-1] + NEAR[-1] == slabs // 4
    per_slab = wavefields.shape[4] // wavefields.shape[3]
    params = (courant, epsilon, anisotropy_delta, tilt_angle)
    to_partner, to_neighbour = pack(wavefields, params)
    pairs = [(i, i + 1) for i in range(1, slabs - 1, 2)]
    neighbour = lax.ppermute(to_neighbour, SLAB, pairs + [(j, i) for i, j in pairs])
    partner = swap_cores(to_partner)
    prepared = early(wavefields, params, slab_counts, angle_table)
    images = late(wavefields, partner, neighbour, prepared, angle_table.shape[0])
    mine, theirs = pick(loc_patch, spread(images), loc_patch.shape[0] // slabs, per_slab)
    return mine + swap_cores(theirs).astype(F32)


def solution(mesh):
    shape = (mesh.shape["groups"], mesh.shape["slab"] // 2, 2)
    finer = Mesh(mesh.devices.reshape(shape), GROUPS_SLAB)
    in_specs = (
        P(None, None, "groups", SLAB, None),
        P(SLAB, None),
        P(SLAB, None),
        P(SLAB, None),
        P(SLAB, None),
        P(),
        P(),
        P(),
    )
    out_specs = P(GROUPS_SLAB, None)
    return jax.shard_map(
        per_device, mesh=finer, in_specs=in_specs, out_specs=out_specs, check_vma=False
    )
```

```python
import math

import jax
import jax.numpy as jnp
import numpy as np
from jax import lax
from jax.experimental import pallas as pl
from jax.experimental.pallas import tpu as pltpu
from jax.sharding import Mesh
from jax.sharding import PartitionSpec as P


SLAB = ("chip", "core")
GROUPS_SLAB = ("groups", "chip", "core")
LANES = 128
HALF = 4
RUN = 8
PITCH = 40
FAR, NEAR = ((0, 3, 6), (0, 1, 2))
SECOND = (-14336.0, 8064.0, -1008.0, 128.0, -9.0)
SECOND_REST = 14.0
SECOND_UNIT = 5040.0
FIRST = (672.0, -168.0, 32.0, -3.0)
FIRST_UNIT = 840.0
BF16 = jnp.bfloat16
F32 = jnp.float32
VMEM_WHOLE = pl.BlockSpec(memory_space=pltpu.VMEM)


def in_vmem(*arrays):
    return [pltpu.with_memory_space_constraint(a, pltpu.VMEM) for a in arrays]


def weight(kind, offset):
    if abs(offset) > HALF:
        return 0.0
    if kind == 2:
        return SECOND[abs(offset)]
    if offset == 0:
        return 0.0
    return FIRST[abs(offset) - 1] * (1.0 if offset > 0 else -1.0)


def band(kind, outputs, inputs):
    table = np.zeros((len(outputs), len(inputs)), np.float32)
    for i, o in enumerate(outputs):
        for j, n in enumerate(inputs):
            if o is not None and n is not None:
                table[i, j] = weight(kind, n - o)
    return table


def row_tables(rows):
    own = list(range(rows))
    inner = list(range(-HALF, 0)) + list(range(rows, rows + HALF))
    outer = list(range(-2 * HALF, -HALF)) + list(range(rows + HALF, rows + 2 * HALF))
    pad = [None] * 8
    ends = own[:8] + own[-8:]
    edge_in = ends + inner + outer + own[8:16] + own[-16:-8]
    edge_out = ends + inner + pad
    second_in = own + inner + pad
    tables = ((own, own), (edge_out, edge_in), (own, second_in))
    return [np.concatenate([band(2, o, i), band(1, o, i)]) for o, i in tables]


def column_tables(kind):
    block = list(range(2 * LANES))
    inside = band(kind, block, block).T
    across = np.zeros((2 * LANES, 2 * LANES), np.float32)
    for i in range(2 * LANES):
        for o in range(2 * LANES):
            if (i < LANES) != (o < LANES):
                across[i, o] = weight(kind, i - o)
    return inside, across


def depth_table(patch, bins):
    k = np.arange(bins)[:, None]
    z = np.arange(patch)[None, :]
    phase = (2.0 * math.pi / patch * np.mod(k * z, patch)).astype(np.float32)
    table = np.concatenate([np.cos(phase), -np.sin(phase)]).astype(np.float32) * np.float32(1.0 / math.sqrt(patch))
    return table.astype(np.float32)


def quarter_turns(quarter, cosine, sine):
    odd = (quarter & 1) == 1
    c = jnp.where(odd, sine, cosine)
    s = jnp.where(odd, cosine, sine)
    c = jnp.where(((quarter + 1) & 2) == 2, -c, c)
    s = jnp.where((quarter & 2) == 2, -s, s)
    return c, s


def small_cos_sin(y):
    y2 = y * y
    s = y * (1.0 + y2 * (-1.6666654611e-1 + y2 * (8.3321608736e-3 + y2 * -1.9515295891e-4)))
    c = 1.0 - 0.5 * y2 + y2 * y2 * (4.166664568298827e-2 + y2 * (-1.388731625493765e-3 + y2 * 2.443315711809948e-5))
    return c, s


def double_angle(theta):
    n = jnp.floor(theta * (4.0 / math.pi) + 0.5)
    y = 2.0 * theta - n * 1.5703125
    y = y - n * 4.837512969970703e-4
    y = y - n * 7.54978995489188216e-8
    c, s = small_cos_sin(y)
    return quarter_turns(n.astype(jnp.int32), c, s)


def pack_kernel(
    w_top, w_bot, c_top, c_bot, e_top, e_bot, d_top, d_bot, t_top, t_bot, partner_ref, neighbour_ref
):
    low = lax.broadcasted_iota(jnp.int32, (8, w_top.shape[-1]), 0) < HALF

    def half_turn(x):
        return pltpu.roll(x, HALF, 0)

    def emit(out, wave, params, upward):
        def join(a, b):
            return jnp.where(low, half_turn(a), b) if upward else jnp.where(low, a, half_turn(b))

        groups = []
        for w in range(wave.shape[0]):
            for s in range(wave.shape[2]):
                groups.append(wave[w, 0, s])
                groups.append(wave[w, 1, s])
                groups.append(join(wave[w, 2, s], wave[w, 3, s]))
        courant, eps, delta, tilt = (p[...] for p in params)
        high = tilt.astype(BF16).astype(F32)
        groups += [join(courant, eps), join(delta, high), tilt - high]
        groups.append(groups[-1])
        for g in range(0, len(groups), 2):
            out[8 * g : 8 * g + 16, :] = jnp.concatenate(groups[g : g + 2], axis=0).astype(BF16)

    tops = (w_top, (c_top, e_top, d_top, t_top))
    bottoms = (w_bot, (c_bot, e_bot, d_bot, t_bot))
    first = lax.axis_index("core") == 0

    @pl.when(first)
    def _():
        emit(partner_ref, *bottoms, True)
        emit(neighbour_ref, *tops, False)

    @pl.when(jnp.logical_not(first))
    def _():
        emit(partner_ref, *tops, False)
        emit(neighbour_ref, *bottoms, True)


def pack(wavefields, params):
    two, four, shots, rows, cols = wavefields.shape
    last = rows // 8 - 1
    groups = 2 * shots * 3 + 4
    wave_block = (two, four, shots, 8, cols)
    specs = [
        pl.BlockSpec(wave_block, lambda i: (0, 0, 0, 0, 0)),
        pl.BlockSpec(wave_block, lambda i: (0, 0, 0, last, 0)),
    ]
    args = [wavefields, wavefields]
    for p in params:
        specs += [pl.BlockSpec((8, cols), lambda i: (0, 0)), pl.BlockSpec((8, cols), lambda i: (last, 0))]
        args += [p, p]
    out = pltpu.VMEM((8 * groups, cols), BF16)
    return pl.pallas_call(
        pack_kernel,
        grid=(1,),
        in_specs=specs,
        out_specs=[VMEM_WHOLE] * 2,
        out_shape=[out, out],
        compiler_params=pltpu.CompilerParams(vmem_limit_bytes=8 << 20),
        name="pack",
    )(*(pltpu.with_memory_space_constraint(a, pltpu.HBM) for a in args))


def coefficients(courant, eps, delta, tilt):
    cosine, sine = double_angle(tilt)
    scaled = courant * (1.0 / SECOND_UNIT)
    stretch = 1.0 + 2.0 * delta
    return (
        0.5 + 0.5 * cosine,
        sine * (SECOND_UNIT / (FIRST_UNIT * FIRST_UNIT)),
        scaled * (1.0 + 2.0 * eps),
        scaled * (stretch * lax.rsqrt(stretch)),
        scaled,
    )


class Filler:
    def __init__(self, jobs, points):
        self.jobs, self.points, self.done, self.calls = (jobs, points, 0, 0)

    def __call__(self):
        self.calls += 1
        self.upto(-(-len(self.jobs) * self.calls // self.points))

    def upto(self, count):
        for job in self.jobs[self.done : count]:
            job()
        self.done = max(self.done, min(count, len(self.jobs)))

    def finish(self):
        self.upto(len(self.jobs))


def along_columns(out, source, inside, across, fill):
    out[:, LANES : 3 * LANES] = jnp.dot(source[:, LANES : 3 * LANES], across[...], preferred_element_type=F32)
    fill()
    left = jnp.dot(source[:, : 2 * LANES], inside[...], preferred_element_type=F32)
    out[:, :LANES] = left[:, :LANES]
    out[:, LANES : 2 * LANES] += left[:, LANES:]
    fill()
    right = jnp.dot(source[:, 2 * LANES :], inside[...], preferred_element_type=F32)
    out[:, 2 * LANES : 3 * LANES] += right[:, :LANES]
    out[:, 3 * LANES :] = right[:, LANES:]
    fill()


def derive(field, slope, zz, xx, xz, table, columns, fields, fill):
    count = table.shape[0] // 2
    for f in range(2):
        source = field[f]
        product = jnp.dot(table[count:, :], source, preferred_element_type=F32)
        slope[f * count : (f + 1) * count, :] = product.astype(BF16)
        fill()
        zz[f * count : (f + 1) * count, :] = jnp.dot(table[:count, :], source, preferred_element_type=F32)
        fill()
    along_columns(xx, fields, columns[0], columns[1], fill)
    along_columns(xz, slope[...], columns[2], columns[3], fill)


def tilted(f, value, zz, xx, xz, mix, twist):
    turn = mix * (xx - zz) - twist * xz
    rest = SECOND_REST * value
    return (zz + turn) - rest if f == 0 else (xx - turn) - rest


def early_kernel(
    counts_ref, wave_ref, courant_ref, eps_ref, delta_ref, tilt_ref, angle_ref, own_ref,
    xx_ref, xx_across_ref, x_ref, x_across_ref,
    mix_ref, twist_ref, a_ref, b_ref, c_ref, low_c, low_s, high_c, high_s, alive_ref, next_ref,
    field_ref, slope_ref, zz_ref, xx_out, xz_out,
):
    rows, _ = courant_ref.shape
    wavefields, _, shots = wave_ref.shape[:3]
    columns = (xx_ref, xx_across_ref, x_ref, x_across_ref)
    items = [(w, s) for w in range(wavefields) for s in range(shots)]

    def coefficient_job(r):
        def job():
            at = slice(r, r + 8)
            values = coefficients(courant_ref[at, :], eps_ref[at, :], delta_ref[at, :], tilt_ref[at, :])
            for ref, value in zip((mix_ref, twist_ref, a_ref, b_ref, c_ref), values, strict=True):
                ref[at, :] = value

        return job

    fill = Filler([coefficient_job(r) for r in range(0, rows, 8)], 20)

    def matmuls(i):
        w, s = items[i]
        k = i % 2
        for f in range(2):
            field_ref[k, f * rows : (f + 1) * rows, :] = wave_ref[w, f, s].astype(BF16)
        parts = [field_ref.at[k, f * rows : (f + 1) * rows, :][...] for f in range(2)]
        derive(
            parts, slope_ref.at[k], zz_ref.at[k], xx_out.at[k], xz_out.at[k], own_ref, columns,
            field_ref.at[k][...], fill,
        )

    def advance(i):
        w, s = items[i]
        k = i % 2
        for r in range(8, rows - 8, 8):
            at = slice(r, r + 8)
            p, q, p0, q0 = (wave_ref[w, f, s, at, :] for f in range(4))
            mix, twist = (mix_ref[at, :], twist_ref[at, :])

            def operator(f, value):
                here = slice(f * rows + r, f * rows + r + 8)
                return tilted(f, value, zz_ref[k, here, :], xx_out[k, here, :], xz_out[k, here, :], mix, twist)

            across, along = (operator(0, p), operator(1, q))
            a, b, c = (a_ref[at, :], b_ref[at, :], c_ref[at, :])
            next_ref[i, 0, at, :] = (2.0 * p - p0) + (a * across + b * along)
            next_ref[i, 1, at, :] = (2.0 * q - q0) + (b * across + c * along)

    @pl.when(lax.axis_index("core") >= 0)
    def _():
        matmuls(0)
        matmuls(1)
        fill.finish()
        slant_factors(angle_ref, low_c, low_s, high_c, high_s)

    @pl.when(lax.axis_index("core") >= 0)
    def _():
        advance(0)
        matmuls(2)

    @pl.when(lax.axis_index("core") >= 0)
    def _():
        advance(1)
        matmuls(3)

    advance(2)
    advance(len(items) - 1)
    live = lax.broadcasted_iota(jnp.int32, (8, LANES), 0) < counts_ref[lax.axis_index(SLAB)]
    alive_ref[...] = jnp.where(live, 1.0, 0.0)


def slant_factors(angle_ref, low_c, low_s, high_c, high_s):
    right_half = lax.broadcasted_iota(jnp.int32, (LANES, LANES), 1) >= LANES // 2
    angles = jnp.concatenate([angle_ref[...], angle_ref[...]], axis=1)
    lateral = lax.broadcasted_iota(jnp.int32, (LANES, LANES), 0)
    modulus = 16 * LANES
    turn = (lateral * angles) & (modulus - 1)
    quarter = (turn + modulus // 8) >> int(math.log2(modulus // 4))
    rest = turn - quarter * (modulus // 4)
    c1, s1 = small_cos_sin(rest.astype(F32) * (2.0 * math.pi / modulus))
    c1, s1 = quarter_turns(quarter, c1, s1)

    def times(x, y):
        return (x[0] * y[0] - x[1] * y[1], x[0] * y[1] + x[1] * y[0])

    low_c[...], low_s[...] = (c1, s1)
    stride = (c1, s1)
    for _ in range(int(math.log2(RUN))):
        stride = times(stride, stride)
    scale = 1.0 / math.sqrt(LANES)
    value = (jnp.where(right_half, 0.0, scale), jnp.where(right_half, scale, 0.0))
    for j in range(high_c.shape[0]):
        high_c[j], high_s[j] = value
        value = times(value, stride)


def late_kernel(
    wave_ref, partner_ref, neighbour_ref, mix_ref, twist_ref, a_ref, b_ref, c_ref,
    low_c, low_s, high_c, high_s, alive_ref, next_ref,
    edge_table_ref, two_ref, xx_ref, xx_across_ref, x_ref, x_across_ref, depth_ref,
    out_ref,
    edge_z, edge_x, edge_slope, edge_zz, edge_xx, edge_xz, edge_next,
    field_ref, slope_ref, zz_ref, xx_out, xz_out, split_ref, spectra_ref, image_ref, slant_ref,
):
    wavefields, _, shots, rows, cols = wave_ref.shape
    bins = rows // 2
    per_slab = cols // LANES
    columns = (xx_ref, xx_across_ref, x_ref, x_across_ref)
    items = [(w, s) for w in range(wavefields) for s in range(shots)]
    low = lax.broadcasted_iota(jnp.int32, (8, cols), 0) < HALF
    first = lax.axis_index("core") == 0
    coefficient_refs = (mix_ref, twist_ref, a_ref, b_ref, c_ref)

    def half_turn(x):
        return pltpu.roll(x, HALF, 0)

    def group(g):
        at = slice(8 * g, 8 * g + 8)
        a, b = (partner_ref[at, :].astype(F32), neighbour_ref[at, :].astype(F32))
        return jnp.where(first, b, a), jnp.where(first, a, b)

    def first_halves(g):
        u, d = group(g)
        return jnp.where(low, u, half_turn(d))

    def second_halves(g):
        u, d = group(g)
        return jnp.where(low, half_turn(u), d)

    def slant_job(j, r):
        def job():
            at = slice(r, r + 16)
            one = (low_c[at, :], low_s[at, :])
            back = (high_c[j, at, :], high_s[j, at, :])
            here = (back[0] * one[0] - back[1] * one[1], back[0] * one[1] + back[1] * one[0])
            twice = 2.0 * one[0]
            for i in range(RUN):
                slant_ref[RUN * j + i, at, :] = back[0].astype(BF16)
                slant_ref[RUN * j + i, LANES + r : LANES + r + 16, :] = back[1].astype(BF16)
                back, here = here, tuple(twice * x - y for x, y in zip(here, back, strict=True))

        return job

    jobs = [slant_job(j, r) for j in range(bins // RUN) for r in range(0, LANES, 16)]
    fill = Filler(jobs, 6 + 10 * len(items))

    def current(i, f, r):
        if r == 0:
            return edge_next[i, f, 0:8, :]
        if r == rows - 8:
            return edge_next[i, f, 8:16, :]
        return next_ref[i, f, r : r + 8, :]

    def matmuls(i):
        k = i % 2
        for f in range(2):
            for r in range(0, rows, 16):
                pair = jnp.concatenate([current(i, f, r), current(i, f, r + 8)], axis=0)
                pair = pair.astype(BF16)
                field_ref[k, f * rows + r : f * rows + r + 16, :] = pair
            edge = edge_next[i, f, 16:24, :]
            pair = jnp.concatenate([edge, jnp.zeros_like(edge)], axis=0).astype(BF16)
            field_ref[k, 2 * rows + 16 * f : 2 * rows + 16 * f + 16, :] = pair
        parts = [
            jnp.concatenate(
                [
                    field_ref[k, f * rows : (f + 1) * rows, :],
                    field_ref[k, 2 * rows + 16 * f : 2 * rows + 16 * f + 16, :],
                ],
                axis=0,
            )
            for f in range(2)
        ]
        derive(
            parts, slope_ref.at[k], zz_ref.at[k], xx_out.at[k], xz_out.at[k], two_ref, columns,
            field_ref[k, : 2 * rows, :], fill,
        )

    def advance(i):
        w, s = items[i]
        k = i % 2
        for r in range(0, rows, 16):
            parts = []
            for h in (r, r + 8):
                at = slice(h, h + 8)
                mix, twist, a, b = (ref[at, :] for ref in coefficient_refs[:4])

                def operator(f, value):
                    here = slice(f * rows + h, f * rows + h + 8)
                    return tilted(
                        f, value, zz_ref[k, here, :], xx_out[k, here, :], xz_out[k, here, :], mix, twist
                    )

                p, q = (current(i, f, h) for f in range(2))
                across, along = (operator(0, p), operator(1, q))
                parts.append((2.0 * p - wave_ref[w, 0, s, at, :]) + (a * across + b * along))
            value = jnp.concatenate(parts, axis=0)
            top = value.astype(BF16)
            split_ref[k, r : r + 16, :] = top
            split_ref[k, rows + r : rows + r + 16, :] = (value - top.astype(F32)).astype(BF16)
            split_ref[k, 2 * rows + r : 2 * rows + r + 16, :] = top

    def transform(i):
        spectra = jnp.dot(depth_ref[...], split_ref[i % 2], preferred_element_type=F32)
        for part in range(2):
            for m in range(per_slab):
                start = 16 * part + per_slab * i + m
                spectra_ref[pl.ds(start, bins, stride=PITCH), :] = spectra[
                    part * bins : (part + 1) * bins, m * LANES : (m + 1) * LANES
                ]

    @pl.when(lax.axis_index("core") >= 0)
    def _():
        tall = 32
        halos = []
        for i, (w, s) in enumerate(items):
            halo = []
            for f in range(2):
                u, d = group(3 * i + f)
                inner = jnp.where(low, half_turn(u), half_turn(d))
                outer = jnp.where(low, u, d)
                halo.append(inner)
                pieces = (
                    wave_ref[w, f, s, 0:8, :], wave_ref[w, f, s, rows - 8 : rows, :], inner, outer,
                    wave_ref[w, f, s, 8:16, :], wave_ref[w, f, s, rows - 16 : rows - 8, :],
                )
                for n in range(0, 6, 2):
                    pair = jnp.concatenate(pieces[n : n + 2], axis=0).astype(BF16)
                    edge_z[i, f, 8 * n : 8 * n + 16, :] = pair
                    if n < 4:
                        at = (2 * i + f) * tall + 8 * n
                        edge_x[at : at + 16, :] = pair
            halo += [first_halves(3 * i + 2), second_halves(3 * i + 2)]
            halos.append(halo)
        for i in range(len(items)):
            for f in range(2):
                product = jnp.dot(edge_table_ref[...], edge_z[i, f], preferred_element_type=F32)
                at = (2 * i + f) * tall
                edge_zz[at : at + tall, :] = product[:tall]
                edge_slope[at : at + tall, :] = product[tall:].astype(BF16)
        along_columns(edge_xx, edge_x[...], xx_ref, xx_across_ref, fill)
        along_columns(edge_xz, edge_slope[...], x_ref, x_across_ref, fill)
        g = 3 * len(items)
        beyond = coefficients(
            first_halves(g), second_halves(g), first_halves(g + 1), second_halves(g + 1) + first_halves(g + 2)
        )

        def edge_advance(i):
            w, s = items[i]
            for n, r in enumerate((0, rows - 8, None)):
                if r is None:
                    fields = halos[i]
                    mix, twist, a, b, c = beyond
                else:
                    at = slice(r, r + 8)
                    fields = [wave_ref[w, f, s, at, :] for f in range(4)]
                    mix, twist, a, b, c = (ref[at, :] for ref in coefficient_refs)
                p, q, p0, q0 = fields

                def operator(f, value):
                    here = slice((2 * i + f) * tall + 8 * n, (2 * i + f) * tall + 8 * n + 8)
                    return tilted(f, value, edge_zz[here, :], edge_xx[here, :], edge_xz[here, :], mix, twist)

                across, along = (operator(0, p), operator(1, q))
                edge_next[i, 0, 8 * n : 8 * n + 8, :] = (2.0 * p - p0) + (a * across + b * along)
                edge_next[i, 1, 8 * n : 8 * n + 8, :] = (2.0 * q - q0) + (b * across + c * along)

        for i in range(len(items)):
            edge_advance(i)
        matmuls(0)
        for i in range(1, 4):
            matmuls(i)
            advance(i - 1)
            transform(i - 1)
        fill.finish()

    for i in range(4, len(items)):
        matmuls(i)
        advance(i - 1)
        transform(i - 1)
    advance(len(items) - 1)
    transform(len(items) - 1)

    left_lane = lax.broadcasted_iota(jnp.int32, (8, LANES), 1) < LANES // 2
    alive = alive_ref[...]
    for j in range(bins // RUN):
        pair = []
        for i in range(RUN):
            at = (RUN * j + i) * PITCH
            left = jnp.concatenate(
                [spectra_ref[at : at + 16, :], spectra_ref[at + 16 : at + 32, :]], axis=1
            ).astype(BF16)
            stack = jnp.dot(left, slant_ref[RUN * j + i], preferred_element_type=F32)
            product = stack[:8] * stack[8:]
            pair.append(product + pltpu.roll(product, 4, 0))
            if i % 2 == 1:
                even, odd = pair
                even = even + pltpu.roll(even, LANES // 2, 1)
                odd = odd + pltpu.roll(odd, LANES // 2, 1)
                pair = []
                where_to = (RUN * j + i) // 2 * LANES
                image_ref[:, where_to : where_to + LANES] = alive * jnp.where(left_lane, even, odd)
    out_ref[...] = image_ref[:per_slab, :].astype(BF16)


def column_operands():
    return [jnp.asarray(t, dtype=BF16) for kind in (2, 1) for t in column_tables(kind)]


def early(wavefields, params, slab_counts, angle_table):
    two, _, shots, rows, cols = wavefields.shape
    field = pltpu.VMEM((rows, cols), F32)
    table = pltpu.VMEM((rows // 2 // RUN, LANES, LANES), F32)
    own = jnp.asarray(row_tables(rows)[0], dtype=BF16)
    args = [wavefields, *params, angle_table.reshape(1, -1), own, *column_operands()]
    outs = [field] * 5 + [pltpu.VMEM((LANES, LANES), F32)] * 2 + [table] * 2 + [
        pltpu.VMEM((8, LANES), F32),
        pltpu.VMEM((two * shots, 2, rows, cols), F32),
    ]
    return pl.pallas_call(
        early_kernel,
        in_specs=[pl.BlockSpec(memory_space=pltpu.SMEM)] + [VMEM_WHOLE] * len(args),
        out_specs=[VMEM_WHOLE] * len(outs),
        out_shape=outs,
        scratch_shapes=[
            pltpu.VMEM((2, 2 * rows, cols), BF16),
            pltpu.VMEM((2, 2 * rows, cols), BF16),
            pltpu.VMEM((2, 2 * rows, cols), F32),
            pltpu.VMEM((2, 2 * rows, cols), F32),
            pltpu.VMEM((2, 2 * rows, cols), F32),
        ],
        compiler_params=pltpu.CompilerParams(vmem_limit_bytes=24 << 20),
        name="early",
    )(slab_counts, *in_vmem(*args))


def late(wavefields, partner, neighbour, prepared, angles):
    two, _, shots, rows, cols = wavefields.shape
    bins = rows // 2
    per_slab = cols // rows
    items = two * shots
    _, edge, both = (jnp.asarray(t, dtype=BF16) for t in row_tables(rows))
    depth = depth_table(rows, bins)
    depth_top = depth.astype(jnp.bfloat16)
    depth_low = (depth - depth_top.astype(np.float32)).astype(jnp.bfloat16)
    depth = jnp.asarray(np.concatenate([depth_top, depth_top, depth_low], axis=1), dtype=BF16)
    args = [wavefields, partner, neighbour, *prepared, edge, both, *column_operands(), depth]
    out_shape = (per_slab, bins * angles)
    scratch = [
        pltpu.VMEM((items, 2, 48, cols), BF16),
        pltpu.VMEM((items * 2 * 32, cols), BF16),
        pltpu.VMEM((items * 2 * 32, cols), BF16),
        pltpu.VMEM((items * 2 * 32, cols), F32),
        pltpu.VMEM((items * 2 * 32, cols), F32),
        pltpu.VMEM((items * 2 * 32, cols), F32),
        pltpu.VMEM((items, 2, 24, cols), F32),
        pltpu.VMEM((2, 2 * (rows + 16), cols), BF16),
        pltpu.VMEM((2, 2 * rows, cols), BF16),
        pltpu.VMEM((2, 2 * rows, cols), F32),
        pltpu.VMEM((2, 2 * rows, cols), F32),
        pltpu.VMEM((2, 2 * rows, cols), F32),
        pltpu.VMEM((2, 3 * rows, cols), BF16),
        pltpu.VMEM((PITCH * bins, LANES), F32),
        pltpu.VMEM((8, bins * angles), F32),
        pltpu.VMEM((bins, 2 * LANES, LANES), BF16),
    ]
    return pl.pallas_call(
        late_kernel,
        in_specs=[VMEM_WHOLE] * len(args),
        out_specs=VMEM_WHOLE,
        out_shape=pltpu.VMEM(out_shape, BF16),
        scratch_shapes=scratch,
        compiler_params=pltpu.CompilerParams(vmem_limit_bytes=36 << 20),
        name="late",
    )(*in_vmem(*args))


def pick_kernel(loc_ref, *refs, per_slab):
    held_refs, (mine_ref, theirs_ref) = (refs[:-2], refs[-2:])
    slab = lax.axis_index(SLAB)
    chip, core = (lax.axis_index("chip"), lax.axis_index("core"))
    chips = lax.axis_size("chip")
    count = mine_ref.shape[0]
    per_row = LANES // count
    row = loc_ref[pl.ds(slab // per_row, 1), :]
    spot = slab % per_row
    partner = spot + 1 - 2 * core
    loc = jnp.concatenate(
        [pltpu.roll(row, (LANES - s * count) % LANES, 1)[:, :count] for s in (spot, partner)], axis=1
    )
    owner = loc // per_slab
    ahead = lax.rem(owner // 2 - chip + chips, chips)
    up = ahead <= chips // 2
    hops = jnp.where(up, ahead, chips - ahead)
    holder = jnp.where(hops == chips // 2, owner % 2, jnp.where(up, 1, 0))
    index = (2 * (hops // len(NEAR)) + jnp.where(owner % 2 == holder, 0, 1)) * per_slab + loc % per_slab
    total = None
    for near, ref in enumerate(held_refs):
        held = lax.broadcasted_iota(jnp.int32, (ref.shape[0], 2 * count), 0)
        hit = (held == index) & (holder == core) & (hops % len(NEAR) == near)
        hot = jnp.where(hit, 1.0, 0.0).astype(BF16)
        part = lax.dot_general(hot, ref[...], (((0,), (0,)), ((), ())), preferred_element_type=F32)
        total = part if total is None else total + part
    mine_ref[...] = total[:count]
    theirs_ref[...] = total[count:].astype(BF16)


def pick(loc_patch, held, count, per_slab):
    width = held[0].shape[1]
    return pl.pallas_call(
        lambda *refs: pick_kernel(*refs, per_slab=per_slab),
        in_specs=[VMEM_WHOLE] * (1 + len(held)),
        out_specs=[VMEM_WHOLE] * 2,
        out_shape=[pltpu.VMEM((count, width), F32), pltpu.VMEM((count, width), BF16)],
        compiler_params=pltpu.CompilerParams(vmem_limit_bytes=8 << 20),
        name="pick",
    )(*in_vmem(loc_patch.reshape(-1, LANES), *held))


def swap_cores(array):
    return lax.ppermute(array, "core", [(0, 1), (1, 0)])


def onward(array, hops):
    chips = lax.axis_size("chip")
    pairs = [(2 * i, 2 * ((i + hops) % chips)) for i in range(chips)]
    pairs += [(2 * i + 1, 2 * ((i - hops) % chips) + 1) for i in range(chips)]
    return lax.ppermute(array, SLAB, pairs)


def spread(images):
    held = jnp.concatenate([images, swap_cores(images)])
    held = jnp.concatenate([held] + [onward(held, h) for h in FAR[1:]])
    short = held[: held.shape[0] - images.shape[0]]
    return [held] + [onward(short if h == NEAR[-1] else held, h) for h in NEAR[1:]]


def per_device(
    wavefields, courant, epsilon, anisotropy_delta, tilt_angle, loc_patch, slab_counts, angle_table
):
    slabs = lax.axis_size(SLAB)
    assert FAR[-1] + NEAR[-1] == slabs // 4
    per_slab = wavefields.shape[4] // wavefields.shape[3]
    params = (courant, epsilon, anisotropy_delta, tilt_angle)
    to_partner, to_neighbour = pack(wavefields, params)
    pairs = [(i, i + 1) for i in range(1, slabs - 1, 2)]
    neighbour = lax.ppermute(to_neighbour, SLAB, pairs + [(j, i) for i, j in pairs])
    partner = swap_cores(to_partner)
    prepared = early(wavefields, params, slab_counts, angle_table)
    images = late(wavefields, partner, neighbour, prepared, angle_table.shape[0])
    mine, theirs = pick(loc_patch, spread(images), loc_patch.shape[0] // slabs, per_slab)
    return mine + swap_cores(theirs).astype(F32)


def solution(mesh):
    shape = (mesh.shape["groups"], mesh.shape["slab"] // 2, 2)
    finer = Mesh(mesh.devices.reshape(shape), GROUPS_SLAB)
    in_specs = (
        P(None, None, "groups", SLAB, None),
        P(SLAB, None),
        P(SLAB, None),
        P(SLAB, None),
        P(SLAB, None),
        P(),
        P(),
        P(),
    )
    out_specs = P(GROUPS_SLAB, None)
    return jax.shard_map(
        per_device, mesh=finer, in_specs=in_specs, out_specs=out_specs, check_vma=False
    )
```

```python
import math

import jax
import jax.numpy as jnp
import numpy as np
from jax import lax
from jax.experimental import pallas as pl
from jax.experimental.pallas import tpu as pltpu
from jax.sharding import Mesh
from jax.sharding import PartitionSpec as P


SLAB = ("chip", "core")
GROUPS_SLAB = ("groups", "chip", "core")
LANES = 128
HALF = 4
RUN = 8
PITCH = 40
FAR, NEAR = ((0, 3, 6), (0, 1, 2))
SECOND = (-14336.0, 8064.0, -1008.0, 128.0, -9.0)
SECOND_REST = 14.0
SECOND_UNIT = 5040.0
FIRST = (672.0, -168.0, 32.0, -3.0)
FIRST_UNIT = 840.0
BF16 = jnp.bfloat16
F32 = jnp.float32
VMEM_WHOLE = pl.BlockSpec(memory_space=pltpu.VMEM)


def in_vmem(*arrays):
    return [pltpu.with_memory_space_constraint(a, pltpu.VMEM) for a in arrays]


def weight(kind, offset):
    if abs(offset) > HALF:
        return 0.0
    if kind == 2:
        return SECOND[abs(offset)]
    if offset == 0:
        return 0.0
    return FIRST[abs(offset) - 1] * (1.0 if offset > 0 else -1.0)


def band(kind, outputs, inputs):
    table = np.zeros((len(outputs), len(inputs)), np.float32)
    for i, o in enumerate(outputs):
        for j, n in enumerate(inputs):
            if o is not None and n is not None:
                table[i, j] = weight(kind, n - o)
    return table


def row_tables(rows):
    own = list(range(rows))
    inner = list(range(-HALF, 0)) + list(range(rows, rows + HALF))
    outer = list(range(-2 * HALF, -HALF)) + list(range(rows + HALF, rows + 2 * HALF))
    pad = [None] * 8
    ends = own[:8] + own[-8:]
    edge_in = ends + inner + outer + own[8:16] + own[-16:-8]
    edge_out = ends + inner + pad
    second_in = own + inner + pad
    tables = ((own, own), (edge_out, edge_in), (own, second_in))
    return [np.concatenate([band(2, o, i), band(1, o, i)]) for o, i in tables]


def column_tables(kind):
    block = list(range(2 * LANES))
    inside = band(kind, block, block).T
    across = np.zeros((2 * LANES, 2 * LANES), np.float32)
    for i in range(2 * LANES):
        for o in range(2 * LANES):
            if (i < LANES) != (o < LANES):
                across[i, o] = weight(kind, i - o)
    return inside, across


def depth_table(patch, bins):
    k = np.arange(bins)[:, None]
    z = np.arange(patch)[None, :]
    phase = (2.0 * math.pi / patch * np.mod(k * z, patch)).astype(np.float32)
    table = np.concatenate([np.cos(phase), -np.sin(phase)]).astype(np.float32) * np.float32(1.0 / math.sqrt(patch))
    return table.astype(np.float32)


def quarter_turns(quarter, cosine, sine):
    odd = (quarter & 1) == 1
    c = jnp.where(odd, sine, cosine)
    s = jnp.where(odd, cosine, sine)
    c = jnp.where(((quarter + 1) & 2) == 2, -c, c)
    s = jnp.where((quarter & 2) == 2, -s, s)
    return c, s


def small_cos_sin(y):
    y2 = y * y
    s = y * (1.0 + y2 * (-1.6666654611e-1 + y2 * (8.3321608736e-3 + y2 * -1.9515295891e-4)))
    c = 1.0 - 0.5 * y2 + y2 * y2 * (4.166664568298827e-2 + y2 * (-1.388731625493765e-3 + y2 * 2.443315711809948e-5))
    return c, s


def double_angle(theta):
    n = jnp.floor(theta * (4.0 / math.pi) + 0.5)
    y = 2.0 * theta - n * 1.5703125
    y = y - n * 4.837512969970703e-4
    y = y - n * 7.54978995489188216e-8
    c, s = small_cos_sin(y)
    return quarter_turns(n.astype(jnp.int32), c, s)


def pack_kernel(
    w_top, w_bot, c_top, c_bot, e_top, e_bot, d_top, d_bot, t_top, t_bot, partner_ref, neighbour_ref
):
    low = lax.broadcasted_iota(jnp.int32, (8, w_top.shape[-1]), 0) < HALF

    def half_turn(x):
        return pltpu.roll(x, HALF, 0)

    def emit(out, wave, params, upward):
        def join(a, b):
            return jnp.where(low, half_turn(a), b) if upward else jnp.where(low, a, half_turn(b))

        groups = []
        for w in range(wave.shape[0]):
            for s in range(wave.shape[2]):
                groups.append(wave[w, 0, s])
                groups.append(wave[w, 1, s])
                groups.append(join(wave[w, 2, s], wave[w, 3, s]))
        courant, eps, delta, tilt = (p[...] for p in params)
        high = tilt.astype(BF16).astype(F32)
        groups += [join(courant, eps), join(delta, high), tilt - high]
        groups.append(groups[-1])
        for g in range(0, len(groups), 2):
            out[8 * g : 8 * g + 16, :] = jnp.concatenate(groups[g : g + 2], axis=0).astype(BF16)

    tops = (w_top, (c_top, e_top, d_top, t_top))
    bottoms = (w_bot, (c_bot, e_bot, d_bot, t_bot))
    first = lax.axis_index("core") == 0

    @pl.when(first)
    def _():
        emit(partner_ref, *bottoms, True)
        emit(neighbour_ref, *tops, False)

    @pl.when(jnp.logical_not(first))
    def _():
        emit(partner_ref, *tops, False)
        emit(neighbour_ref, *bottoms, True)


def pack(wavefields, params):
    two, four, shots, rows, cols = wavefields.shape
    last = rows // 8 - 1
    groups = 2 * shots * 3 + 4
    wave_block = (two, four, shots, 8, cols)
    specs = [
        pl.BlockSpec(wave_block, lambda i: (0, 0, 0, 0, 0)),
        pl.BlockSpec(wave_block, lambda i: (0, 0, 0, last, 0)),
    ]
    args = [wavefields, wavefields]
    for p in params:
        specs += [pl.BlockSpec((8, cols), lambda i: (0, 0)), pl.BlockSpec((8, cols), lambda i: (last, 0))]
        args += [p, p]
    out = pltpu.VMEM((8 * groups, cols), BF16)
    return pl.pallas_call(
        pack_kernel,
        grid=(1,),
        in_specs=specs,
        out_specs=[VMEM_WHOLE] * 2,
        out_shape=[out, out],
        compiler_params=pltpu.CompilerParams(vmem_limit_bytes=8 << 20),
        name="pack",
    )(*(pltpu.with_memory_space_constraint(a, pltpu.HBM) for a in args))


def coefficients(courant, eps, delta, tilt):
    cosine, sine = double_angle(tilt)
    scaled = courant * (1.0 / SECOND_UNIT)
    stretch = 1.0 + 2.0 * delta
    return (
        0.5 + 0.5 * cosine,
        sine * (SECOND_UNIT / (FIRST_UNIT * FIRST_UNIT)),
        scaled * (1.0 + 2.0 * eps),
        scaled * (stretch * lax.rsqrt(stretch)),
        scaled,
    )


class Filler:
    def __init__(self, jobs, points):
        self.jobs, self.points, self.done, self.calls = (jobs, points, 0, 0)

    def __call__(self):
        self.calls += 1
        self.upto(-(-len(self.jobs) * self.calls // self.points))

    def upto(self, count):
        for job in self.jobs[self.done : count]:
            job()
        self.done = max(self.done, min(count, len(self.jobs)))

    def finish(self):
        self.upto(len(self.jobs))


def along_columns(out, source, inside, across, fill):
    out[:, LANES : 3 * LANES] = jnp.dot(source[:, LANES : 3 * LANES], across[...], preferred_element_type=F32)
    fill()
    left = jnp.dot(source[:, : 2 * LANES], inside[...], preferred_element_type=F32)
    out[:, :LANES] = left[:, :LANES]
    out[:, LANES : 2 * LANES] += left[:, LANES:]
    fill()
    right = jnp.dot(source[:, 2 * LANES :], inside[...], preferred_element_type=F32)
    out[:, 2 * LANES : 3 * LANES] += right[:, :LANES]
    out[:, 3 * LANES :] = right[:, LANES:]
    fill()


def derive(field, slope, zz, xx, xz, table, columns, fields, fill):
    count = table.shape[0] // 2
    for f in range(2):
        source = field[f]
        product = jnp.dot(table[count:, :], source, preferred_element_type=F32)
        slope[f * count : (f + 1) * count, :] = product.astype(BF16)
        fill()
        zz[f * count : (f + 1) * count, :] = jnp.dot(table[:count, :], source, preferred_element_type=F32)
        fill()
    along_columns(xx, fields, columns[0], columns[1], fill)
    along_columns(xz, slope[...], columns[2], columns[3], fill)


def tilted(f, value, zz, xx, xz, mix, twist):
    turn = mix * (xx - zz) - twist * xz
    rest = SECOND_REST * value
    return (zz + turn) - rest if f == 0 else (xx - turn) - rest


def early_kernel(
    counts_ref, wave_ref, courant_ref, eps_ref, delta_ref, tilt_ref, angle_ref, own_ref,
    xx_ref, xx_across_ref, x_ref, x_across_ref,
    mix_ref, twist_ref, a_ref, b_ref, c_ref, low_c, low_s, high_c, high_s, alive_ref, next_ref,
    field_ref, slope_ref, zz_ref, xx_out, xz_out,
):
    rows, _ = courant_ref.shape
    wavefields, _, shots = wave_ref.shape[:3]
    columns = (xx_ref, xx_across_ref, x_ref, x_across_ref)
    items = [(w, s) for w in range(wavefields) for s in range(shots)]

    def coefficient_job(r):
        def job():
            at = slice(r, r + 8)
            values = coefficients(courant_ref[at, :], eps_ref[at, :], delta_ref[at, :], tilt_ref[at, :])
            for ref, value in zip((mix_ref, twist_ref, a_ref, b_ref, c_ref), values, strict=True):
                ref[at, :] = value

        return job

    fill = Filler([coefficient_job(r) for r in range(0, rows, 8)], 20)

    def matmuls(i):
        w, s = items[i]
        k = i % 2
        for f in range(2):
            field_ref[k, f * rows : (f + 1) * rows, :] = wave_ref[w, f, s].astype(BF16)
        parts = [field_ref.at[k, f * rows : (f + 1) * rows, :][...] for f in range(2)]
        derive(
            parts, slope_ref.at[k], zz_ref.at[k], xx_out.at[k], xz_out.at[k], own_ref, columns,
            field_ref.at[k][...], fill,
        )

    def advance(i):
        w, s = items[i]
        k = i % 2
        for r in range(8, rows - 8, 8):
            at = slice(r, r + 8)
            p, q, p0, q0 = (wave_ref[w, f, s, at, :] for f in range(4))
            mix, twist = (mix_ref[at, :], twist_ref[at, :])

            def operator(f, value):
                here = slice(f * rows + r, f * rows + r + 8)
                return tilted(f, value, zz_ref[k, here, :], xx_out[k, here, :], xz_out[k, here, :], mix, twist)

            across, along = (operator(0, p), operator(1, q))
            a, b, c = (a_ref[at, :], b_ref[at, :], c_ref[at, :])
            next_ref[i, 0, at, :] = (2.0 * p - p0) + (a * across + b * along)
            next_ref[i, 1, at, :] = (2.0 * q - q0) + (b * across + c * along)

    @pl.when(lax.axis_index("core") >= 0)
    def _():
        matmuls(0)
        matmuls(1)
        fill.finish()
        slant_factors(angle_ref, low_c, low_s, high_c, high_s)

    @pl.when(lax.axis_index("core") >= 0)
    def _():
        advance(0)
        matmuls(2)

    @pl.when(lax.axis_index("core") >= 0)
    def _():
        advance(1)
        matmuls(3)

    advance(2)
    advance(len(items) - 1)
    live = lax.broadcasted_iota(jnp.int32, (8, LANES), 0) < counts_ref[lax.axis_index(SLAB)]
    alive_ref[...] = jnp.where(live, 1.0, 0.0)


def slant_factors(angle_ref, low_c, low_s, high_c, high_s):
    right_half = lax.broadcasted_iota(jnp.int32, (LANES, LANES), 1) >= LANES // 2
    angles = jnp.concatenate([angle_ref[...], angle_ref[...]], axis=1)
    lateral = lax.broadcasted_iota(jnp.int32, (LANES, LANES), 0)
    modulus = 16 * LANES
    turn = (lateral * angles) & (modulus - 1)
    quarter = (turn + modulus // 8) >> int(math.log2(modulus // 4))
    rest = turn - quarter * (modulus // 4)
    c1, s1 = small_cos_sin(rest.astype(F32) * (2.0 * math.pi / modulus))
    c1, s1 = quarter_turns(quarter, c1, s1)

    def times(x, y):
        return (x[0] * y[0] - x[1] * y[1], x[0] * y[1] + x[1] * y[0])

    low_c[...], low_s[...] = (c1, s1)
    stride = (c1, s1)
    for _ in range(int(math.log2(RUN))):
        stride = times(stride, stride)
    scale = 1.0 / math.sqrt(LANES)
    value = (jnp.where(right_half, 0.0, scale), jnp.where(right_half, scale, 0.0))
    for j in range(high_c.shape[0]):
        high_c[j], high_s[j] = value
        value = times(value, stride)


def late_kernel(
    wave_ref, partner_ref, neighbour_ref, mix_ref, twist_ref, a_ref, b_ref, c_ref,
    low_c, low_s, high_c, high_s, alive_ref, next_ref,
    edge_table_ref, two_ref, xx_ref, xx_across_ref, x_ref, x_across_ref, depth_ref,
    out_ref,
    edge_z, edge_x, edge_slope, edge_zz, edge_xx, edge_xz, edge_next,
    field_ref, slope_ref, zz_ref, xx_out, xz_out, split_ref, spectra_ref, image_ref, slant_ref,
):
    wavefields, _, shots, rows, cols = wave_ref.shape
    bins = rows // 2
    per_slab = cols // LANES
    columns = (xx_ref, xx_across_ref, x_ref, x_across_ref)
    items = [(w, s) for w in range(wavefields) for s in range(shots)]
    low = lax.broadcasted_iota(jnp.int32, (8, cols), 0) < HALF
    first = lax.axis_index("core") == 0
    coefficient_refs = (mix_ref, twist_ref, a_ref, b_ref, c_ref)

    def half_turn(x):
        return pltpu.roll(x, HALF, 0)

    def group(g):
        at = slice(8 * g, 8 * g + 8)
        a, b = (partner_ref[at, :].astype(F32), neighbour_ref[at, :].astype(F32))
        return jnp.where(first, b, a), jnp.where(first, a, b)

    def first_halves(g):
        u, d = group(g)
        return jnp.where(low, u, half_turn(d))

    def second_halves(g):
        u, d = group(g)
        return jnp.where(low, half_turn(u), d)

    def slant_job(j, r):
        def job():
            at = slice(r, r + 16)
            one = (low_c[at, :], low_s[at, :])
            back = (high_c[j, at, :], high_s[j, at, :])
            here = (back[0] * one[0] - back[1] * one[1], back[0] * one[1] + back[1] * one[0])
            twice = 2.0 * one[0]
            for i in range(RUN):
                slant_ref[RUN * j + i, at, :] = back[0].astype(BF16)
                slant_ref[RUN * j + i, LANES + r : LANES + r + 16, :] = back[1].astype(BF16)
                back, here = here, tuple(twice * x - y for x, y in zip(here, back, strict=True))

        return job

    jobs = [slant_job(j, r) for j in range(bins // RUN) for r in range(0, LANES, 16)]
    fill = Filler(jobs, 6 + 10 * len(items))

    def current(i, f, r):
        if r == 0:
            return edge_next[i, f, 0:8, :]
        if r == rows - 8:
            return edge_next[i, f, 8:16, :]
        return next_ref[i, f, r : r + 8, :]

    def matmuls(i):
        k = i % 2
        for f in range(2):
            for r in range(0, rows, 16):
                pair = jnp.concatenate([current(i, f, r), current(i, f, r + 8)], axis=0)
                pair = pair.astype(BF16)
                field_ref[k, f * rows + r : f * rows + r + 16, :] = pair
            edge = edge_next[i, f, 16:24, :]
            pair = jnp.concatenate([edge, jnp.zeros_like(edge)], axis=0).astype(BF16)
            field_ref[k, 2 * rows + 16 * f : 2 * rows + 16 * f + 16, :] = pair
        parts = [
            jnp.concatenate(
                [
                    field_ref[k, f * rows : (f + 1) * rows, :],
                    field_ref[k, 2 * rows + 16 * f : 2 * rows + 16 * f + 16, :],
                ],
                axis=0,
            )
            for f in range(2)
        ]
        derive(
            parts, slope_ref.at[k], zz_ref.at[k], xx_out.at[k], xz_out.at[k], two_ref, columns,
            field_ref[k, : 2 * rows, :], fill,
        )

    def advance(i):
        w, s = items[i]
        k = i % 2
        for r in range(0, rows, 16):
            parts = []
            for h in (r, r + 8):
                at = slice(h, h + 8)
                mix, twist, a, b = (ref[at, :] for ref in coefficient_refs[:4])

                def operator(f, value):
                    here = slice(f * rows + h, f * rows + h + 8)
                    return tilted(
                        f, value, zz_ref[k, here, :], xx_out[k, here, :], xz_out[k, here, :], mix, twist
                    )

                p, q = (current(i, f, h) for f in range(2))
                across, along = (operator(0, p), operator(1, q))
                parts.append((2.0 * p - wave_ref[w, 0, s, at, :]) + (a * across + b * along))
            value = jnp.concatenate(parts, axis=0)
            top = value.astype(BF16)
            split_ref[k, r : r + 16, :] = top
            split_ref[k, rows + r : rows + r + 16, :] = (value - top.astype(F32)).astype(BF16)
            split_ref[k, 2 * rows + r : 2 * rows + r + 16, :] = top

    def transform(i):
        spectra = jnp.dot(depth_ref[...], split_ref[i % 2], preferred_element_type=F32)
        for part in range(2):
            for m in range(per_slab):
                start = 16 * part + per_slab * i + m
                spectra_ref[pl.ds(start, bins, stride=PITCH), :] = spectra[
                    part * bins : (part + 1) * bins, m * LANES : (m + 1) * LANES
                ]

    @pl.when(lax.axis_index("core") >= 0)
    def _():
        tall = 32
        halos = []
        for i, (w, s) in enumerate(items):
            halo = []
            for f in range(2):
                u, d = group(3 * i + f)
                inner = jnp.where(low, half_turn(u), half_turn(d))
                outer = jnp.where(low, u, d)
                halo.append(inner)
                pieces = (
                    wave_ref[w, f, s, 0:8, :], wave_ref[w, f, s, rows - 8 : rows, :], inner, outer,
                    wave_ref[w, f, s, 8:16, :], wave_ref[w, f, s, rows - 16 : rows - 8, :],
                )
                for n in range(0, 6, 2):
                    pair = jnp.concatenate(pieces[n : n + 2], axis=0).astype(BF16)
                    edge_z[i, f, 8 * n : 8 * n + 16, :] = pair
                    if n < 4:
                        at = (2 * i + f) * tall + 8 * n
                        edge_x[at : at + 16, :] = pair
            halo += [first_halves(3 * i + 2), second_halves(3 * i + 2)]
            halos.append(halo)
        for i in range(len(items)):
            for f in range(2):
                product = jnp.dot(edge_table_ref[...], edge_z[i, f], preferred_element_type=F32)
                at = (2 * i + f) * tall
                edge_zz[at : at + tall, :] = product[:tall]
                edge_slope[at : at + tall, :] = product[tall:].astype(BF16)
        along_columns(edge_xx, edge_x[...], xx_ref, xx_across_ref, fill)
        along_columns(edge_xz, edge_slope[...], x_ref, x_across_ref, fill)
        g = 3 * len(items)
        beyond = coefficients(
            first_halves(g), second_halves(g), first_halves(g + 1), second_halves(g + 1) + first_halves(g + 2)
        )

        def edge_advance(i):
            w, s = items[i]
            for n, r in enumerate((0, rows - 8, None)):
                if r is None:
                    fields = halos[i]
                    mix, twist, a, b, c = beyond
                else:
                    at = slice(r, r + 8)
                    fields = [wave_ref[w, f, s, at, :] for f in range(4)]
                    mix, twist, a, b, c = (ref[at, :] for ref in coefficient_refs)
                p, q, p0, q0 = fields

                def operator(f, value):
                    here = slice((2 * i + f) * tall + 8 * n, (2 * i + f) * tall + 8 * n + 8)
                    return tilted(f, value, edge_zz[here, :], edge_xx[here, :], edge_xz[here, :], mix, twist)

                across, along = (operator(0, p), operator(1, q))
                edge_next[i, 0, 8 * n : 8 * n + 8, :] = (2.0 * p - p0) + (a * across + b * along)
                edge_next[i, 1, 8 * n : 8 * n + 8, :] = (2.0 * q - q0) + (b * across + c * along)

        for i in range(len(items)):
            edge_advance(i)
        matmuls(0)
        for i in range(1, 4):
            matmuls(i)
            advance(i - 1)
            transform(i - 1)
        fill.finish()

    for i in range(4, len(items)):
        matmuls(i)
        advance(i - 1)
        transform(i - 1)
    advance(len(items) - 1)
    transform(len(items) - 1)

    left_lane = lax.broadcasted_iota(jnp.int32, (8, LANES), 1) < LANES // 2
    alive = alive_ref[...]
    for j in range(bins // RUN):
        pair = []
        for i in range(RUN):
            at = (RUN * j + i) * PITCH
            left = jnp.concatenate(
                [spectra_ref[at : at + 16, :], spectra_ref[at + 16 : at + 32, :]], axis=1
            ).astype(BF16)
            stack = jnp.dot(left, slant_ref[RUN * j + i], preferred_element_type=F32)
            product = stack[:8] * stack[8:]
            pair.append(product + pltpu.roll(product, 4, 0))
            if i % 2 == 1:
                even, odd = pair
                even = even + pltpu.roll(even, LANES // 2, 1)
                odd = odd + pltpu.roll(odd, LANES // 2, 1)
                pair = []
                where_to = (RUN * j + i) // 2 * LANES
                image_ref[:, where_to : where_to + LANES] = alive * jnp.where(left_lane, even, odd)
    out_ref[...] = image_ref[:per_slab, :].astype(BF16)


def column_operands():
    return [jnp.asarray(t, dtype=BF16) for kind in (2, 1) for t in column_tables(kind)]


def early(wavefields, params, slab_counts, angle_table):
    two, _, shots, rows, cols = wavefields.shape
    field = pltpu.VMEM((rows, cols), F32)
    table = pltpu.VMEM((rows // 2 // RUN, LANES, LANES), F32)
    own = jnp.asarray(row_tables(rows)[0], dtype=BF16)
    args = [wavefields, *params, angle_table.reshape(1, -1), own, *column_operands()]
    outs = [field] * 5 + [pltpu.VMEM((LANES, LANES), F32)] * 2 + [table] * 2 + [
        pltpu.VMEM((8, LANES), F32),
        pltpu.VMEM((two * shots, 2, rows, cols), F32),
    ]
    return pl.pallas_call(
        early_kernel,
        in_specs=[pl.BlockSpec(memory_space=pltpu.SMEM)] + [VMEM_WHOLE] * len(args),
        out_specs=[VMEM_WHOLE] * len(outs),
        out_shape=outs,
        scratch_shapes=[
            pltpu.VMEM((2, 2 * rows, cols), BF16),
            pltpu.VMEM((2, 2 * rows, cols), BF16),
            pltpu.VMEM((2, 2 * rows, cols), F32),
            pltpu.VMEM((2, 2 * rows, cols), F32),
            pltpu.VMEM((2, 2 * rows, cols), F32),
        ],
        compiler_params=pltpu.CompilerParams(vmem_limit_bytes=24 << 20),
        name="early",
    )(slab_counts, *in_vmem(*args))


def late(wavefields, partner, neighbour, prepared, angles):
    two, _, shots, rows, cols = wavefields.shape
    bins = rows // 2
    per_slab = cols // rows
    items = two * shots
    _, edge, both = (jnp.asarray(t, dtype=BF16) for t in row_tables(rows))
    depth = depth_table(rows, bins)
    depth_top = depth.astype(jnp.bfloat16)
    depth_low = (depth - depth_top.astype(np.float32)).astype(jnp.bfloat16)
    depth = jnp.asarray(np.concatenate([depth_top, depth_top, depth_low], axis=1), dtype=BF16)
    args = [wavefields, partner, neighbour, *prepared, edge, both, *column_operands(), depth]
    out_shape = (per_slab, bins * angles)
    scratch = [
        pltpu.VMEM((items, 2, 48, cols), BF16),
        pltpu.VMEM((items * 2 * 32, cols), BF16),
        pltpu.VMEM((items * 2 * 32, cols), BF16),
        pltpu.VMEM((items * 2 * 32, cols), F32),
        pltpu.VMEM((items * 2 * 32, cols), F32),
        pltpu.VMEM((items * 2 * 32, cols), F32),
        pltpu.VMEM((items, 2, 24, cols), F32),
        pltpu.VMEM((2, 2 * (rows + 16), cols), BF16),
        pltpu.VMEM((2, 2 * rows, cols), BF16),
        pltpu.VMEM((2, 2 * rows, cols), F32),
        pltpu.VMEM((2, 2 * rows, cols), F32),
        pltpu.VMEM((2, 2 * rows, cols), F32),
        pltpu.VMEM((2, 3 * rows, cols), BF16),
        pltpu.VMEM((PITCH * bins, LANES), F32),
        pltpu.VMEM((8, bins * angles), F32),
        pltpu.VMEM((bins, 2 * LANES, LANES), BF16),
    ]
    return pl.pallas_call(
        late_kernel,
        in_specs=[VMEM_WHOLE] * len(args),
        out_specs=VMEM_WHOLE,
        out_shape=pltpu.VMEM(out_shape, BF16),
        scratch_shapes=scratch,
        compiler_params=pltpu.CompilerParams(vmem_limit_bytes=36 << 20),
        name="late",
    )(*in_vmem(*args))


def pick_kernel(loc_ref, *refs, per_slab, count, pieces, begun):
    held_refs, rest = (refs[: len(pieces)], refs[len(pieces) :])
    slab = lax.axis_index(SLAB)
    chip, core = (lax.axis_index("chip"), lax.axis_index("core"))
    chips = lax.axis_size("chip")
    per_row = LANES // count
    row = loc_ref[pl.ds(slab // per_row, 1), :]
    spot = slab % per_row
    partner = spot + 1 - 2 * core
    loc = jnp.concatenate(
        [pltpu.roll(row, (LANES - s * count) % LANES, 1)[:, :count] for s in (spot, partner)], axis=1
    )
    owner = loc // per_slab
    ahead = lax.rem(owner // 2 - chip + chips, chips)
    up = ahead <= chips // 2
    hops = jnp.where(up, ahead, chips - ahead)
    holder = jnp.where(hops == chips // 2, owner % 2, jnp.where(up, 1, 0))
    far_hops, near_hops = (hops // len(NEAR), hops % len(NEAR))
    block = 2 * per_slab
    index = jnp.where(owner % 2 == holder, 0, per_slab) + loc % per_slab
    index = index + jnp.where(far_hops > 0, far_hops - 1, 0) * block
    total = rest[0][...] if begun else None
    for (near, by_far), ref in zip(pieces, held_refs, strict=True):
        held = lax.broadcasted_iota(jnp.int32, (ref.shape[0], 2 * count), 0)
        hit = (held == index) & (holder == core) & (near_hops == near) & ((far_hops > 0) == by_far)
        hot = jnp.where(hit, 1.0, 0.0).astype(BF16)
        part = lax.dot_general(hot, ref[...], (((0,), (0,)), ((), ())), preferred_element_type=F32)
        total = part if total is None else total + part
    if begun:
        mine_ref, theirs_ref = rest[1:]
        mine_ref[...] = total[:count]
        theirs_ref[...] = total[count:].astype(BF16)
    else:
        rest[0][...] = total


def pick(loc_patch, held, count, per_slab, begun=None):
    width = held[0][2].shape[1]
    pieces = [h[:2] for h in held]
    args = [loc_patch.reshape(-1, LANES)] + [h[2] for h in held] + ([] if begun is None else [begun])
    outs = [pltpu.VMEM((2 * count, width), F32)]
    if begun is not None:
        outs = [pltpu.VMEM((count, width), F32), pltpu.VMEM((count, width), BF16)]
    return pl.pallas_call(
        lambda *refs: pick_kernel(
            *refs, per_slab=per_slab, count=count, pieces=pieces, begun=begun is not None
        ),
        in_specs=[VMEM_WHOLE] * len(args),
        out_specs=[VMEM_WHOLE] * len(outs),
        out_shape=outs,
        compiler_params=pltpu.CompilerParams(vmem_limit_bytes=8 << 20),
        name="pick",
    )(*in_vmem(*args))


def swap_cores(array):
    return lax.ppermute(array, "core", [(0, 1), (1, 0)])


def onward(array, hops):
    chips = lax.axis_size("chip")
    pairs = [(2 * i, 2 * ((i + hops) % chips)) for i in range(chips)]
    pairs += [(2 * i + 1, 2 * ((i - hops) % chips) + 1) for i in range(chips)]
    return lax.ppermute(array, SLAB, pairs)


def spread(images):
    count = images.shape[0]
    chip = jnp.concatenate([images, swap_cores(images)])
    far = [onward(chip, h) for h in FAR[1:]]
    near = [onward(chip, h) for h in NEAR[1:]]
    came = jnp.concatenate(far)
    short = came[: came.shape[0] - count]
    both = [onward(short if h == NEAR[-1] else came, h) for h in NEAR[1:]]
    return (
        [(n, False, a) for n, a in enumerate([chip] + near)],
        [(n, True, a) for n, a in enumerate([came] + both)],
    )


def per_device(
    wavefields, courant, epsilon, anisotropy_delta, tilt_angle, loc_patch, slab_counts, angle_table
):
    slabs = lax.axis_size(SLAB)
    assert FAR[-1] + NEAR[-1] == slabs // 4
    per_slab = wavefields.shape[4] // wavefields.shape[3]
    params = (courant, epsilon, anisotropy_delta, tilt_angle)
    to_partner, to_neighbour = pack(wavefields, params)
    pairs = [(i, i + 1) for i in range(1, slabs - 1, 2)]
    neighbour = lax.ppermute(to_neighbour, SLAB, pairs + [(j, i) for i, j in pairs])
    partner = swap_cores(to_partner)
    prepared = early(wavefields, params, slab_counts, angle_table)
    images = late(wavefields, partner, neighbour, prepared, angle_table.shape[0])
    close, distant = spread(images)
    count = loc_patch.shape[0] // slabs
    (begun,) = pick(loc_patch, close, count, per_slab)
    mine, theirs = pick(loc_patch, distant, count, per_slab, begun)
    return mine + swap_cores(theirs).astype(F32)


def solution(mesh):
    shape = (mesh.shape["groups"], mesh.shape["slab"] // 2, 2)
    finer = Mesh(mesh.devices.reshape(shape), GROUPS_SLAB)
    in_specs = (
        P(None, None, "groups", SLAB, None),
        P(SLAB, None),
        P(SLAB, None),
        P(SLAB, None),
        P(SLAB, None),
        P(),
        P(),
        P(),
    )
    out_specs = P(GROUPS_SLAB, None)
    return jax.shard_map(
        per_device, mesh=finer, in_specs=in_specs, out_specs=out_specs, check_vma=False
    )
```

```python
import math

import jax
import jax.numpy as jnp
import numpy as np
from jax import lax
from jax.experimental import pallas as pl
from jax.experimental.pallas import tpu as pltpu
from jax.sharding import Mesh
from jax.sharding import PartitionSpec as P


SLAB = ("chip", "core")
GROUPS_SLAB = ("groups", "chip", "core")
LANES = 128
HALF = 4
RUN = 8
PITCH = 40
FAR, NEAR = ((0, 3, 6), (0, 1, 2))
SECOND = (-14336.0, 8064.0, -1008.0, 128.0, -9.0)
SECOND_REST = 14.0
SECOND_UNIT = 5040.0
FIRST = (672.0, -168.0, 32.0, -3.0)
FIRST_UNIT = 840.0
BF16 = jnp.bfloat16
F32 = jnp.float32
VMEM_WHOLE = pl.BlockSpec(memory_space=pltpu.VMEM)


def in_vmem(*arrays):
    return [pltpu.with_memory_space_constraint(a, pltpu.VMEM) for a in arrays]


def weight(kind, offset):
    if abs(offset) > HALF:
        return 0.0
    if kind == 2:
        return SECOND[abs(offset)]
    if offset == 0:
        return 0.0
    return FIRST[abs(offset) - 1] * (1.0 if offset > 0 else -1.0)


def band(kind, outputs, inputs):
    table = np.zeros((len(outputs), len(inputs)), np.float32)
    for i, o in enumerate(outputs):
        for j, n in enumerate(inputs):
            if o is not None and n is not None:
                table[i, j] = weight(kind, n - o)
    return table


def row_tables(rows):
    own = list(range(rows))
    inner = list(range(-HALF, 0)) + list(range(rows, rows + HALF))
    outer = list(range(-2 * HALF, -HALF)) + list(range(rows + HALF, rows + 2 * HALF))
    pad = [None] * 8
    ends = own[:8] + own[-8:]
    edge_in = ends + inner + outer + own[8:16] + own[-16:-8]
    edge_out = ends + inner + pad
    second_in = own + inner + pad
    tables = ((own, own), (edge_out, edge_in), (own, second_in))
    return [np.concatenate([band(2, o, i), band(1, o, i)]) for o, i in tables]


def column_tables(kind):
    block = list(range(2 * LANES))
    inside = band(kind, block, block).T
    across = np.zeros((2 * LANES, 2 * LANES), np.float32)
    for i in range(2 * LANES):
        for o in range(2 * LANES):
            if (i < LANES) != (o < LANES):
                across[i, o] = weight(kind, i - o)
    return inside, across


def depth_table(patch, bins):
    k = np.arange(bins)[:, None]
    z = np.arange(patch)[None, :]
    phase = (2.0 * math.pi / patch * np.mod(k * z, patch)).astype(np.float32)
    table = np.concatenate([np.cos(phase), -np.sin(phase)]).astype(np.float32) * np.float32(1.0 / math.sqrt(patch))
    return table.astype(np.float32)


def quarter_turns(quarter, cosine, sine):
    odd = (quarter & 1) == 1
    c = jnp.where(odd, sine, cosine)
    s = jnp.where(odd, cosine, sine)
    c = jnp.where(((quarter + 1) & 2) == 2, -c, c)
    s = jnp.where((quarter & 2) == 2, -s, s)
    return c, s


def small_cos_sin(y):
    y2 = y * y
    s = y * (1.0 + y2 * (-1.6666654611e-1 + y2 * (8.3321608736e-3 + y2 * -1.9515295891e-4)))
    c = 1.0 - 0.5 * y2 + y2 * y2 * (4.166664568298827e-2 + y2 * (-1.388731625493765e-3 + y2 * 2.443315711809948e-5))
    return c, s


def double_angle(theta):
    n = jnp.floor(theta * (4.0 / math.pi) + 0.5)
    y = 2.0 * theta - n * 1.5703125
    y = y - n * 4.837512969970703e-4
    y = y - n * 7.54978995489188216e-8
    c, s = small_cos_sin(y)
    return quarter_turns(n.astype(jnp.int32), c, s)


def pack_kernel(
    w_top, w_bot, c_top, c_bot, e_top, e_bot, d_top, d_bot, t_top, t_bot, partner_ref, neighbour_ref
):
    low = lax.broadcasted_iota(jnp.int32, (8, w_top.shape[-1]), 0) < HALF

    def half_turn(x):
        return pltpu.roll(x, HALF, 0)

    def emit(out, wave, params, upward):
        def join(a, b):
            return jnp.where(low, half_turn(a), b) if upward else jnp.where(low, a, half_turn(b))

        groups = []
        for w in range(wave.shape[0]):
            for s in range(wave.shape[2]):
                groups.append(wave[w, 0, s])
                groups.append(wave[w, 1, s])
                groups.append(join(wave[w, 2, s], wave[w, 3, s]))
        courant, eps, delta, tilt = (p[...] for p in params)
        high = tilt.astype(BF16).astype(F32)
        groups += [join(courant, eps), join(delta, high), tilt - high]
        groups.append(groups[-1])
        for g in range(0, len(groups), 2):
            out[8 * g : 8 * g + 16, :] = jnp.concatenate(groups[g : g + 2], axis=0).astype(BF16)

    tops = (w_top, (c_top, e_top, d_top, t_top))
    bottoms = (w_bot, (c_bot, e_bot, d_bot, t_bot))
    first = lax.axis_index("core") == 0

    @pl.when(first)
    def _():
        emit(partner_ref, *bottoms, True)
        emit(neighbour_ref, *tops, False)

    @pl.when(jnp.logical_not(first))
    def _():
        emit(partner_ref, *tops, False)
        emit(neighbour_ref, *bottoms, True)


def pack(wavefields, params):
    two, four, shots, rows, cols = wavefields.shape
    last = rows // 8 - 1
    groups = 2 * shots * 3 + 4
    wave_block = (two, four, shots, 8, cols)
    specs = [
        pl.BlockSpec(wave_block, lambda i: (0, 0, 0, 0, 0)),
        pl.BlockSpec(wave_block, lambda i: (0, 0, 0, last, 0)),
    ]
    args = [wavefields, wavefields]
    for p in params:
        specs += [pl.BlockSpec((8, cols), lambda i: (0, 0)), pl.BlockSpec((8, cols), lambda i: (last, 0))]
        args += [p, p]
    out = pltpu.VMEM((8 * groups, cols), BF16)
    return pl.pallas_call(
        pack_kernel,
        grid=(1,),
        in_specs=specs,
        out_specs=[VMEM_WHOLE] * 2,
        out_shape=[out, out],
        compiler_params=pltpu.CompilerParams(vmem_limit_bytes=8 << 20),
        name="pack",
    )(*(pltpu.with_memory_space_constraint(a, pltpu.HBM) for a in args))


def coefficients(courant, eps, delta, tilt):
    cosine, sine = double_angle(tilt)
    scaled = courant * (1.0 / SECOND_UNIT)
    stretch = 1.0 + 2.0 * delta
    return (
        0.5 + 0.5 * cosine,
        sine * (SECOND_UNIT / (FIRST_UNIT * FIRST_UNIT)),
        scaled * (1.0 + 2.0 * eps),
        scaled * (stretch * lax.rsqrt(stretch)),
        scaled,
    )


class Filler:
    def __init__(self, jobs, points):
        self.jobs, self.points, self.done, self.calls = (jobs, points, 0, 0)

    def __call__(self):
        self.calls += 1
        self.upto(-(-len(self.jobs) * self.calls // self.points))

    def upto(self, count):
        for job in self.jobs[self.done : count]:
            job()
        self.done = max(self.done, min(count, len(self.jobs)))

    def finish(self):
        self.upto(len(self.jobs))


def along_columns(out, source, inside, across, fill):
    out[:, LANES : 3 * LANES] = jnp.dot(source[:, LANES : 3 * LANES], across[...], preferred_element_type=F32)
    fill()
    left = jnp.dot(source[:, : 2 * LANES], inside[...], preferred_element_type=F32)
    out[:, :LANES] = left[:, :LANES]
    out[:, LANES : 2 * LANES] += left[:, LANES:]
    fill()
    right = jnp.dot(source[:, 2 * LANES :], inside[...], preferred_element_type=F32)
    out[:, 2 * LANES : 3 * LANES] += right[:, :LANES]
    out[:, 3 * LANES :] = right[:, LANES:]
    fill()


def derive(field, slope, zz, xx, xz, table, columns, fields, fill):
    count = table.shape[0] // 2
    for f in range(2):
        source = field[f]
        product = jnp.dot(table[count:, :], source, preferred_element_type=F32)
        slope[f * count : (f + 1) * count, :] = product.astype(BF16)
        fill()
        zz[f * count : (f + 1) * count, :] = jnp.dot(table[:count, :], source, preferred_element_type=F32)
        fill()
    along_columns(xx, fields, columns[0], columns[1], fill)
    along_columns(xz, slope[...], columns[2], columns[3], fill)


def tilted(f, value, zz, xx, xz, mix, twist):
    turn = mix * (xx - zz) - twist * xz
    rest = SECOND_REST * value
    return (zz + turn) - rest if f == 0 else (xx - turn) - rest


def early_kernel(
    counts_ref, wave_ref, courant_ref, eps_ref, delta_ref, tilt_ref, angle_ref, own_ref,
    xx_ref, xx_across_ref, x_ref, x_across_ref,
    mix_ref, twist_ref, a_ref, b_ref, c_ref, low_c, low_s, high_c, high_s, alive_ref, next_ref,
    field_ref, slope_ref, zz_ref, xx_out, xz_out,
):
    rows, _ = courant_ref.shape
    wavefields, _, shots = wave_ref.shape[:3]
    columns = (xx_ref, xx_across_ref, x_ref, x_across_ref)
    items = [(w, s) for w in range(wavefields) for s in range(shots)]

    def coefficient_job(r):
        def job():
            at = slice(r, r + 8)
            values = coefficients(courant_ref[at, :], eps_ref[at, :], delta_ref[at, :], tilt_ref[at, :])
            for ref, value in zip((mix_ref, twist_ref, a_ref, b_ref, c_ref), values, strict=True):
                ref[at, :] = value

        return job

    fill = Filler([coefficient_job(r) for r in range(0, rows, 8)], 20)

    def matmuls(i):
        w, s = items[i]
        k = i % 2
        for f in range(2):
            field_ref[k, f * rows : (f + 1) * rows, :] = wave_ref[w, f, s].astype(BF16)
        parts = [field_ref.at[k, f * rows : (f + 1) * rows, :][...] for f in range(2)]
        derive(
            parts, slope_ref.at[k], zz_ref.at[k], xx_out.at[k], xz_out.at[k], own_ref, columns,
            field_ref.at[k][...], fill,
        )

    def advance(i):
        w, s = items[i]
        k = i % 2
        for r in range(8, rows - 8, 8):
            at = slice(r, r + 8)
            p, q, p0, q0 = (wave_ref[w, f, s, at, :] for f in range(4))
            mix, twist = (mix_ref[at, :], twist_ref[at, :])

            def operator(f, value):
                here = slice(f * rows + r, f * rows + r + 8)
                return tilted(f, value, zz_ref[k, here, :], xx_out[k, here, :], xz_out[k, here, :], mix, twist)

            across, along = (operator(0, p), operator(1, q))
            a, b, c = (a_ref[at, :], b_ref[at, :], c_ref[at, :])
            next_ref[i, 0, at, :] = (2.0 * p - p0) + (a * across + b * along)
            next_ref[i, 1, at, :] = (2.0 * q - q0) + (b * across + c * along)

    @pl.when(lax.axis_index("core") >= 0)
    def _():
        matmuls(0)
        matmuls(1)
        fill.finish()
        slant_factors(angle_ref, low_c, low_s, high_c, high_s)

    @pl.when(lax.axis_index("core") >= 0)
    def _():
        advance(0)
        matmuls(2)

    @pl.when(lax.axis_index("core") >= 0)
    def _():
        advance(1)
        matmuls(3)

    advance(2)
    advance(len(items) - 1)
    live = lax.broadcasted_iota(jnp.int32, (8, LANES), 0) < counts_ref[lax.axis_index(SLAB)]
    alive_ref[...] = jnp.where(live, 1.0, 0.0)


def slant_factors(angle_ref, low_c, low_s, high_c, high_s):
    right_half = lax.broadcasted_iota(jnp.int32, (LANES, LANES), 1) >= LANES // 2
    angles = jnp.concatenate([angle_ref[...], angle_ref[...]], axis=1)
    lateral = lax.broadcasted_iota(jnp.int32, (LANES, LANES), 0)
    modulus = 16 * LANES
    turn = (lateral * angles) & (modulus - 1)
    quarter = (turn + modulus // 8) >> int(math.log2(modulus // 4))
    rest = turn - quarter * (modulus // 4)
    c1, s1 = small_cos_sin(rest.astype(F32) * (2.0 * math.pi / modulus))
    c1, s1 = quarter_turns(quarter, c1, s1)

    def times(x, y):
        return (x[0] * y[0] - x[1] * y[1], x[0] * y[1] + x[1] * y[0])

    low_c[...], low_s[...] = (c1, s1)
    stride = (c1, s1)
    for _ in range(int(math.log2(RUN))):
        stride = times(stride, stride)
    scale = 1.0 / math.sqrt(LANES)
    value = (jnp.where(right_half, 0.0, scale), jnp.where(right_half, scale, 0.0))
    for j in range(high_c.shape[0]):
        high_c[j], high_s[j] = value
        value = times(value, stride)


def late_kernel(
    wave_ref, partner_ref, neighbour_ref, mix_ref, twist_ref, a_ref, b_ref, c_ref,
    low_c, low_s, high_c, high_s, alive_ref, next_ref,
    edge_table_ref, two_ref, xx_ref, xx_across_ref, x_ref, x_across_ref, depth_ref,
    out_ref,
    edge_z, edge_x, edge_slope, edge_zz, edge_xx, edge_xz, edge_next,
    field_ref, slope_ref, zz_ref, xx_out, xz_out, split_ref, spectra_ref, image_ref, slant_ref,
):
    wavefields, _, shots, rows, cols = wave_ref.shape
    bins = rows // 2
    per_slab = cols // LANES
    columns = (xx_ref, xx_across_ref, x_ref, x_across_ref)
    items = [(w, s) for w in range(wavefields) for s in range(shots)]
    low = lax.broadcasted_iota(jnp.int32, (8, cols), 0) < HALF
    first = lax.axis_index("core") == 0
    coefficient_refs = (mix_ref, twist_ref, a_ref, b_ref, c_ref)

    def half_turn(x):
        return pltpu.roll(x, HALF, 0)

    def group(g):
        at = slice(8 * g, 8 * g + 8)
        a, b = (partner_ref[at, :].astype(F32), neighbour_ref[at, :].astype(F32))
        return jnp.where(first, b, a), jnp.where(first, a, b)

    def first_halves(g):
        u, d = group(g)
        return jnp.where(low, u, half_turn(d))

    def second_halves(g):
        u, d = group(g)
        return jnp.where(low, half_turn(u), d)

    def slant_job(j, r):
        def job():
            at = slice(r, r + 16)
            one = (low_c[at, :], low_s[at, :])
            back = (high_c[j, at, :], high_s[j, at, :])
            here = (back[0] * one[0] - back[1] * one[1], back[0] * one[1] + back[1] * one[0])
            twice = 2.0 * one[0]
            for i in range(RUN):
                slant_ref[RUN * j + i, at, :] = back[0].astype(BF16)
                slant_ref[RUN * j + i, LANES + r : LANES + r + 16, :] = back[1].astype(BF16)
                back, here = here, tuple(twice * x - y for x, y in zip(here, back, strict=True))

        return job

    jobs = [slant_job(j, r) for j in range(bins // RUN) for r in range(0, LANES, 16)]
    fill = Filler(jobs, 6 + 10 * len(items))

    def current(i, f, r):
        if r == 0:
            return edge_next[i, f, 0:8, :]
        if r == rows - 8:
            return edge_next[i, f, 8:16, :]
        return next_ref[i, f, r : r + 8, :]

    def matmuls(i):
        k = i % 2
        for f in range(2):
            for r in range(0, rows, 16):
                pair = jnp.concatenate([current(i, f, r), current(i, f, r + 8)], axis=0)
                pair = pair.astype(BF16)
                field_ref[k, f * rows + r : f * rows + r + 16, :] = pair
            edge = edge_next[i, f, 16:24, :]
            pair = jnp.concatenate([edge, jnp.zeros_like(edge)], axis=0).astype(BF16)
            field_ref[k, 2 * rows + 16 * f : 2 * rows + 16 * f + 16, :] = pair
        parts = [
            jnp.concatenate(
                [
                    field_ref[k, f * rows : (f + 1) * rows, :],
                    field_ref[k, 2 * rows + 16 * f : 2 * rows + 16 * f + 16, :],
                ],
                axis=0,
            )
            for f in range(2)
        ]
        derive(
            parts, slope_ref.at[k], zz_ref.at[k], xx_out.at[k], xz_out.at[k], two_ref, columns,
            field_ref[k, : 2 * rows, :], fill,
        )

    def advance(i):
        w, s = items[i]
        k = i % 2
        for r in range(0, rows, 16):
            parts = []
            for h in (r, r + 8):
                at = slice(h, h + 8)
                mix, twist, a, b = (ref[at, :] for ref in coefficient_refs[:4])

                def operator(f, value):
                    here = slice(f * rows + h, f * rows + h + 8)
                    return tilted(
                        f, value, zz_ref[k, here, :], xx_out[k, here, :], xz_out[k, here, :], mix, twist
                    )

                p, q = (current(i, f, h) for f in range(2))
                across, along = (operator(0, p), operator(1, q))
                parts.append((2.0 * p - wave_ref[w, 0, s, at, :]) + (a * across + b * along))
            value = jnp.concatenate(parts, axis=0)
            top = value.astype(BF16)
            split_ref[k, r : r + 16, :] = top
            split_ref[k, rows + r : rows + r + 16, :] = (value - top.astype(F32)).astype(BF16)
            split_ref[k, 2 * rows + r : 2 * rows + r + 16, :] = top

    def transform(i):
        spectra = jnp.dot(depth_ref[...], split_ref[i % 2], preferred_element_type=F32)
        for part in range(2):
            for m in range(per_slab):
                start = 16 * part + per_slab * i + m
                spectra_ref[pl.ds(start, bins, stride=PITCH), :] = spectra[
                    part * bins : (part + 1) * bins, m * LANES : (m + 1) * LANES
                ]

    @pl.when(lax.axis_index("core") >= 0)
    def _():
        tall = 32
        halos = []
        for i, (w, s) in enumerate(items):
            halo = []
            for f in range(2):
                u, d = group(3 * i + f)
                inner = jnp.where(low, half_turn(u), half_turn(d))
                outer = jnp.where(low, u, d)
                halo.append(inner)
                pieces = (
                    wave_ref[w, f, s, 0:8, :], wave_ref[w, f, s, rows - 8 : rows, :], inner, outer,
                    wave_ref[w, f, s, 8:16, :], wave_ref[w, f, s, rows - 16 : rows - 8, :],
                )
                for n in range(0, 6, 2):
                    pair = jnp.concatenate(pieces[n : n + 2], axis=0).astype(BF16)
                    edge_z[i, f, 8 * n : 8 * n + 16, :] = pair
                    if n < 4:
                        at = (2 * i + f) * tall + 8 * n
                        edge_x[at : at + 16, :] = pair
            halo += [first_halves(3 * i + 2), second_halves(3 * i + 2)]
            halos.append(halo)
        for i in range(len(items)):
            for f in range(2):
                product = jnp.dot(edge_table_ref[...], edge_z[i, f], preferred_element_type=F32)
                at = (2 * i + f) * tall
                edge_zz[at : at + tall, :] = product[:tall]
                edge_slope[at : at + tall, :] = product[tall:].astype(BF16)
        along_columns(edge_xx, edge_x[...], xx_ref, xx_across_ref, fill)
        along_columns(edge_xz, edge_slope[...], x_ref, x_across_ref, fill)
        g = 3 * len(items)
        beyond = coefficients(
            first_halves(g), second_halves(g), first_halves(g + 1), second_halves(g + 1) + first_halves(g + 2)
        )

        def edge_advance(i):
            w, s = items[i]
            for n, r in enumerate((0, rows - 8, None)):
                if r is None:
                    fields = halos[i]
                    mix, twist, a, b, c = beyond
                else:
                    at = slice(r, r + 8)
                    fields = [wave_ref[w, f, s, at, :] for f in range(4)]
                    mix, twist, a, b, c = (ref[at, :] for ref in coefficient_refs)
                p, q, p0, q0 = fields

                def operator(f, value):
                    here = slice((2 * i + f) * tall + 8 * n, (2 * i + f) * tall + 8 * n + 8)
                    return tilted(f, value, edge_zz[here, :], edge_xx[here, :], edge_xz[here, :], mix, twist)

                across, along = (operator(0, p), operator(1, q))
                edge_next[i, 0, 8 * n : 8 * n + 8, :] = (2.0 * p - p0) + (a * across + b * along)
                edge_next[i, 1, 8 * n : 8 * n + 8, :] = (2.0 * q - q0) + (b * across + c * along)

        for i in range(len(items)):
            edge_advance(i)
        matmuls(0)
        for i in range(1, 4):
            matmuls(i)
            advance(i - 1)
            transform(i - 1)
        fill.finish()

    for i in range(4, len(items)):
        matmuls(i)
        advance(i - 1)
        transform(i - 1)
    advance(len(items) - 1)
    transform(len(items) - 1)

    left_lane = lax.broadcasted_iota(jnp.int32, (8, LANES), 1) < LANES // 2
    alive = alive_ref[...]
    for j in range(bins // RUN):
        pair = []
        for i in range(RUN):
            at = (RUN * j + i) * PITCH
            left = jnp.concatenate(
                [spectra_ref[at : at + 16, :], spectra_ref[at + 16 : at + 32, :]], axis=1
            ).astype(BF16)
            stack = jnp.dot(left, slant_ref[RUN * j + i], preferred_element_type=F32)
            product = stack[:8] * stack[8:]
            pair.append(product + pltpu.roll(product, 4, 0))
            if i % 2 == 1:
                even, odd = pair
                even = even + pltpu.roll(even, LANES // 2, 1)
                odd = odd + pltpu.roll(odd, LANES // 2, 1)
                pair = []
                where_to = (RUN * j + i) // 2 * LANES
                image_ref[:, where_to : where_to + LANES] = alive * jnp.where(left_lane, even, odd)
    out_ref[...] = image_ref[:per_slab, :].astype(BF16)


def column_operands():
    return [jnp.asarray(t, dtype=BF16) for kind in (2, 1) for t in column_tables(kind)]


def early(wavefields, params, slab_counts, angle_table):
    two, _, shots, rows, cols = wavefields.shape
    field = pltpu.VMEM((rows, cols), F32)
    table = pltpu.VMEM((rows // 2 // RUN, LANES, LANES), F32)
    own = jnp.asarray(row_tables(rows)[0], dtype=BF16)
    args = [wavefields, *params, angle_table.reshape(1, -1), own, *column_operands()]
    outs = [field] * 5 + [pltpu.VMEM((LANES, LANES), F32)] * 2 + [table] * 2 + [
        pltpu.VMEM((8, LANES), F32),
        pltpu.VMEM((two * shots, 2, rows, cols), F32),
    ]
    return pl.pallas_call(
        early_kernel,
        in_specs=[pl.BlockSpec(memory_space=pltpu.SMEM)] + [VMEM_WHOLE] * len(args),
        out_specs=[VMEM_WHOLE] * len(outs),
        out_shape=outs,
        scratch_shapes=[
            pltpu.VMEM((2, 2 * rows, cols), BF16),
            pltpu.VMEM((2, 2 * rows, cols), BF16),
            pltpu.VMEM((2, 2 * rows, cols), F32),
            pltpu.VMEM((2, 2 * rows, cols), F32),
            pltpu.VMEM((2, 2 * rows, cols), F32),
        ],
        compiler_params=pltpu.CompilerParams(vmem_limit_bytes=24 << 20),
        name="early",
    )(slab_counts, *in_vmem(*args))


def late(wavefields, partner, neighbour, prepared, angles):
    two, _, shots, rows, cols = wavefields.shape
    bins = rows // 2
    per_slab = cols // rows
    items = two * shots
    _, edge, both = (jnp.asarray(t, dtype=BF16) for t in row_tables(rows))
    depth = depth_table(rows, bins)
    depth_top = depth.astype(jnp.bfloat16)
    depth_low = (depth - depth_top.astype(np.float32)).astype(jnp.bfloat16)
    depth = jnp.asarray(np.concatenate([depth_top, depth_top, depth_low], axis=1), dtype=BF16)
    args = [wavefields, partner, neighbour, *prepared, edge, both, *column_operands(), depth]
    out_shape = (per_slab, bins * angles)
    scratch = [
        pltpu.VMEM((items, 2, 48, cols), BF16),
        pltpu.VMEM((items * 2 * 32, cols), BF16),
        pltpu.VMEM((items * 2 * 32, cols), BF16),
        pltpu.VMEM((items * 2 * 32, cols), F32),
        pltpu.VMEM((items * 2 * 32, cols), F32),
        pltpu.VMEM((items * 2 * 32, cols), F32),
        pltpu.VMEM((items, 2, 24, cols), F32),
        pltpu.VMEM((2, 2 * (rows + 16), cols), BF16),
        pltpu.VMEM((2, 2 * rows, cols), BF16),
        pltpu.VMEM((2, 2 * rows, cols), F32),
        pltpu.VMEM((2, 2 * rows, cols), F32),
        pltpu.VMEM((2, 2 * rows, cols), F32),
        pltpu.VMEM((2, 3 * rows, cols), BF16),
        pltpu.VMEM((PITCH * bins, LANES), F32),
        pltpu.VMEM((8, bins * angles), F32),
        pltpu.VMEM((bins, 2 * LANES, LANES), BF16),
    ]
    return pl.pallas_call(
        late_kernel,
        in_specs=[VMEM_WHOLE] * len(args),
        out_specs=VMEM_WHOLE,
        out_shape=pltpu.VMEM(out_shape, BF16),
        scratch_shapes=scratch,
        compiler_params=pltpu.CompilerParams(vmem_limit_bytes=36 << 20),
        name="late",
    )(*in_vmem(*args))


def pick_kernel(loc_ref, *refs, per_slab):
    held_refs, (mine_ref, theirs_ref) = (refs[:-2], refs[-2:])
    slab = lax.axis_index(SLAB)
    chip, core = (lax.axis_index("chip"), lax.axis_index("core"))
    chips = lax.axis_size("chip")
    count = mine_ref.shape[0]
    per_row = LANES // count
    row = loc_ref[pl.ds(slab // per_row, 1), :]
    spot = slab % per_row
    partner = spot + 1 - 2 * core
    loc = jnp.concatenate(
        [pltpu.roll(row, (LANES - s * count) % LANES, 1)[:, :count] for s in (spot, partner)], axis=1
    )
    owner = loc // per_slab
    ahead = lax.rem(owner // 2 - chip + chips, chips)
    up = ahead <= chips // 2
    hops = jnp.where(up, ahead, chips - ahead)
    holder = jnp.where(up, 1, 0)
    index = (2 * (hops // len(NEAR)) + jnp.where(owner % 2 == holder, 0, 1)) * per_slab + loc % per_slab
    total = None
    for near, ref in enumerate(held_refs):
        held = lax.broadcasted_iota(jnp.int32, (ref.shape[0], 2 * count), 0)
        hit = (held == index) & (holder == core) & (hops % len(NEAR) == near)
        hot = jnp.where(hit, 1.0, 0.0).astype(BF16)
        part = lax.dot_general(hot, ref[...], (((0,), (0,)), ((), ())), preferred_element_type=F32)
        total = part if total is None else total + part
    mine_ref[...] = total[:count]
    theirs_ref[...] = total[count:].astype(BF16)


def pick(loc_patch, held, count, per_slab):
    width = held[0].shape[1]
    return pl.pallas_call(
        lambda *refs: pick_kernel(*refs, per_slab=per_slab),
        in_specs=[VMEM_WHOLE] * (1 + len(held)),
        out_specs=[VMEM_WHOLE] * 2,
        out_shape=[pltpu.VMEM((count, width), F32), pltpu.VMEM((count, width), BF16)],
        compiler_params=pltpu.CompilerParams(vmem_limit_bytes=8 << 20),
        name="pick",
    )(*in_vmem(loc_patch.reshape(-1, LANES), *held))


def swap_cores(array):
    return lax.ppermute(array, "core", [(0, 1), (1, 0)])


def onward(array, hops):
    chips = lax.axis_size("chip")
    pairs = [(2 * i, 2 * ((i + hops) % chips)) for i in range(chips)]
    pairs += [(2 * i + 1, 2 * ((i - hops) % chips) + 1) for i in range(chips)]
    return lax.ppermute(array, SLAB, pairs)


def spread(images):
    held = jnp.concatenate([images, swap_cores(images)])
    held = jnp.concatenate([held] + [onward(held, h) for h in FAR[1:]])
    return [held] + [onward(held, h) for h in NEAR[1:]]


def per_device(
    wavefields, courant, epsilon, anisotropy_delta, tilt_angle, loc_patch, slab_counts, angle_table
):
    slabs = lax.axis_size(SLAB)
    assert FAR[-1] + NEAR[-1] == slabs // 4
    per_slab = wavefields.shape[4] // wavefields.shape[3]
    params = (courant, epsilon, anisotropy_delta, tilt_angle)
    to_partner, to_neighbour = pack(wavefields, params)
    pairs = [(i, i + 1) for i in range(1, slabs - 1, 2)]
    neighbour = lax.ppermute(to_neighbour, SLAB, pairs + [(j, i) for i, j in pairs])
    partner = swap_cores(to_partner)
    prepared = early(wavefields, params, slab_counts, angle_table)
    images = late(wavefields, partner, neighbour, prepared, angle_table.shape[0])
    mine, theirs = pick(loc_patch, spread(images), loc_patch.shape[0] // slabs, per_slab)
    return mine + swap_cores(theirs).astype(F32)


def solution(mesh):
    shape = (mesh.shape["groups"], mesh.shape["slab"] // 2, 2)
    finer = Mesh(mesh.devices.reshape(shape), GROUPS_SLAB)
    in_specs = (
        P(None, None, "groups", SLAB, None),
        P(SLAB, None),
        P(SLAB, None),
        P(SLAB, None),
        P(SLAB, None),
        P(),
        P(),
        P(),
    )
    out_specs = P(GROUPS_SLAB, None)
    return jax.shard_map(
        per_device, mesh=finer, in_specs=in_specs, out_specs=out_specs, check_vma=False
    )
```
